16 devices in a mesh: nodes: 16 (over z, y, x, core).
Axes of the slice: x: 2, y: 2, z: 2, core: 2. Of those that a mesh axis runs over, the one named last changes fastest.
Arguments:
- adjacency: bfloat16 [16384, 16384], P('nodes')
- features: bfloat16 [16384, 100], P('nodes')
- w_hidden: float32 [100, 128], replicated
- w_output: float32 [128, 47], replicated
- labels: int32 [16384], P('nodes')
- train_mask: int32 [16384], P('nodes')
- block_mask: int32 [16, 16], replicated
Outputs:
- output 1: float32 [], replicated
- output 2: float32 [100, 128], replicated
- output 3: float32 [128, 47], replicated
All inputs are finite; a program needn't handle non-finite values.
Results may differ from the reference program's by a relative error of at most 0.001.
Values are sent between devices in bfloat16 or wider.
A program may use at most 1 GiB of HBM per device.

```python
import jax
import jax.numpy as jnp
from jax import lax

NUM_NODES = 16384
BLOCKS = 16
F_IN = 100
HID = 128
CLASSES = 47
EDGE_PERCENT = 15
BLOCK_ROWS = NUM_NODES // BLOCKS


def setup_inputs(seed: int = 0) -> dict:
    keys = jax.random.split(jax.random.key(seed), 9)
    thresholds = jax.random.randint(keys[0], (BLOCKS, 1), BLOCKS // 8, BLOCKS + 1, dtype=jnp.int32)
    block_draw = jax.random.randint(keys[1], (BLOCKS, BLOCKS), 0, BLOCKS, dtype=jnp.int32)
    block_mask = jnp.maximum((block_draw < thresholds).astype(jnp.int32), jnp.eye(BLOCKS, dtype=jnp.int32))
    col_ids = jnp.arange(NUM_NODES, dtype=jnp.int32)

    def edge_rows(block_id):
        edge_draw = jax.random.randint(jax.random.fold_in(keys[2], block_id), (BLOCK_ROWS, NUM_NODES), 0, 100, dtype=jnp.int32)
        row_ids = block_id * BLOCK_ROWS + jnp.arange(BLOCK_ROWS, dtype=jnp.int32)
        col_keep = jnp.repeat(block_mask[block_id], BLOCK_ROWS) > 0
        edge_on = ((edge_draw < EDGE_PERCENT) | (row_ids[:, None] == col_ids[None, :])) & col_keep[None, :]
        raw_weight = edge_on.astype(jnp.float32)
        return (raw_weight / jnp.sum(raw_weight, axis=1, keepdims=True)).astype(jnp.bfloat16)

    adjacency = lax.map(edge_rows, jnp.arange(BLOCKS, dtype=jnp.int32)).reshape(NUM_NODES, NUM_NODES)
    centers = jax.random.normal(keys[3], (BLOCKS, F_IN), jnp.float32)
    noise = jax.random.normal(keys[4], (NUM_NODES, F_IN), jnp.float32)
    features = (jnp.repeat(centers, BLOCK_ROWS, axis=0) + noise).astype(jnp.bfloat16)
    w_hidden = jax.random.normal(keys[5], (F_IN, HID), jnp.float32) * (F_IN ** -0.5 * BLOCKS ** 0.25)
    w_output = jax.random.normal(keys[6], (HID, CLASSES), jnp.float32) * (2.0 * HID ** -0.5)
    labels = jax.random.randint(keys[7], (NUM_NODES,), 0, CLASSES, dtype=jnp.int32)
    label_draw = jax.random.randint(keys[8], (NUM_NODES,), 0, 100, dtype=jnp.int32)
    train_mask = jnp.maximum((label_draw < 40).astype(jnp.int32), (col_ids == 0).astype(jnp.int32))
    return dict(adjacency=adjacency, features=features, w_hidden=w_hidden, w_output=w_output, labels=labels, train_mask=train_mask, block_mask=block_mask)


def masked_product(adj_blocks, block_mask, values):
    width = values.shape[-1]
    value_blocks = values.reshape(BLOCKS, BLOCK_ROWS, width)

    def one_block(block_item):
        adj_rows, mask_row = block_item
        scaled = value_blocks * mask_row.astype(values.dtype)[:, None, None]
        return jnp.dot(adj_rows, scaled.reshape(NUM_NODES, width), preferred_element_type=jnp.float32)

    return lax.map(one_block, (adj_blocks, block_mask)).reshape(NUM_NODES, width)


def masked_transpose_product(adj_blocks, block_mask, grads):
    width = grads.shape[-1]
    grad_blocks = grads.reshape(BLOCKS, BLOCK_ROWS, width)

    def add_block(running_sum, block_item):
        adj_rows, mask_row, grad_rows = block_item
        contrib = jnp.dot(adj_rows.T, grad_rows, preferred_element_type=jnp.float32)
        contrib = contrib.reshape(BLOCKS, BLOCK_ROWS, width) * mask_row.astype(jnp.float32)[:, None, None]
        return running_sum + contrib.reshape(NUM_NODES, width), None

    start_sum = jnp.zeros((NUM_NODES, width), jnp.float32)
    total_sum, _ = lax.scan(add_block, start_sum, (adj_blocks, block_mask, grad_blocks))
    return total_sum


def reference(adjacency, features, w_hidden, w_output, labels, train_mask, block_mask):
    adj_blocks = adjacency.reshape(BLOCKS, BLOCK_ROWS, NUM_NODES)
    w_hidden_bf = w_hidden.astype(jnp.bfloat16)
    w_output_bf = w_output.astype(jnp.bfloat16)
    proj_one = jnp.dot(features, w_hidden_bf, preferred_element_type=jnp.float32).astype(jnp.bfloat16)
    agg_one = masked_product(adj_blocks, block_mask, proj_one)
    hidden = jnp.maximum(agg_one, 0.0).astype(jnp.bfloat16)
    proj_two = jnp.dot(hidden, w_output_bf, preferred_element_type=jnp.float32).astype(jnp.bfloat16)
    logits = masked_product(adj_blocks, block_mask, proj_two)
    label_weight = train_mask.astype(jnp.float32)
    label_count = jnp.sum(label_weight)
    log_norm = jax.nn.logsumexp(logits, axis=-1)
    one_hot = (labels[:, None] == jnp.arange(CLASSES)[None, :]).astype(jnp.float32)
    picked = jnp.sum(logits * one_hot, axis=-1)
    mean_loss = jnp.sum(label_weight * (log_norm - picked)) / label_count
    probabilities = jnp.exp(logits - log_norm[:, None])
    grad_logits = ((probabilities - one_hot) * (label_weight / label_count)[:, None]).astype(jnp.bfloat16)
    grad_proj_two = masked_transpose_product(adj_blocks, block_mask, grad_logits).astype(jnp.bfloat16)
    grad_w_output = jnp.dot(hidden.T, grad_proj_two, preferred_element_type=jnp.float32)
    grad_hidden = jnp.dot(grad_proj_two, w_output_bf.T, preferred_element_type=jnp.float32)
    grad_agg = jnp.where(agg_one > 0, grad_hidden, 0.0).astype(jnp.bfloat16)
    grad_proj_one = masked_transpose_product(adj_blocks, block_mask, grad_agg).astype(jnp.bfloat16)
    grad_w_hidden = jnp.dot(features.T, grad_proj_one, preferred_element_type=jnp.float32)
    return (mean_loss, grad_w_hidden, grad_w_output)
```

```python
import jax
import jax.numpy as jnp
from jax import lax
from jax.experimental import pallas as pl
from jax.experimental.pallas import tpu as pltpu
from jax.sharding import PartitionSpec as P

AXIS_NAME = 'nodes'
MESH = pl.DeviceIdType.MESH
F32, BF16 = jnp.float32, jnp.bfloat16
BLK = 1024
NB = 16
F_IN, F_PAD, MASK_ROW = 100, 112, 100
HID = 128
CLS, CLS_PAD = 47, 48
QS = [0, 1, 2, 4, 3, 5, 6, 7]
QI = {q: i for i, q in enumerate(QS)}
ORDERS = [(1, 2, 4), (2, 4, 1), (4, 1, 2)]
X_CHUNKS = [(0, 48), (48, 32), (80, 32)]
Y_CHUNKS = [(0, 16), (16, 16), (32, 16)]
D1_CHUNKS = [(0, 48), (48, 40), (88, 40)]
AR_ROWS = 80


def dot_last(lhs, rhs):
    return lax.dot_general(lhs, rhs, (((1,), (1,)), ((), ())), preferred_element_type=F32)


def dot_first(lhs, rhs):
    return lax.dot_general(lhs, rhs, (((0,), (0,)), ((), ())), preferred_element_type=F32)


def step_kernel(adj_hbm, x_hbm, wh_ref, wot_ref, lab_ref, msk_ref, bm_ref, gwh_ref, gwot_ref, loss_ref,
                adj, xall, yall, z1, z1t, z2, hid, gt, et, con, part2, part1, rb2, rb1, whs, wos, macc, lossv, gwhs, gwos, ar, arp, ars, arb, arg,
                a_sem, x_sem, ici_send, d2d_send, ag1_recv, ag1_d2d, ag2_recv, ag2_d2d, rs2_recv, rs2_d2d, rs1_recv, rs1_d2d,
                ar_send, ar_recv):
    me = lax.axis_index(AXIS_NAME)
    coords = [me % 2, (me // 2) % 2, (me // 4) % 2, me // 8]

    def dev(rel):
        total = 0
        for bit in range(4):
            total = total + ((coords[bit] + ((rel >> bit) & 1)) % 2) * (1 << bit)
        return total

    def rel_of(slot):
        return 2 * QS[slot // 2] + slot % 2

    def rcopy(src, dst, send_sem, recv_sem, rel):
        return pltpu.make_async_remote_copy(src_ref=src, dst_ref=dst, send_sem=send_sem, recv_sem=recv_sem,
                                            device_id=(dev(rel),), device_id_type=MESH)

    def a_copy(slot, blk=0):
        return pltpu.make_async_copy(adj_hbm.at[:, pl.ds(pl.multiple_of(blk * BLK, BLK), BLK)], adj.at[slot], a_sem.at[slot])

    a_order = [0, 1, 2, 4, 6, 3, 5, 7, 8, 10, 12, 9, 11, 13, 14, 15]

    def start_a(lo, hi):
        for slot in a_order[lo:hi]:
            a_copy(slot, dev(rel_of(slot))).start()

    x_copy = pltpu.make_async_copy(x_hbm, xall.at[0], x_sem)
    x_copy.start()
    start_a(0, 6)
    barrier = pltpu.get_barrier_semaphore()
    peers = [1] + [2 * q for q in range(1, 8)]
    for rel in peers:
        pl.semaphore_signal(barrier, inc=1, device_id=(dev(rel),), device_id_type=MESH)

    whs[...] = jnp.zeros_like(whs)
    whs[0:F_IN, :] = wh_ref[...].astype(BF16)
    wos[...] = jnp.zeros_like(wos)
    wos[0:CLS, :] = wot_ref[...].astype(BF16)
    macc[...] = jnp.zeros_like(macc)
    x_copy.wait()
    pl.semaphore_wait(barrier, len(peers))

    def mask_of(slot):
        if isinstance(slot, int):
            return bm_ref[me, dev(rel_of(slot))]
        i = slot // 2
        c = slot % 2
        bits = []
        for bit in (1, 2, 4):
            b = 0
            for pos, q in enumerate(QS):
                if q & bit:
                    d = (i - pos) * (i - pos)
                    b = b + 1 // (1 + d)
            bits.append(b)
        total = ((coords[0] + c) % 2)
        for n, b in enumerate(bits):
            total = total + ((coords[n + 1] + b) % 2) * (2 << n)
        return bm_ref[me, total]


    def ag_ops(buf, chunks, recv, recv_d2d):
        def ici(src_q, dim, k):
            dst_q = src_q ^ dim
            lo, n = chunks[k]
            idx = k * 7 + QI[dst_q] - 1
            return rcopy(buf.at[2 * QI[src_q], pl.ds(lo, n), :], buf.at[2 * QI[dst_q], pl.ds(lo, n), :],
                         ici_send.at[idx], recv.at[idx], 2 * dim)

        def d2d(q_idx):
            return rcopy(buf.at[2 * q_idx], buf.at[2 * q_idx + 1], d2d_send.at[q_idx], recv_d2d.at[q_idx], 1)

        def recv_wait(dst_q, k):
            o = ORDERS[k]
            dim = max((d for d in o if dst_q & d), key=o.index)
            ici(dst_q ^ dim, dim, k).wait_recv()

        def send_own():
            for j in range(3):
                for k in range(3):
                    ici(0, ORDERS[k][j], k).start()
            d2d(0).start()

        def near():
            for k in range(3):
                a, b, c = ORDERS[k]
                recv_wait(a, k)
                ici(a, b, k).start()
                ici(a, c, k).start()
            for k in range(3):
                a, b, c = ORDERS[k]
                recv_wait(b, k)
                ici(b, c, k).start()

        def near_last():
            for k in range(3):
                recv_wait(ORDERS[k][2], k)
            for q in (1, 2, 4):
                d2d(QI[q]).start()

        def mid():
            for k in range(3):
                a, b, c = ORDERS[k]
                recv_wait(a | b, k)
                ici(a | b, c, k).start()

        def mid_last():
            for k in range(3):
                recv_wait(ORDERS[k][0] | ORDERS[k][2], k)
            for k in range(3):
                recv_wait(ORDERS[k][1] | ORDERS[k][2], k)
            for q in (3, 5, 6):
                d2d(QI[q]).start()

        def far():
            for k in range(3):
                recv_wait(7, k)
            d2d(QI[7]).start()

        def wait_sends():
            for k in range(3):
                o = ORDERS[k]
                for q in range(1, 8):
                    dim = max((d for d in o if q & d), key=o.index)
                    ici(q ^ dim, dim, k).wait_send()
            for i in range(8):
                d2d(i).wait_send()

        return dict(d2d=d2d, send_own=send_own, near=near, near_last=near_last, mid=mid, mid_last=mid_last, far=far,
                    wait_sends=wait_sends)

    def forward_pass(ag, compute, first):
        compute(0)
        ag['near']()
        ag['d2d'](0).wait_recv()
        compute(1)
        ag['near_last']()

        def group(g, carry):
            base = 2 + (g % 2) + 6 * (g // 2)

            @pl.when(g == 1)
            def _():
                ag['mid']()
                for q in (1, 2, 4):
                    ag['d2d'](QI[q]).wait_recv()

            @pl.when(g == 2)
            def _():
                ag['mid_last']()

            @pl.when(g == 3)
            def _():
                ag['far']()
                for q in (3, 5, 6):
                    ag['d2d'](QI[q]).wait_recv()

            for j in range(3):
                compute(base + 2 * j)
            return carry

        lax.fori_loop(0, 4, group, 0)
        compute(14)
        ag['d2d'](7).wait_recv()
        compute(15)
        ag['wait_sends']()

    ag1 = ag_ops(xall, X_CHUNKS, ag1_recv, ag1_d2d)
    ag1['send_own']()
    start_a(6, 16)

    def compute1(slot):
        a_copy(slot).wait()
        xt = xall[slot]
        macc[...] += xall[slot, MASK_ROW - 4:MASK_ROW + 12, :].astype(F32)
        yt = (dot_first(whs[...], xt).astype(BF16).astype(F32) * mask_of(slot).astype(F32)).astype(BF16)
        prod = dot_last(adj[slot], yt)
        if isinstance(slot, int) and slot == 0:
            z1[...] = prod
        else:
            z1[...] += prod

    forward_pass(ag1, compute1, True)
    label_count = jnp.sum(macc[4:5, :])

    hid[...] = jnp.maximum(z1[...], 0.0).astype(BF16)
    yall[0] = dot_last(wos[...], hid[...]).astype(BF16)
    ag2 = ag_ops(yall, Y_CHUNKS, ag2_recv, ag2_d2d)
    z1t[...] = jnp.transpose(z1[...])
    ag2['send_own']()

    def compute2(slot):
        yt = (yall[slot].astype(F32) * mask_of(slot).astype(F32)).astype(BF16)
        prod = dot_last(adj[slot], yt)
        if isinstance(slot, int) and slot == 0:
            z2[...] = prod
        else:
            z2[...] += prod

    forward_pass(ag2, compute2, False)

    zt = jnp.transpose(z2[...])
    cls_id = lax.broadcasted_iota(jnp.int32, (CLS_PAD, BLK), 0)
    valid = cls_id < CLS
    top = jnp.max(jnp.where(valid, zt, -jnp.inf), axis=0, keepdims=True)
    expz = jnp.where(valid, jnp.exp(zt - top), 0.0)
    log_norm = jnp.log(jnp.sum(expz, axis=0, keepdims=True)) + top
    one_hot = cls_id == lab_ref[...]
    picked = jnp.sum(jnp.where(one_hot, zt, 0.0), axis=0, keepdims=True)
    weight = msk_ref[...].astype(F32)
    loss_terms = weight * (log_norm - picked)
    acc = loss_terms[:, 0:128]
    for n in range(1, BLK // 128):
        acc = acc + loss_terms[:, 128 * n:128 * (n + 1)]
    lossv[...] = acc
    prob = jnp.exp(zt - log_norm)
    grad = (prob - one_hot.astype(F32)) * (weight / label_count)
    gt[...] = jnp.where(valid, grad, 0.0).astype(BF16)


    def reduce_pass(lhs_ref, rows, chunks, part, rb, recv, recv_d2d):
        def dim_of(q, k):
            return next(d for d in reversed(ORDERS[k]) if q & d)

        def ici(q, k):
            lo, n = chunks[k]
            idx = k * 7 + QI[q] - 1
            return rcopy(con.at[2 * QI[q], pl.ds(lo, n), :], rb.at[QI[q] - 1, pl.ds(lo, n), :], ici_send.at[idx],
                         recv.at[idx], 2 * dim_of(q, k))

        def d2d(i):
            return rcopy(con.at[2 * i + 1, pl.ds(0, rows), :], part.at[i], d2d_send.at[i], recv_d2d.at[i], 1)

        def sources(q, k):
            out = []
            for d in reversed(ORDERS[k]):
                if q & d:
                    break
                out.append(q ^ d)
            return out

        def compute(slot):
            lhs = (lhs_ref[...].astype(F32) * mask_of(slot).astype(F32)).astype(BF16)
            con[slot, 0:rows, :] = jnp.dot(lhs, adj[slot], preferred_element_type=F32)

        waiting = {(q, k): set(sources(q, k)) for q in range(8) for k in range(3)}

        def pair_sum(q):
            i = QI[q]
            d2d(i).wait_recv()
            con[2 * i, 0:rows, :] += part[i]
            for k in range(3):
                if q and not waiting[q, k]:
                    ici(q, k).start()

        def take(src, k):
            d = dim_of(src, k)
            q = src ^ d
            lo, n = chunks[k]
            ici(src, k).wait_recv()
            con[2 * QI[q], lo:lo + n, :] += rb[QI[src] - 1, lo:lo + n, :]
            waiting[q, k].discard(src)
            if q and not waiting[q, k]:
                ici(q, k).start()

        def body(n, carry):
            i = 7 - n
            compute(2 * i + 1)
            d2d(i).start()
            compute(2 * i)
            for m in range(1, 8):
                @pl.when(n == m)
                def _(m=m):
                    pair_sum(QS[8 - m])
            return carry

        lax.fori_loop(0, 8, body, 0)
        pair_sum(0)
        send_rank = {q: r for r, q in enumerate(reversed(QS))}
        todo = []
        for k in range(3):
            for src in range(1, 8):
                phase = list(reversed(ORDERS[k])).index(dim_of(src, k))
                todo.append((phase, send_rank[src], k, src))
        for phase, _, k, src in sorted(todo):
            take(src, k)
        for k in range(3):
            for q in range(1, 8):
                ici(q, k).wait_send()
        for i in range(8):
            d2d(i).wait_send()

    reduce_pass(gt, CLS_PAD, Y_CHUNKS, part2, rb2, rs2_recv, rs2_d2d)
    d2t = con[0, 0:CLS_PAD, :].astype(BF16)
    gwo = jnp.dot(d2t, hid[...], preferred_element_type=F32)
    et[...] = jnp.where(z1t[...] > 0, dot_first(wos[...], d2t), 0.0).astype(BF16)
    row_id = lax.broadcasted_iota(jnp.int32, (CLS_PAD, HID), 0)
    gwos[...] = jnp.where(row_id == CLS, lossv[...], gwo)

    reduce_pass(et, HID, D1_CHUNKS, part1, rb1, rs1_recv, rs1_d2d)
    d1t = con[0].astype(BF16)
    gwhs[...] = dot_last(xall[0], d1t)

    ar[0] = gwhs[0:AR_ROWS, :]
    ar[1, 0:24, :] = gwhs[AR_ROWS:104, :]
    ar[1, 24:72, :] = gwos[...]
    ar[1, 72:80, :] = jnp.zeros((8, HID), F32)
    core = coords[0]
    pair = rcopy(ar.at[1 - core], arp, ar_send.at[0], ar_recv.at[0], 1)
    pair.start()
    pair.wait()
    arg[0] = ar[core] + arp[...]
    sends = [rcopy(arg.at[0], arg.at[q], ar_send.at[q], ar_recv.at[q], 2 * q) for q in range(1, 8)]
    for q in (7, 6, 5, 3, 4, 2, 1):
        sends[q - 1].start()
    for cp in sends:
        cp.wait()
    total = ((arg[0] + arg[1]) + (arg[2] + arg[3])) + ((arg[4] + arg[5]) + (arg[6] + arg[7]))
    ars[...] = total
    back = rcopy(ars, arb, ar_send.at[8], ar_recv.at[8], 1)
    back.start()
    ar[core] = total
    back.wait()
    ar[1 - core] = arb[...]
    gwh_ref[0:AR_ROWS, :] = ar[0]
    gwh_ref[AR_ROWS:F_IN, :] = ar[1, 0:F_IN - AR_ROWS, :]
    gwot_ref[...] = ar[1, 24:24 + CLS, :]
    loss_ref[...] = jnp.sum(ar[1, 24 + CLS:24 + CLS_PAD, :], axis=1, keepdims=True) / label_count


def device_step(adj_rows, feat_rows, w_hidden, w_output, labels, train_mask, block_mask):
    mask_row = train_mask.astype(BF16)[None, :]
    x_ext = jnp.concatenate([feat_rows.T, mask_row, jnp.zeros((F_PAD - F_IN - 1, BLK), BF16)], axis=0)
    dma = pltpu.SemaphoreType.DMA
    vmem = pl.BlockSpec(memory_space=pltpu.VMEM)
    hbm = pl.BlockSpec(memory_space=pl.ANY)
    gwh, gwot, loss = pl.pallas_call(
        step_kernel,
        name='gcn_step',
        out_shape=(jax.ShapeDtypeStruct((F_IN, HID), F32), jax.ShapeDtypeStruct((CLS, HID), F32),
                   jax.ShapeDtypeStruct((1, 1), F32)),
        in_specs=[hbm, hbm, vmem, vmem, vmem, vmem, pl.BlockSpec(memory_space=pltpu.SMEM)],
        out_specs=(vmem, vmem, vmem),
        scratch_shapes=[
            pltpu.VMEM((NB, BLK, BLK), BF16),
            pltpu.VMEM((NB, F_PAD, BLK), BF16),
            pltpu.VMEM((NB, CLS_PAD, BLK), BF16),
            pltpu.VMEM((BLK, HID), F32),
            pltpu.VMEM((HID, BLK), F32),
            pltpu.VMEM((BLK, CLS_PAD), F32),
            pltpu.VMEM((BLK, HID), BF16),
            pltpu.VMEM((CLS_PAD, BLK), BF16),
            pltpu.VMEM((HID, BLK), BF16),
            pltpu.VMEM((NB, HID, BLK), F32),
            pltpu.VMEM((8, CLS_PAD, BLK), F32),
            pltpu.VMEM((8, HID, BLK), F32),
            pltpu.VMEM((7, CLS_PAD, BLK), F32),
            pltpu.VMEM((7, HID, BLK), F32),
            pltpu.VMEM((F_PAD, HID), BF16),
            pltpu.VMEM((CLS_PAD, HID), BF16),
            pltpu.VMEM((16, BLK), F32),
            pltpu.VMEM((1, 128), F32),
            pltpu.VMEM((F_PAD, HID), F32),
            pltpu.VMEM((CLS_PAD, HID), F32),
            pltpu.VMEM((2, AR_ROWS, HID), F32),
            pltpu.VMEM((AR_ROWS, HID), F32),
            pltpu.VMEM((AR_ROWS, HID), F32),
            pltpu.VMEM((AR_ROWS, HID), F32),
            pltpu.VMEM((8, AR_ROWS, HID), F32),
            dma((NB,)), dma, dma((21,)), dma((8,)),
            dma((21,)), dma((8,)), dma((21,)), dma((8,)), dma((21,)), dma((8,)), dma((21,)), dma((8,)),
            dma((9,)), dma((9,)),
        ],
        compiler_params=pltpu.CompilerParams(collective_id=0, has_side_effects=True, vmem_limit_bytes=67043328),
    )(adj_rows, x_ext, w_hidden, w_output.T, labels[None, :], train_mask[None, :], block_mask)
    return loss[0, 0], gwh, gwot.T


def solution(mesh):
    row_spec = P(AXIS_NAME, None)
    vec_spec = P(AXIS_NAME)
    return jax.shard_map(device_step, mesh=mesh, in_specs=(row_spec, row_spec, P(), P(), vec_spec, vec_spec, P()), out_specs=(P(), P(), P()), check_vma=False)
```

```python
import jax
import jax.numpy as jnp
from jax import lax
from jax.experimental import pallas as pl
from jax.experimental.pallas import tpu as pltpu
from jax.sharding import PartitionSpec as P

AXIS_NAME = 'nodes'
MESH = pl.DeviceIdType.MESH
F32, BF16 = jnp.float32, jnp.bfloat16
BLK = 1024
NB = 16
F_IN, F_PAD = 100, 104
HID = 128
CLS, CLS_PAD = 47, 48
QS = [0, 1, 2, 4, 3, 5, 6, 7]
QI = {q: i for i, q in enumerate(QS)}
ORDERS = [(1, 2, 4), (2, 4, 1), (4, 1, 2)]
X_CHUNKS = [(0, 40), (40, 32), (72, 32)]
Y_CHUNKS = [(0, 16), (16, 16), (32, 16)]
D1_CHUNKS = [(0, 48), (48, 40), (88, 40)]
GWO_HALF, GWH_HALF = 24, 56
M_TILE = 256


def dot_last(lhs, rhs):
    return lax.dot_general(lhs, rhs, (((1,), (1,)), ((), ())), preferred_element_type=F32)


def dot_first(lhs, rhs):
    return lax.dot_general(lhs, rhs, (((0,), (0,)), ((), ())), preferred_element_type=F32)


def step_kernel(adj_hbm, x_ref, wh_ref, wot_ref, lab_ref, msk_ref, bm_ref, gwh_ref, gwot_ref, loss_ref,
                adj, xall, yall, y1b, z1, z1t, z2, hid, gt, et, con, part2, part1, rb2, rb1, whs, wos, macc, lossv,
                gwos, gwop, gwor, gwog, gwof, gwhs, gwhp, gwhr, gwhg, gwhf,
                a_sem, ici_send, d2d_send, recv_a, d2d_a, recv_b, d2d_b,
                gwo_send, gwo_recv, gwh_send, gwh_recv):
    me = lax.axis_index(AXIS_NAME)
    coords = [me % 2, (me // 2) % 2, (me // 4) % 2, me // 8]

    def dev(rel):
        total = 0
        for bit in range(4):
            total = total + ((coords[bit] + ((rel >> bit) & 1)) % 2) * (1 << bit)
        return total

    def rel_of(slot):
        return 2 * QS[slot // 2] + slot % 2

    def rcopy(src, dst, send_sem, recv_sem, rel):
        return pltpu.make_async_remote_copy(src_ref=src, dst_ref=dst, send_sem=send_sem, recv_sem=recv_sem,
                                            device_id=(dev(rel),), device_id_type=MESH)

    def a_copy(slot, blk=0):
        return pltpu.make_async_copy(adj_hbm.at[:, pl.ds(pl.multiple_of(blk * BLK, BLK), BLK)], adj.at[slot], a_sem.at[slot])

    a_order = [0, 1, 2, 4, 6, 3, 5, 7, 8, 10, 12, 9, 11, 13, 14, 15]

    def start_a(lo, hi):
        for slot in a_order[lo:hi]:
            a_copy(slot, dev(rel_of(slot))).start()

    start_a(0, 6)
    barrier = pltpu.get_barrier_semaphore()
    peers = [1] + [2 * q for q in range(1, 8)]
    for rel in peers:
        pl.semaphore_signal(barrier, inc=1, device_id=(dev(rel),), device_id_type=MESH)

    xall[0, 0:F_PAD - 8, :] = x_ref[0:F_PAD - 8, :]
    xall[0, F_PAD - 8:F_PAD, :] = jnp.concatenate([x_ref[F_PAD - 8:F_IN, :], jnp.zeros((F_PAD - F_IN, BLK), BF16)], axis=0)
    whs[...] = jnp.zeros_like(whs)
    whs[0:F_IN, :] = wh_ref[...].astype(BF16)
    wos[...] = jnp.zeros_like(wos)
    wos[0:CLS, :] = wot_ref[...].astype(BF16)
    macc[...] = jnp.zeros_like(macc)
    z1[...] = jnp.zeros_like(z1)
    z2[...] = jnp.zeros_like(z2)
    pl.semaphore_wait(barrier, len(peers))

    def mask_of(slot):
        if isinstance(slot, int):
            return bm_ref[me, dev(rel_of(slot))]
        i = slot // 2
        c = slot % 2
        bits = []
        for bit in (1, 2, 4):
            b = 0
            for pos, q in enumerate(QS):
                if q & bit:
                    d = (i - pos) * (i - pos)
                    b = b + 1 // (1 + d)
            bits.append(b)
        total = ((coords[0] + c) % 2)
        for n, b in enumerate(bits):
            total = total + ((coords[n + 1] + b) % 2) * (2 << n)
        return bm_ref[me, total]


    def ag_ops(buf, chunks, recv, recv_d2d):
        def ici(src_q, dim, k):
            dst_q = src_q ^ dim
            lo, n = chunks[k]
            idx = k * 7 + QI[dst_q] - 1
            return rcopy(buf.at[2 * QI[src_q], pl.ds(lo, n), :], buf.at[2 * QI[dst_q], pl.ds(lo, n), :],
                         ici_send.at[idx], recv.at[idx], 2 * dim)

        def d2d(q_idx):
            return rcopy(buf.at[2 * q_idx], buf.at[2 * q_idx + 1], d2d_send.at[q_idx], recv_d2d.at[q_idx], 1)

        def recv_wait(dst_q, k):
            o = ORDERS[k]
            dim = max((d for d in o if dst_q & d), key=o.index)
            ici(dst_q ^ dim, dim, k).wait_recv()

        def send_own():
            for j in range(3):
                for k in range(3):
                    ici(0, ORDERS[k][j], k).start()
            d2d(0).start()

        def near():
            for k in range(3):
                a, b, c = ORDERS[k]
                recv_wait(a, k)
                ici(a, b, k).start()
                ici(a, c, k).start()
            for k in range(3):
                a, b, c = ORDERS[k]
                recv_wait(b, k)
                ici(b, c, k).start()

        def near_last():
            for k in range(3):
                recv_wait(ORDERS[k][2], k)
            for q in (1, 2, 4):
                d2d(QI[q]).start()

        def mid():
            for k in range(3):
                a, b, c = ORDERS[k]
                recv_wait(a | b, k)
                ici(a | b, c, k).start()

        def mid_last():
            for k in range(3):
                recv_wait(ORDERS[k][0] | ORDERS[k][2], k)
            for k in range(3):
                recv_wait(ORDERS[k][1] | ORDERS[k][2], k)
            for q in (3, 5, 6):
                d2d(QI[q]).start()

        def far():
            for k in range(3):
                recv_wait(7, k)
            d2d(QI[7]).start()

        def wait_sends():
            for k in range(3):
                o = ORDERS[k]
                for q in range(1, 8):
                    dim = max((d for d in o if q & d), key=o.index)
                    ici(q ^ dim, dim, k).wait_send()
            for i in range(8):
                d2d(i).wait_send()

        return dict(d2d=d2d, send_own=send_own, near=near, near_last=near_last, mid=mid, mid_last=mid_last, far=far,
                    wait_sends=wait_sends)

    def forward_pass(ag, compute):
        compute([0])
        ag['near']()
        ag['d2d'](0).wait_recv()
        compute([1])
        ag['near_last']()

        def group(g, carry):
            base = 2 + (g % 2) + 6 * (g // 2)

            @pl.when(g == 1)
            def _():
                ag['mid']()
                for q in (1, 2, 4):
                    ag['d2d'](QI[q]).wait_recv()

            @pl.when(g == 2)
            def _():
                ag['mid_last']()

            @pl.when(g == 3)
            def _():
                ag['far']()
                for q in (3, 5, 6):
                    ag['d2d'](QI[q]).wait_recv()

            compute([base, base + 2, base + 4])
            return carry

        lax.fori_loop(0, 4, group, 0)
        compute([14])
        ag['d2d'](7).wait_recv()
        compute([15])
        ag['wait_sends']()

    ag1 = ag_ops(xall, X_CHUNKS, recv_a, d2d_a)
    ag1['send_own']()
    start_a(6, 16)

    def accumulate(out, slots, blocks):
        for lo in range(0, BLK, M_TILE):
            acc = out[lo:lo + M_TILE, :]
            for slot, block in zip(slots, blocks):
                acc = acc + dot_last(adj[slot, lo:lo + M_TILE, :], block)
            out[lo:lo + M_TILE, :] = acc

    def compute1(slots):
        for slot in slots:
            a_copy(slot).wait()
        for j, slot in enumerate(slots):
            yt = dot_first(whs[...], xall[slot]).astype(BF16)
            y1b[j] = (yt.astype(F32) * mask_of(slot).astype(F32)).astype(BF16)
        accumulate(z1, slots, [y1b[j] for j in range(len(slots))])

    forward_pass(ag1, compute1)

    hid[...] = jnp.maximum(z1[...], 0.0).astype(BF16)
    cls_id = lax.broadcasted_iota(jnp.int32, (CLS_PAD, BLK), 0)
    weight = msk_ref[...].astype(F32)
    yall[0] = jnp.where(cls_id == CLS, weight, dot_last(wos[...], hid[...])).astype(BF16)
    ag2 = ag_ops(yall, Y_CHUNKS, recv_b, d2d_b)
    ag2['send_own']()
    z1t[...] = jnp.transpose(z1[...])

    def compute2(slots):
        blocks = []
        for slot in slots:
            macc[...] += yall[slot, CLS_PAD - 16:CLS_PAD, :].astype(F32)
            blocks.append((yall[slot].astype(F32) * mask_of(slot).astype(F32)).astype(BF16))
        accumulate(z2, slots, blocks)

    forward_pass(ag2, compute2)
    label_count = jnp.sum(macc[15:16, :])

    zt = jnp.transpose(z2[...])
    valid = cls_id < CLS
    top = jnp.max(jnp.where(valid, zt, -jnp.inf), axis=0, keepdims=True)
    expz = jnp.where(valid, jnp.exp(zt - top), 0.0)
    log_norm = jnp.log(jnp.sum(expz, axis=0, keepdims=True)) + top
    one_hot = cls_id == lab_ref[...]
    picked = jnp.sum(jnp.where(one_hot, zt, 0.0), axis=0, keepdims=True)
    loss_terms = weight * (log_norm - picked)
    acc = loss_terms[:, 0:128]
    for n in range(1, BLK // 128):
        acc = acc + loss_terms[:, 128 * n:128 * (n + 1)]
    lossv[...] = acc
    prob = jnp.exp(zt - log_norm)
    grad = (prob - one_hot.astype(F32)) * (weight / label_count)
    gt[...] = jnp.where(valid, grad, 0.0).astype(BF16)


    def reduce_pass(lhs_ref, rows, chunks, part, rb, recv, recv_d2d, early, hooks):
        def dim_of(q, k):
            return next(d for d in reversed(ORDERS[k]) if q & d)

        def ici(q, k):
            lo, n = chunks[k]
            idx = k * 7 + QI[q] - 1
            return rcopy(con.at[2 * QI[q], pl.ds(lo, n), :], rb.at[QI[q] - 1, pl.ds(lo, n), :], ici_send.at[idx],
                         recv.at[idx], 2 * dim_of(q, k))

        def d2d(i):
            return rcopy(con.at[2 * i + 1, pl.ds(0, rows), :], part.at[i], d2d_send.at[i], recv_d2d.at[i], 1)

        def sources(q, k):
            out = []
            for d in reversed(ORDERS[k]):
                if q & d:
                    break
                out.append(q ^ d)
            return out

        def compute(slot):
            lhs = (lhs_ref[...].astype(F32) * mask_of(slot).astype(F32)).astype(BF16)
            con[slot, 0:rows, :] = jnp.dot(lhs, adj[slot], preferred_element_type=F32)

        waiting = {(q, k): set(sources(q, k)) for q in range(8) for k in range(3)}

        def pair_sum(q):
            i = QI[q]
            d2d(i).wait_recv()
            con[2 * i, 0:rows, :] += part[i]
            for k in range(3):
                if q and not waiting[q, k]:
                    ici(q, k).start()

        def take(src, k):
            d = dim_of(src, k)
            q = src ^ d
            lo, n = chunks[k]
            ici(src, k).wait_recv()
            con[2 * QI[q], lo:lo + n, :] += rb[QI[src] - 1, lo:lo + n, :]
            waiting[q, k].discard(src)
            if q and not waiting[q, k]:
                ici(q, k).start()

        def body(n, carry):
            i = 7 - n
            compute(2 * i + 1)
            d2d(i).start()
            compute(2 * i)
            for m in range(8):
                @pl.when(n == m)
                def _(m=m):
                    if m:
                        pair_sum(QS[8 - m])
                    for r in early.get(m, ()):
                        take_rank(r)
                    for hook in hooks.get(m, ()):
                        hook()
            return carry

        rank = {q: r for r, q in enumerate(reversed(QS))}
        taken = set()

        def sources_of(k, phase):
            d = ORDERS[k][2 - phase]
            later = [e for e in ORDERS[k][3 - phase:]]
            return sorted((q for q in range(1, 8) if q & d and not any(q & e for e in later)), key=rank.get)

        def take_rank(r, phase=0):
            for k in range(3):
                take(sources_of(k, phase)[r], k)
                taken.add((phase, r))

        lax.fori_loop(0, 8, body, 0)
        for r in range(4):
            if (0, r) not in taken:
                take_rank(r)
            if r == 2:
                for hook in hooks.get('mid', ()):
                    hook()
                pair_sum(0)
        take_rank(0, 1)
        take_rank(1, 1)
        for hook in hooks.get('late', ()):
            hook()
        take_rank(0, 2)
        for k in range(3):
            for q in range(1, 8):
                ici(q, k).wait_send()
        for i in range(8):
            d2d(i).wait_send()

    reduce_pass(gt, CLS_PAD, Y_CHUNKS, part2, rb2, recv_a, d2d_a, {6: [0], 7: [1]}, {})
    d2t = con[0, 0:CLS_PAD, :].astype(BF16)
    gwo = jnp.dot(d2t, hid[...], preferred_element_type=F32)
    et[...] = jnp.where(z1t[...] > 0, dot_first(wos[...], d2t), 0.0).astype(BF16)
    row_id = lax.broadcasted_iota(jnp.int32, (CLS_PAD, HID), 0)
    gwos[...] = jnp.where(row_id == CLS, lossv[...], gwo)

    core = coords[0]

    def all_sum(rows, total_rows, src, halves, other, own, gathered, final, send, recv):
        def prepare():
            halves[0] = src[0:rows, :]
            halves[1, 0:total_rows - rows, :] = src[rows:total_rows, :]
            if total_rows < 2 * rows:
                halves[1, total_rows - rows:rows, :] = jnp.zeros((2 * rows - total_rows, HID), F32)

        pair = rcopy(halves.at[1 - core], other, send.at[0], recv.at[0], 1)
        sends = [rcopy(gathered.at[0], gathered.at[q], send.at[q], recv.at[q], 2 * q) for q in range(1, 8)]
        back = rcopy(own, final, send.at[8], recv.at[8], 1)

        def start():
            prepare()
            pair.start()

        def spread():
            pair.wait()
            gathered[0] = halves[core] + other[...]
            for q in (7, 6, 5, 3, 4, 2, 1):
                sends[q - 1].start()

        def collect():
            for cp in sends:
                cp.wait()
            g = gathered
            own[...] = ((g[0] + g[1]) + (g[2] + g[3])) + ((g[4] + g[5]) + (g[6] + g[7]))
            back.start()

        def finish():
            halves[core] = own[...]
            back.wait()
            halves[1 - core] = final[...]

        return start, spread, collect, finish

    gwo_start, gwo_spread, gwo_collect, gwo_finish = all_sum(GWO_HALF, CLS_PAD, gwos, gwop, gwof.at[0], gwor, gwog,
                                                             gwof.at[1], gwo_send, gwo_recv)
    gwh_start, gwh_spread, gwh_collect, gwh_finish = all_sum(GWH_HALF, F_PAD, gwhs, gwhp, gwhf.at[0], gwhr, gwhg,
                                                             gwhf.at[1], gwh_send, gwh_recv)
    gwo_start()

    def gwo_out():
        gwo_finish()
        gwot_ref[0:GWO_HALF, :] = gwop[0]
        gwot_ref[GWO_HALF:CLS, :] = gwop[1, 0:CLS - GWO_HALF, :]
        loss_ref[...] = jnp.sum(gwop[1, GWO_HALF - 1:GWO_HALF, :], axis=1, keepdims=True) / label_count

    reduce_pass(et, HID, D1_CHUNKS, part1, rb1, recv_b, d2d_b, {},
                {0: [gwo_spread], 'mid': [gwo_collect], 'late': [gwo_out]})
    gwhs[...] = dot_last(xall[0], con[0].astype(BF16))
    gwh_start()
    gwh_spread()
    gwh_collect()
    gwh_finish()
    gwh_ref[0:GWH_HALF, :] = gwhp[0]
    gwh_ref[GWH_HALF:F_IN, :] = gwhp[1, 0:F_IN - GWH_HALF, :]


def device_step(adj_rows, feat_rows, w_hidden, w_output, labels, train_mask, block_mask):
    dma = pltpu.SemaphoreType.DMA
    vmem = pl.BlockSpec(memory_space=pltpu.VMEM)
    hbm = pl.BlockSpec(memory_space=pl.ANY)
    gwh, gwot, loss = pl.pallas_call(
        step_kernel,
        name='gcn_step',
        out_shape=(jax.ShapeDtypeStruct((F_IN, HID), F32), jax.ShapeDtypeStruct((CLS, HID), F32),
                   jax.ShapeDtypeStruct((1, 1), F32)),
        in_specs=[hbm, vmem, vmem, vmem, vmem, vmem, pl.BlockSpec(memory_space=pltpu.SMEM)],
        out_specs=(vmem, vmem, vmem),
        scratch_shapes=[
            pltpu.VMEM((NB, BLK, BLK), BF16),
            pltpu.VMEM((NB, F_PAD, BLK), BF16),
            pltpu.VMEM((NB, CLS_PAD, BLK), BF16),
            pltpu.VMEM((3, HID, BLK), BF16),
            pltpu.VMEM((BLK, HID), F32),
            pltpu.VMEM((HID, BLK), F32),
            pltpu.VMEM((BLK, CLS_PAD), F32),
            pltpu.VMEM((BLK, HID), BF16),
            pltpu.VMEM((CLS_PAD, BLK), BF16),
            pltpu.VMEM((HID, BLK), BF16),
            pltpu.VMEM((NB, HID, BLK), F32),
            pltpu.VMEM((8, CLS_PAD, BLK), F32),
            pltpu.VMEM((8, HID, BLK), F32),
            pltpu.VMEM((7, CLS_PAD, BLK), F32),
            pltpu.VMEM((7, HID, BLK), F32),
            pltpu.VMEM((F_PAD, HID), BF16),
            pltpu.VMEM((CLS_PAD, HID), BF16),
            pltpu.VMEM((16, BLK), F32),
            pltpu.VMEM((1, 128), F32),
            pltpu.VMEM((CLS_PAD, HID), F32),
            pltpu.VMEM((2, GWO_HALF, HID), F32),
            pltpu.VMEM((GWO_HALF, HID), F32),
            pltpu.VMEM((8, GWO_HALF, HID), F32),
            pltpu.VMEM((2, GWO_HALF, HID), F32),
            pltpu.VMEM((F_PAD, HID), F32),
            pltpu.VMEM((2, GWH_HALF, HID), F32),
            pltpu.VMEM((GWH_HALF, HID), F32),
            pltpu.VMEM((8, GWH_HALF, HID), F32),
            pltpu.VMEM((2, GWH_HALF, HID), F32),
            dma((NB,)), dma((21,)), dma((8,)),
            dma((21,)), dma((8,)), dma((21,)), dma((8,)),
            dma((9,)), dma((9,)), dma((9,)), dma((9,)),
        ],
        compiler_params=pltpu.CompilerParams(collective_id=0, has_side_effects=True, vmem_limit_bytes=67043328),
    )(adj_rows, feat_rows.T, w_hidden, w_output.T, labels[None, :], train_mask[None, :], block_mask)
    return loss[0, 0], gwh, gwot.T


def solution(mesh):
    row_spec = P(AXIS_NAME, None)
    vec_spec = P(AXIS_NAME)
    return jax.shard_map(device_step, mesh=mesh, in_specs=(row_spec, row_spec, P(), P(), vec_spec, vec_spec, P()), out_specs=(P(), P(), P()), check_vma=False)
```

```python
import jax
import jax.numpy as jnp
from jax import lax
from jax.experimental import pallas as pl
from jax.experimental.pallas import tpu as pltpu
from jax.sharding import PartitionSpec as P

AXIS_NAME = 'nodes'
MESH = pl.DeviceIdType.MESH
F32, BF16 = jnp.float32, jnp.bfloat16
BLK = 1024
NB = 16
F_IN, F_PAD = 100, 104
HID = 128
CLS, CLS_PAD = 47, 48
QS = [0, 1, 2, 4, 3, 5, 6, 7]
QI = {q: i for i, q in enumerate(QS)}
ORDERS = [(1, 2, 4), (2, 4, 1), (4, 1, 2)]
X_CHUNKS = [(0, 40), (40, 32), (72, 32)]
Y_CHUNKS = [(0, 16), (16, 16), (32, 16)]
D1_CHUNKS = [(0, 48), (48, 40), (88, 40)]
GWO_HALF, GWH_HALF = 24, 56
OUT_ROWS = F_PAD + CLS_PAD
M_TILE = 256


def later_dims(q, k):
    order = ORDERS[k]
    return order[1 + max(order.index(d) for d in order if q & d):]


def last_dim(q, k):
    return max((d for d in ORDERS[k] if q & d), key=ORDERS[k].index)


def plan_gather(sizes, cost, max_group):
    link = {1: 0.0, 2: 0.0, 4: 0.0, 0: 0.0}
    ops, arrive, relayed, ready = [], {}, {}, [0]
    now = 0.0

    def send(table, key, dim, size):
        link[dim] = max(now, link[dim]) + size / (46.6 if dim else 600.0)
        table[key] = link[dim] + (2.3 if dim else 0.95)

    for j in range(3):
        for k in range(3):
            send(arrive, (ORDERS[k][j], k), ORDERS[k][j], sizes[k])
    send(relayed, 0, 0, sum(sizes))
    got = {q: 0 for q in range(8)}
    while arrive or relayed or ready:
        key = min(arrive, key=arrive.get, default=None)
        if key is not None and arrive[key] <= now:
            del arrive[key]
            q, k = key
            ops.append(('recv', q, k))
            for d in later_dims(q, k):
                send(arrive, (q | d, k), d, sizes[k])
            got[q] += 1
            if got[q] == 3:
                ops.append(('relay', q))
                send(relayed, q, 0, sum(sizes))
                ready.append(2 * QI[q])
            continue
        for q in sorted(relayed, key=relayed.get):
            if relayed[q] <= now:
                del relayed[q]
                ops.append(('take', q))
                ready.append(2 * QI[q] + 1)
        if ready:
            ops.append(('dot', ready[:max_group]))
            now += cost(len(ready[:max_group]))
            ready = ready[max_group:]
        else:
            now = min(list(arrive.values()) + list(relayed.values()))
    return ops


def dot_last(lhs, rhs):
    return lax.dot_general(lhs, rhs, (((1,), (1,)), ((), ())), preferred_element_type=F32)


def dot_first(lhs, rhs):
    return lax.dot_general(lhs, rhs, (((0,), (0,)), ((), ())), preferred_element_type=F32)


def step_kernel(adj_hbm, x_hbm, wh_hbm, wot_hbm, lab_hbm, msk_hbm, bm_hbm, out_ref,
                x_ref, wh_ref, wot_ref, lab_ref, msk_ref, bm_ref,
                adj, xall, yall, y1b, z1, z1t, z2, hid, gt, et, con, part2, part1, rb2, rb1, whs, wos, macc, lossv,
                gwos, gwop, gwor, gwog, gwof, gwhs, gwhp, gwhr, gwhg, gwhf,
                io_sem, a_sem, ici_send, d2d_send, recv_a, d2d_a, recv_b, d2d_b,
                gwo_send, gwo_recv, gwh_send, gwh_recv):
    me = lax.axis_index(AXIS_NAME)
    coords = [me % 2, (me // 2) % 2, (me // 4) % 2, me // 8]

    def dev(rel):
        total = 0
        for bit in range(4):
            total = total + ((coords[bit] + ((rel >> bit) & 1)) % 2) * (1 << bit)
        return total

    def rel_of(slot):
        return 2 * QS[slot // 2] + slot % 2

    def rcopy(src, dst, send_sem, recv_sem, rel):
        return pltpu.make_async_remote_copy(src_ref=src, dst_ref=dst, send_sem=send_sem, recv_sem=recv_sem,
                                            device_id=(dev(rel),), device_id_type=MESH)

    def a_copy(slot, blk=0):
        return pltpu.make_async_copy(adj_hbm.at[:, pl.ds(pl.multiple_of(blk * BLK, BLK), BLK)], adj.at[slot], a_sem.at[slot])

    plan1 = plan_gather([n * 2.048 for _, n in X_CHUNKS], lambda n: 0.2 + 0.54 * n, 2)
    a_order = [slot for op in plan1 if op[0] == 'dot' for slot in op[1]]

    def start_a(lo, hi):
        for slot in a_order[lo:hi]:
            a_copy(slot, dev(rel_of(slot))).start()

    loads = [pltpu.make_async_copy(src, dst, io_sem.at[n]) for n, (src, dst) in enumerate(
        [(x_hbm, x_ref), (wh_hbm, wh_ref), (wot_hbm, wot_ref), (lab_hbm, lab_ref), (msk_hbm, msk_ref), (bm_hbm, bm_ref)])]
    barrier = pltpu.get_barrier_semaphore()
    peers = [1] + [2 * q for q in range(1, 8)]
    for rel in peers:
        pl.semaphore_signal(barrier, inc=1, device_id=(dev(rel),), device_id_type=MESH)

    for load in loads:
        load.start()
    start_a(0, 6)
    macc[...] = jnp.zeros_like(macc)
    z1[...] = jnp.zeros_like(z1)
    z2[...] = jnp.zeros_like(z2)
    whs[...] = jnp.zeros_like(whs)
    wos[...] = jnp.zeros_like(wos)
    for load in loads:
        load.wait()
    xall[0, 0:F_PAD - 8, :] = x_ref[0:F_PAD - 8, :]
    xall[0, F_PAD - 8:F_PAD, :] = jnp.concatenate([x_ref[F_PAD - 8:F_IN, :], jnp.zeros((F_PAD - F_IN, BLK), BF16)], axis=0)
    whs[0:F_IN, :] = wh_ref[...].astype(BF16)
    wos[0:CLS, :] = wot_ref[...].astype(BF16)
    pl.semaphore_wait(barrier, len(peers))

    def mask_of(slot):
        if isinstance(slot, int):
            return bm_ref[me, dev(rel_of(slot))]
        i = slot // 2
        c = slot % 2
        bits = []
        for bit in (1, 2, 4):
            b = 0
            for pos, q in enumerate(QS):
                if q & bit:
                    d = (i - pos) * (i - pos)
                    b = b + 1 // (1 + d)
            bits.append(b)
        total = ((coords[0] + c) % 2)
        for n, b in enumerate(bits):
            total = total + ((coords[n + 1] + b) % 2) * (2 << n)
        return bm_ref[me, total]


    def gather_product(buf, chunks, recv, recv_d2d, ops, first, dots):
        def ici(src_q, dim, k):
            dst_q = src_q ^ dim
            lo, n = chunks[k]
            return rcopy(buf.at[2 * QI[src_q], pl.ds(lo, n), :], buf.at[2 * QI[dst_q], pl.ds(lo, n), :],
                         ici_send, recv.at[k * 7 + QI[dst_q] - 1], 2 * dim)

        def relay(q):
            return rcopy(buf.at[2 * QI[q]], buf.at[2 * QI[q] + 1], d2d_send, recv_d2d.at[QI[q]], 1)

        for j in range(3):
            for k in range(3):
                ici(0, ORDERS[k][j], k).start()
        relay(0).start()
        first()
        for op, q, *k in ops:
            if op == 'dot':
                dots(q)
            elif op == 'take':
                relay(q).wait_recv()
            elif op == 'relay':
                relay(q).start()
            else:
                d = last_dim(q, k[0])
                ici(q ^ d, d, k[0]).wait_recv()
                for d in later_dims(q, k[0]):
                    ici(q, d, k[0]).start()
        for count, sem, rel in ((7, ici_send, 2), (8, d2d_send, 1)):
            sent = buf.at[pl.ds(0, count)]
            rcopy(sent, sent, sem, recv.at[0], rel).wait_send()

    def accumulate(out, slots, blocks):
        for lo in range(0, BLK, M_TILE):
            acc = out[lo:lo + M_TILE, :]
            for slot, block in zip(slots, blocks):
                acc = acc + dot_last(adj[slot, lo:lo + M_TILE, :], block)
            out[lo:lo + M_TILE, :] = acc

    def dots1(slots):
        for slot in slots:
            a_copy(slot).wait()
        for j, slot in enumerate(slots):
            yt = dot_first(whs[...], xall[slot]).astype(BF16)
            y1b[j] = (yt.astype(F32) * mask_of(slot).astype(F32)).astype(BF16)
        accumulate(z1, slots, [y1b[j] for j in range(len(slots))])

    gather_product(xall, X_CHUNKS, recv_a, d2d_a, plan1, lambda: start_a(6, 16), dots1)

    cls_id = lax.broadcasted_iota(jnp.int32, (CLS_PAD, BLK), 0)
    weight = msk_ref[...].astype(F32)
    hid[...] = jnp.maximum(z1[...], 0.0).astype(BF16)
    yall[0] = jnp.where(cls_id == CLS, weight, dot_last(wos[...], hid[...])).astype(BF16)

    def dots2(slots):
        blocks = []
        for slot in slots:
            macc[...] += yall[slot, CLS_PAD - 16:CLS_PAD, :].astype(F32)
            blocks.append((yall[slot].astype(F32) * mask_of(slot).astype(F32)).astype(BF16))
        accumulate(z2, slots, blocks)

    def keep_sign():
        z1t[...] = jnp.transpose(z1[...])

    plan2 = plan_gather([n * 2.048 for _, n in Y_CHUNKS], lambda n: 0.13 + 0.54 * n, 2)
    gather_product(yall, Y_CHUNKS, recv_b, d2d_b, plan2, keep_sign, dots2)
    label_count = jnp.sum(macc[15:16, :])

    zt = jnp.transpose(z2[...])
    valid = cls_id < CLS
    top = jnp.max(jnp.where(valid, zt, -jnp.inf), axis=0, keepdims=True)
    expz = jnp.where(valid, jnp.exp(zt - top), 0.0)
    log_norm = jnp.log(jnp.sum(expz, axis=0, keepdims=True)) + top
    one_hot = cls_id == lab_ref[...]
    picked = jnp.sum(jnp.where(one_hot, zt, 0.0), axis=0, keepdims=True)
    loss_terms = weight * (log_norm - picked)
    acc = loss_terms[:, 0:128]
    for n in range(1, BLK // 128):
        acc = acc + loss_terms[:, 128 * n:128 * (n + 1)]
    lossv[...] = acc
    prob = jnp.exp(zt - log_norm)
    grad = (prob - one_hot.astype(F32)) * (weight / label_count)
    gt[...] = jnp.where(valid, grad, 0.0).astype(BF16)


    def reduce_pass(lhs_ref, rows, chunks, part, rb, recv, recv_d2d, early, hooks):
        def dim_of(q, k):
            return next(d for d in reversed(ORDERS[k]) if q & d)

        def ici(q, k):
            lo, n = chunks[k]
            idx = k * 7 + QI[q] - 1
            return rcopy(con.at[2 * QI[q], pl.ds(lo, n), :], rb.at[QI[q] - 1, pl.ds(lo, n), :], ici_send,
                         recv.at[idx], 2 * dim_of(q, k))

        def d2d(i):
            return rcopy(con.at[2 * i + 1, pl.ds(0, rows), :], part.at[i], d2d_send, recv_d2d.at[i], 1)

        def sources(q, k):
            out = []
            for d in reversed(ORDERS[k]):
                if q & d:
                    break
                out.append(q ^ d)
            return out

        def compute(slot):
            lhs = (lhs_ref[...].astype(F32) * mask_of(slot).astype(F32)).astype(BF16)
            con[slot, 0:rows, :] = jnp.dot(lhs, adj[slot], preferred_element_type=F32)

        waiting = {(q, k): set(sources(q, k)) for q in range(8) for k in range(3)}

        def pair_sum(q):
            i = QI[q]
            d2d(i).wait_recv()
            con[2 * i, 0:rows, :] += part[i]
            for k in range(3):
                if q and not waiting[q, k]:
                    ici(q, k).start()

        def take(src, k):
            d = dim_of(src, k)
            q = src ^ d
            lo, n = chunks[k]
            ici(src, k).wait_recv()
            con[2 * QI[q], lo:lo + n, :] += rb[QI[src] - 1, lo:lo + n, :]
            waiting[q, k].discard(src)
            if q and not waiting[q, k]:
                ici(q, k).start()

        def body(n, carry):
            i = 7 - n
            compute(2 * i + 1)
            d2d(i).start()
            compute(2 * i)
            for m in range(8):
                @pl.when(n == m)
                def _(m=m):
                    if m:
                        pair_sum(QS[8 - m])
                    for r in early.get(m, ()):
                        take_rank(r)
                    for hook in hooks.get(m, ()):
                        hook()
            return carry

        rank = {q: r for r, q in enumerate(reversed(QS))}
        taken = set()

        def sources_of(k, phase):
            d = ORDERS[k][2 - phase]
            later = [e for e in ORDERS[k][3 - phase:]]
            return sorted((q for q in range(1, 8) if q & d and not any(q & e for e in later)), key=rank.get)

        def take_rank(r, phase=0):
            for k in range(3):
                take(sources_of(k, phase)[r], k)
                taken.add((phase, r))

        lax.fori_loop(0, 8, body, 0)
        for r in range(4):
            if (0, r) not in taken:
                take_rank(r)
            if r == 2:
                for hook in hooks.get('mid', ()):
                    hook()
                pair_sum(0)
        take_rank(0, 1)
        take_rank(1, 1)
        for hook in hooks.get('late', ()):
            hook()
        take_rank(0, 2)
        for count, sem, rel in ((7, ici_send, 2), (8, d2d_send, 1)):
            sent = con.at[pl.ds(0, count), pl.ds(0, rows), :]
            rcopy(sent, sent, sem, recv.at[0], rel).wait_send()

    reduce_pass(gt, CLS_PAD, Y_CHUNKS, part2, rb2, recv_a, d2d_a, {6: [0], 7: [1]}, {})
    d2t = con[0, 0:CLS_PAD, :].astype(BF16)
    gwo = jnp.dot(d2t, hid[...], preferred_element_type=F32)
    et[...] = jnp.where(z1t[...] > 0, dot_first(wos[...], d2t), 0.0).astype(BF16)
    row_id = lax.broadcasted_iota(jnp.int32, (CLS_PAD, HID), 0)
    gwos[...] = jnp.where(row_id == CLS, lossv[...], gwo)

    core = coords[0]

    def all_sum(rows, total_rows, src, halves, other, own, gathered, final, send, recv):
        def prepare():
            halves[0] = src[0:rows, :]
            halves[1, 0:total_rows - rows, :] = src[rows:total_rows, :]
            if total_rows < 2 * rows:
                halves[1, total_rows - rows:rows, :] = jnp.zeros((2 * rows - total_rows, HID), F32)

        pair = rcopy(halves.at[1 - core], other, send.at[0], recv.at[0], 1)
        sends = [rcopy(gathered.at[0], gathered.at[q], send.at[1], recv.at[q], 2 * q) for q in range(1, 8)]
        back = rcopy(own, final, send.at[2], recv.at[8], 1)

        def start():
            prepare()
            pair.start()

        def spread():
            pair.wait()
            gathered[0] = halves[core] + other[...]
            for q in (7, 6, 5, 3, 4, 2, 1):
                sends[q - 1].start()

        def collect():
            for cp in sends:
                cp.wait_recv()
            rcopy(gathered.at[pl.ds(0, 7)], gathered.at[pl.ds(0, 7)], send.at[1], recv.at[0], 2).wait_send()
            g = gathered
            own[...] = ((g[0] + g[1]) + (g[2] + g[3])) + ((g[4] + g[5]) + (g[6] + g[7]))
            back.start()

        def finish():
            halves[core] = own[...]
            back.wait()
            halves[1 - core] = final[...]

        return start, spread, collect, finish

    gwo_start, gwo_spread, gwo_collect, gwo_finish = all_sum(GWO_HALF, CLS_PAD, gwos, gwop, gwof.at[0], gwor, gwog,
                                                             gwof.at[1], gwo_send, gwo_recv)
    gwh_start, gwh_spread, gwh_collect, gwh_finish = all_sum(GWH_HALF, F_PAD, gwhs, gwhp, gwhf.at[0], gwhr, gwhg,
                                                             gwhf.at[1], gwh_send, gwh_recv)
    gwo_start()

    def gwo_out():
        gwo_finish()
        out_ref[F_PAD:F_PAD + GWO_HALF, :] = gwop[0]
        out_ref[F_PAD + GWO_HALF:OUT_ROWS, :] = gwop[1]
        loss = jnp.sum(gwop[1, GWO_HALF - 1:GWO_HALF, :], axis=1, keepdims=True) / label_count
        out_ref[OUT_ROWS - 1:OUT_ROWS, :] = jnp.broadcast_to(loss, (1, HID))

    reduce_pass(et, HID, D1_CHUNKS, part1, rb1, recv_b, d2d_b, {},
                {0: [gwo_spread], 'mid': [gwo_collect], 'late': [gwo_out]})
    gwhs[...] = dot_last(xall[0], con[0].astype(BF16))
    gwh_start()
    gwh_spread()
    gwh_collect()
    gwh_finish()
    out_ref[0:GWH_HALF, :] = gwhp[0]
    out_ref[GWH_HALF:F_PAD, :] = gwhp[1, 0:F_PAD - GWH_HALF, :]


def split_kernel(sums_ref, gwh_ref, gwot_ref, loss_ref):
    gwh_ref[...] = sums_ref[0:F_IN, :]
    gwot_ref[...] = sums_ref[F_PAD:F_PAD + CLS, :]
    loss_ref[...] = sums_ref[OUT_ROWS - 1:OUT_ROWS, 0:1]


def device_step(adj_rows, feat_rows, w_hidden, w_output, labels, train_mask, block_mask):
    dma = pltpu.SemaphoreType.DMA
    vmem = pl.BlockSpec(memory_space=pltpu.VMEM)
    hbm = pl.BlockSpec(memory_space=pl.ANY)
    sums = pl.pallas_call(
        step_kernel,
        name='gcn_step',
        out_shape=jax.ShapeDtypeStruct((OUT_ROWS, HID), F32),
        in_specs=[hbm] * 7,
        out_specs=vmem,
        scratch_shapes=[
            pltpu.VMEM((F_IN, BLK), BF16),
            pltpu.VMEM((F_IN, HID), F32),
            pltpu.VMEM((CLS, HID), F32),
            pltpu.VMEM((1, BLK), jnp.int32),
            pltpu.VMEM((1, BLK), jnp.int32),
            pltpu.SMEM((NB, NB), jnp.int32),
            pltpu.VMEM((NB, BLK, BLK), BF16),
            pltpu.VMEM((NB, F_PAD, BLK), BF16),
            pltpu.VMEM((NB, CLS_PAD, BLK), BF16),
            pltpu.VMEM((2, HID, BLK), BF16),
            pltpu.VMEM((BLK, HID), F32),
            pltpu.VMEM((HID, BLK), F32),
            pltpu.VMEM((BLK, CLS_PAD), F32),
            pltpu.VMEM((BLK, HID), BF16),
            pltpu.VMEM((CLS_PAD, BLK), BF16),
            pltpu.VMEM((HID, BLK), BF16),
            pltpu.VMEM((NB, HID, BLK), F32),
            pltpu.VMEM((8, CLS_PAD, BLK), F32),
            pltpu.VMEM((8, HID, BLK), F32),
            pltpu.VMEM((7, CLS_PAD, BLK), F32),
            pltpu.VMEM((7, HID, BLK), F32),
            pltpu.VMEM((F_PAD, HID), BF16),
            pltpu.VMEM((CLS_PAD, HID), BF16),
            pltpu.VMEM((16, BLK), F32),
            pltpu.VMEM((1, 128), F32),
            pltpu.VMEM((CLS_PAD, HID), F32),
            pltpu.VMEM((2, GWO_HALF, HID), F32),
            pltpu.VMEM((GWO_HALF, HID), F32),
            pltpu.VMEM((8, GWO_HALF, HID), F32),
            pltpu.VMEM((2, GWO_HALF, HID), F32),
            pltpu.VMEM((F_PAD, HID), F32),
            pltpu.VMEM((2, GWH_HALF, HID), F32),
            pltpu.VMEM((GWH_HALF, HID), F32),
            pltpu.VMEM((8, GWH_HALF, HID), F32),
            pltpu.VMEM((2, GWH_HALF, HID), F32),
            dma((6,)), dma((NB,)), dma, dma, dma((21,)), dma((8,)), dma((21,)), dma((8,)),
            dma((3,)), dma((9,)), dma((3,)), dma((9,)),
        ],
        compiler_params=pltpu.CompilerParams(collective_id=0, has_side_effects=True, vmem_limit_bytes=67043328),
    )(adj_rows, feat_rows.T, w_hidden, w_output.T, labels[None, :], train_mask[None, :], block_mask)
    gwh, gwot, loss = pl.pallas_call(
        split_kernel,
        name='split_sums',
        out_shape=(jax.ShapeDtypeStruct((F_IN, HID), F32), jax.ShapeDtypeStruct((CLS, HID), F32),
                   jax.ShapeDtypeStruct((1, 1), F32)),
        in_specs=[vmem],
        out_specs=(vmem, vmem, vmem),
    )(sums)
    return loss[0, 0], gwh, gwot.T


def solution(mesh):
    row_spec = P(AXIS_NAME, None)
    vec_spec = P(AXIS_NAME)
    return jax.shard_map(device_step, mesh=mesh, in_specs=(row_spec, row_spec, P(), P(), vec_spec, vec_spec, P()), out_specs=(P(), P(), P()), check_vma=False)
```

```python
import jax
import jax.numpy as jnp
from jax import lax
from jax.experimental import pallas as pl
from jax.experimental.pallas import tpu as pltpu
from jax.sharding import PartitionSpec as P

AXIS_NAME = 'nodes'
MESH = pl.DeviceIdType.MESH
F32, BF16 = jnp.float32, jnp.bfloat16
BLK = 1024
NB = 16
F_IN, F_PAD = 100, 104
HID = 128
CLS, CLS_PAD = 47, 48
QS = [0, 1, 2, 4, 3, 5, 6, 7]
QI = {q: i for i, q in enumerate(QS)}
ORDERS = [(1, 2, 4), (2, 4, 1), (4, 1, 2)]
X_CHUNKS = [(0, 40), (40, 32), (72, 32)]
Y_CHUNKS = [(0, 16), (16, 16), (32, 16)]
D2_CHUNKS = [(lo, n, 0, BLK, k) for k, (lo, n) in enumerate(Y_CHUNKS)]
D1_CHUNKS = [(0, 40, 0, BLK, 0), (40, 40, 0, BLK, 1), (80, 40, 0, BLK, 2),
             (120, 8, 0, 384, 0), (120, 8, 384, 384, 1), (120, 8, 768, 256, 2)]
GWO_HALF, GWH_HALF = 24, 56
OUT_ROWS = F_PAD + CLS_PAD
M_TILE = 256
A_AHEAD = 5


def later_dims(q, k):
    order = ORDERS[k]
    return order[1 + max(order.index(d) for d in order if q & d):]


def last_dim(q, k):
    return max((d for d in ORDERS[k] if q & d), key=ORDERS[k].index)


def plan_gather(sizes, cost, max_group):
    link = {1: 0.0, 2: 0.0, 4: 0.0, 0: 0.0}
    ops, arrive, relayed, ready = [], {}, {}, [0]
    now = 0.0

    def send(table, key, dim, size):
        link[dim] = max(now, link[dim]) + size / (46.6 if dim else 600.0)
        table[key] = link[dim] + (2.3 if dim else 0.95)

    for j in range(3):
        for k in range(3):
            send(arrive, (ORDERS[k][j], k), ORDERS[k][j], sizes[k])
    send(relayed, 0, 0, sum(sizes))
    got = {q: 0 for q in range(8)}
    while arrive or relayed or ready:
        key = min(arrive, key=arrive.get, default=None)
        if key is not None and arrive[key] <= now:
            del arrive[key]
            q, k = key
            ops.append(('recv', q, k))
            for d in later_dims(q, k):
                send(arrive, (q | d, k), d, sizes[k])
            got[q] += 1
            if got[q] == 3:
                ops.append(('relay', q))
                send(relayed, q, 0, sum(sizes))
                ready.append(2 * QI[q])
            continue
        for q in sorted(relayed, key=relayed.get):
            if relayed[q] <= now:
                del relayed[q]
                ops.append(('take', q))
                ready.append(2 * QI[q] + 1)
        if ready:
            ops.append(('dot', ready[:max_group]))
            now += cost(len(ready[:max_group]))
            ready = ready[max_group:]
        else:
            now = min(list(arrive.values()) + list(relayed.values()))
    return ops


def dot_last(lhs, rhs):
    return lax.dot_general(lhs, rhs, (((1,), (1,)), ((), ())), preferred_element_type=F32)


def dot_first(lhs, rhs):
    return lax.dot_general(lhs, rhs, (((0,), (0,)), ((), ())), preferred_element_type=F32)


def step_kernel(adj_hbm, x_hbm, wh_hbm, wot_hbm, lab_hbm, msk_hbm, bm_hbm, out_ref,
                x_ref, wh_ref, wot_ref, lab_ref, msk_ref, bm_ref,
                adj, xall, yall, y1b, z1, z1t, z2, hid, gt, et, con, part2, part1, rb2, rb1, whs, wos, macc, lossv,
                gwos, gwop, gwor, gwog, gwof, gwhs, gwhp, gwhr, gwhg, gwhf,
                io_sem, a_sem, ici_send, d2d_send, recv_a, d2d_a, recv_b, d2d_b,
                gwo_send, gwo_recv, gwh_send, gwh_recv):
    me = lax.axis_index(AXIS_NAME)
    coords = [me % 2, (me // 2) % 2, (me // 4) % 2, me // 8]

    def dev(rel):
        total = 0
        for bit in range(4):
            total = total + ((coords[bit] + ((rel >> bit) & 1)) % 2) * (1 << bit)
        return total

    def rel_of(slot):
        return 2 * QS[slot // 2] + slot % 2

    def rcopy(src, dst, send_sem, recv_sem, rel):
        return pltpu.make_async_remote_copy(src_ref=src, dst_ref=dst, send_sem=send_sem, recv_sem=recv_sem,
                                            device_id=(dev(rel),), device_id_type=MESH)

    def a_copy(slot, blk=0):
        return pltpu.make_async_copy(adj_hbm.at[:, pl.ds(pl.multiple_of(blk * BLK, BLK), BLK)], adj.at[slot], a_sem.at[slot])

    plan1 = plan_gather([n * 2.048 for _, n in X_CHUNKS], lambda n: 0.2 + 0.54 * n, 2)
    a_order = [slot for op in plan1 if op[0] == 'dot' for slot in op[1]]

    def start_a(lo, hi):
        for slot in a_order[lo:hi]:
            a_copy(slot, dev(rel_of(slot))).start()

    loads = [pltpu.make_async_copy(src, dst, io_sem.at[n]) for n, (src, dst) in enumerate(
        [(x_hbm, x_ref), (wh_hbm, wh_ref), (wot_hbm, wot_ref), (lab_hbm, lab_ref), (msk_hbm, msk_ref), (bm_hbm, bm_ref)])]
    barrier = pltpu.get_barrier_semaphore()
    peers = [1, 2, 4, 8]
    for rel in peers:
        pl.semaphore_signal(barrier, inc=1, device_id=(dev(rel),), device_id_type=MESH)

    for load in loads:
        load.start()
    start_a(0, A_AHEAD)
    macc[...] = jnp.zeros_like(macc)
    z1[...] = jnp.zeros_like(z1)
    z2[...] = jnp.zeros_like(z2)
    whs[...] = jnp.zeros_like(whs)
    wos[...] = jnp.zeros_like(wos)
    for load in loads:
        load.wait()
    xall[0, 0:F_PAD - 8, :] = x_ref[0:F_PAD - 8, :]
    xall[0, F_PAD - 8:F_PAD, :] = jnp.concatenate([x_ref[F_PAD - 8:F_IN, :], jnp.zeros((F_PAD - F_IN, BLK), BF16)], axis=0)
    whs[0:F_IN, :] = wh_ref[...].astype(BF16)
    wos[0:CLS, :] = wot_ref[...].astype(BF16)
    pl.semaphore_wait(barrier, len(peers))

    def mask_of(slot):
        if isinstance(slot, int):
            return bm_ref[me, dev(rel_of(slot))]
        i = slot // 2
        c = slot % 2
        bits = []
        for bit in (1, 2, 4):
            b = 0
            for pos, q in enumerate(QS):
                if q & bit:
                    d = (i - pos) * (i - pos)
                    b = b + 1 // (1 + d)
            bits.append(b)
        total = ((coords[0] + c) % 2)
        for n, b in enumerate(bits):
            total = total + ((coords[n + 1] + b) % 2) * (2 << n)
        return bm_ref[me, total]


    def gather_product(buf, chunks, recv, recv_d2d, ops, first, dots):
        def ici(src_q, dim, k):
            dst_q = src_q ^ dim
            lo, n = chunks[k]
            return rcopy(buf.at[2 * QI[src_q], pl.ds(lo, n), :], buf.at[2 * QI[dst_q], pl.ds(lo, n), :],
                         ici_send, recv.at[k * 7 + QI[dst_q] - 1], 2 * dim)

        def relay(q):
            return rcopy(buf.at[2 * QI[q]], buf.at[2 * QI[q] + 1], d2d_send, recv_d2d.at[QI[q]], 1)

        for j in range(3):
            for k in range(3):
                ici(0, ORDERS[k][j], k).start()
        relay(0).start()
        first()
        for op, q, *k in ops:
            if op == 'dot':
                dots(q)
            elif op == 'take':
                relay(q).wait_recv()
            elif op == 'relay':
                relay(q).start()
            else:
                d = last_dim(q, k[0])
                ici(q ^ d, d, k[0]).wait_recv()
                for d in later_dims(q, k[0]):
                    ici(q, d, k[0]).start()
        for count, sem, rel in ((7, ici_send, 2), (8, d2d_send, 1)):
            sent = buf.at[pl.ds(0, count)]
            rcopy(sent, sent, sem, recv.at[0], rel).wait_send()

    def accumulate(out, slots, blocks):
        for lo in range(0, BLK, M_TILE):
            acc = out[lo:lo + M_TILE, :]
            for slot, block in zip(slots, blocks):
                acc = acc + dot_last(adj[slot, lo:lo + M_TILE, :], block)
            out[lo:lo + M_TILE, :] = acc

    def dots1(slots):
        for slot in slots:
            a_copy(slot).wait()
            ahead = a_order.index(slot) + A_AHEAD
            start_a(ahead, ahead + 1)
        for j, slot in enumerate(slots):
            yt = dot_first(whs[...], xall[slot]).astype(BF16)
            y1b[j] = (yt.astype(F32) * mask_of(slot).astype(F32)).astype(BF16)
        accumulate(z1, slots, [y1b[j] for j in range(len(slots))])

    gather_product(xall, X_CHUNKS, recv_a, d2d_a, plan1, lambda: None, dots1)

    cls_id = lax.broadcasted_iota(jnp.int32, (CLS_PAD, BLK), 0)
    weight = msk_ref[...].astype(F32)
    hid[...] = jnp.maximum(z1[...], 0.0).astype(BF16)
    yall[0] = jnp.where(cls_id == CLS, weight, dot_last(wos[...], hid[...])).astype(BF16)

    def dots2(slots):
        blocks = []
        for slot in slots:
            macc[...] += yall[slot, CLS_PAD - 16:CLS_PAD, :].astype(F32)
            blocks.append((yall[slot].astype(F32) * mask_of(slot).astype(F32)).astype(BF16))
        accumulate(z2, slots, blocks)

    def keep_sign():
        z1t[...] = jnp.transpose(z1[...])

    plan2 = plan_gather([n * 2.048 for _, n in Y_CHUNKS], lambda n: 0.13 + 0.54 * n, 2)
    gather_product(yall, Y_CHUNKS, recv_b, d2d_b, plan2, keep_sign, dots2)
    label_count = jnp.sum(macc[15:16, :])

    zt = jnp.transpose(z2[...])
    valid = cls_id < CLS
    top = jnp.max(jnp.where(valid, zt, -jnp.inf), axis=0, keepdims=True)
    expz = jnp.where(valid, jnp.exp(zt - top), 0.0)
    log_norm = jnp.log(jnp.sum(expz, axis=0, keepdims=True)) + top
    one_hot = cls_id == lab_ref[...]
    picked = jnp.sum(jnp.where(one_hot, zt, 0.0), axis=0, keepdims=True)
    loss_terms = weight * (log_norm - picked)
    acc = loss_terms[:, 0:128]
    for n in range(1, BLK // 128):
        acc = acc + loss_terms[:, 128 * n:128 * (n + 1)]
    lossv[...] = acc
    prob = jnp.exp(zt - log_norm)
    grad = (prob - one_hot.astype(F32)) * (weight / label_count)
    gt[...] = jnp.where(valid, grad, 0.0).astype(BF16)


    def reduce_pass(lhs_ref, rows, chunks, part, rb, recv, recv_d2d, early, hooks):
        parts = range(len(chunks))

        def order_of(k):
            return ORDERS[chunks[k][4]]

        def dim_of(q, k):
            return next(d for d in reversed(order_of(k)) if q & d)

        def ici(q, k):
            lo, n, lane, lanes, _ = chunks[k]
            idx = k * 7 + QI[q] - 1
            return rcopy(con.at[2 * QI[q], pl.ds(lo, n), pl.ds(lane, lanes)],
                         rb.at[QI[q] - 1, pl.ds(lo, n), pl.ds(lane, lanes)], ici_send,
                         recv.at[idx], 2 * dim_of(q, k))

        def d2d(i):
            return rcopy(con.at[2 * i + 1, pl.ds(0, rows), :], part.at[i], d2d_send, recv_d2d.at[i], 1)

        def sources(q, k):
            out = []
            for d in reversed(order_of(k)):
                if q & d:
                    break
                out.append(q ^ d)
            return out

        def compute(slot):
            lhs = (lhs_ref[...].astype(F32) * mask_of(slot).astype(F32)).astype(BF16)
            con[slot, 0:rows, :] = jnp.dot(lhs, adj[slot], preferred_element_type=F32)

        waiting = {(q, k): set(sources(q, k)) for q in range(8) for k in parts}

        def pair_sum(q):
            i = QI[q]
            d2d(i).wait_recv()
            con[2 * i, 0:rows, :] += part[i]
            for k in parts:
                if q and not waiting[q, k]:
                    ici(q, k).start()

        def take(src, k):
            d = dim_of(src, k)
            q = src ^ d
            lo, n, lane, lanes, _ = chunks[k]
            ici(src, k).wait_recv()
            con[2 * QI[q], lo:lo + n, lane:lane + lanes] += rb[QI[src] - 1, lo:lo + n, lane:lane + lanes]
            waiting[q, k].discard(src)
            if q and not waiting[q, k]:
                ici(q, k).start()

        def body(n, carry):
            i = 7 - n
            compute(2 * i + 1)
            d2d(i).start()
            compute(2 * i)
            for m in range(8):
                @pl.when(n == m)
                def _(m=m):
                    if m:
                        pair_sum(QS[8 - m])
                    for r in early.get(m, ()):
                        take_rank(r)
                    for hook in hooks.get(m, ()):
                        hook()
            return carry

        rank = {q: r for r, q in enumerate(reversed(QS))}
        taken = set()

        def sources_of(k, phase):
            d = order_of(k)[2 - phase]
            later = order_of(k)[3 - phase:]
            return sorted((q for q in range(1, 8) if q & d and not any(q & e for e in later)), key=rank.get)

        def take_rank(r, phase=0):
            for k in parts:
                take(sources_of(k, phase)[r], k)
                taken.add((phase, r))

        lax.fori_loop(0, 8, body, 0)
        for r in range(4):
            if (0, r) not in taken:
                take_rank(r)
            if r == 2:
                for hook in hooks.get('mid', ()):
                    hook()
                pair_sum(0)
        take_rank(0, 1)
        take_rank(1, 1)
        for hook in hooks.get('late', ()):
            hook()
        take_rank(0, 2)
        for count, sem, rel in ((7, ici_send, 2), (8, d2d_send, 1)):
            sent = con.at[pl.ds(0, count), pl.ds(0, rows), :]
            rcopy(sent, sent, sem, recv.at[0], rel).wait_send()

    reduce_pass(gt, CLS_PAD, D2_CHUNKS, part2, rb2, recv_a, d2d_a, {6: [0], 7: [1]}, {})
    d2t = con[0, 0:CLS_PAD, :].astype(BF16)
    gwo = jnp.dot(d2t, hid[...], preferred_element_type=F32)
    et[...] = jnp.where(z1t[...] > 0, dot_first(wos[...], d2t), 0.0).astype(BF16)
    row_id = lax.broadcasted_iota(jnp.int32, (CLS_PAD, HID), 0)
    gwos[...] = jnp.where(row_id == CLS, lossv[...], gwo)

    core = coords[0]

    def all_sum(rows, total_rows, src, halves, other, own, gathered, final, send, recv):
        def prepare():
            halves[0] = src[0:rows, :]
            halves[1, 0:total_rows - rows, :] = src[rows:total_rows, :]
            if total_rows < 2 * rows:
                halves[1, total_rows - rows:rows, :] = jnp.zeros((2 * rows - total_rows, HID), F32)

        pair = rcopy(halves.at[1 - core], other, send.at[0], recv.at[0], 1)
        sends = [rcopy(gathered.at[0], gathered.at[q], send.at[1], recv.at[q], 2 * q) for q in range(1, 8)]
        back = rcopy(own, final, send.at[2], recv.at[8], 1)

        def start():
            prepare()
            pair.start()

        def spread():
            pair.wait()
            gathered[0] = halves[core] + other[...]
            for q in (7, 6, 5, 3, 4, 2, 1):
                sends[q - 1].start()

        def collect():
            for cp in sends:
                cp.wait_recv()
            rcopy(gathered.at[pl.ds(0, 7)], gathered.at[pl.ds(0, 7)], send.at[1], recv.at[0], 2).wait_send()
            g = gathered
            own[...] = ((g[0] + g[1]) + (g[2] + g[3])) + ((g[4] + g[5]) + (g[6] + g[7]))
            back.start()

        def finish():
            halves[core] = own[...]
            back.wait()
            halves[1 - core] = final[...]

        return start, spread, collect, finish

    gwo_start, gwo_spread, gwo_collect, gwo_finish = all_sum(GWO_HALF, CLS_PAD, gwos, gwop, gwof.at[0], gwor, gwog,
                                                             gwof.at[1], gwo_send, gwo_recv)
    gwh_start, gwh_spread, gwh_collect, gwh_finish = all_sum(GWH_HALF, F_PAD, gwhs, gwhp, gwhf.at[0], gwhr, gwhg,
                                                             gwhf.at[1], gwh_send, gwh_recv)
    gwo_start()

    def gwo_out():
        gwo_finish()
        out_ref[F_PAD:F_PAD + GWO_HALF, :] = gwop[0]
        out_ref[F_PAD + GWO_HALF:OUT_ROWS, :] = gwop[1]
        loss = jnp.sum(gwop[1, GWO_HALF - 1:GWO_HALF, :], axis=1, keepdims=True) / label_count
        out_ref[OUT_ROWS - 1:OUT_ROWS, :] = jnp.broadcast_to(loss, (1, HID))

    reduce_pass(et, HID, D1_CHUNKS, part1, rb1, recv_b, d2d_b, {},
                {0: [gwo_spread], 'mid': [gwo_collect], 'late': [gwo_out]})
    gwhs[...] = dot_last(xall[0], con[0].astype(BF16))
    gwh_start()
    gwh_spread()
    gwh_collect()
    gwh_finish()
    out_ref[0:GWH_HALF, :] = gwhp[0]
    out_ref[GWH_HALF:F_PAD, :] = gwhp[1, 0:F_PAD - GWH_HALF, :]


def split_kernel(sums_ref, gwh_ref, gwot_ref, loss_ref):
    gwh_ref[...] = sums_ref[0:F_IN, :]
    gwot_ref[...] = sums_ref[F_PAD:F_PAD + CLS, :]
    loss_ref[...] = sums_ref[OUT_ROWS - 1:OUT_ROWS, 0:1]


def device_step(adj_rows, feat_rows, w_hidden, w_output, labels, train_mask, block_mask):
    dma = pltpu.SemaphoreType.DMA
    vmem = pl.BlockSpec(memory_space=pltpu.VMEM)
    hbm = pl.BlockSpec(memory_space=pl.ANY)
    sums = pl.pallas_call(
        step_kernel,
        name='gcn_step',
        out_shape=jax.ShapeDtypeStruct((OUT_ROWS, HID), F32),
        in_specs=[hbm] * 7,
        out_specs=vmem,
        scratch_shapes=[
            pltpu.VMEM((F_IN, BLK), BF16),
            pltpu.VMEM((F_IN, HID), F32),
            pltpu.VMEM((CLS, HID), F32),
            pltpu.VMEM((1, BLK), jnp.int32),
            pltpu.VMEM((1, BLK), jnp.int32),
            pltpu.SMEM((NB, NB), jnp.int32),
            pltpu.VMEM((NB, BLK, BLK), BF16),
            pltpu.VMEM((NB, F_PAD, BLK), BF16),
            pltpu.VMEM((NB, CLS_PAD, BLK), BF16),
            pltpu.VMEM((2, HID, BLK), BF16),
            pltpu.VMEM((BLK, HID), F32),
            pltpu.VMEM((HID, BLK), F32),
            pltpu.VMEM((BLK, CLS_PAD), F32),
            pltpu.VMEM((BLK, HID), BF16),
            pltpu.VMEM((CLS_PAD, BLK), BF16),
            pltpu.VMEM((HID, BLK), BF16),
            pltpu.VMEM((NB, HID, BLK), F32),
            pltpu.VMEM((8, CLS_PAD, BLK), F32),
            pltpu.VMEM((8, HID, BLK), F32),
            pltpu.VMEM((7, CLS_PAD, BLK), F32),
            pltpu.VMEM((7, HID, BLK), F32),
            pltpu.VMEM((F_PAD, HID), BF16),
            pltpu.VMEM((CLS_PAD, HID), BF16),
            pltpu.VMEM((16, BLK), F32),
            pltpu.VMEM((1, 128), F32),
            pltpu.VMEM((CLS_PAD, HID), F32),
            pltpu.VMEM((2, GWO_HALF, HID), F32),
            pltpu.VMEM((GWO_HALF, HID), F32),
            pltpu.VMEM((8, GWO_HALF, HID), F32),
            pltpu.VMEM((2, GWO_HALF, HID), F32),
            pltpu.VMEM((F_PAD, HID), F32),
            pltpu.VMEM((2, GWH_HALF, HID), F32),
            pltpu.VMEM((GWH_HALF, HID), F32),
            pltpu.VMEM((8, GWH_HALF, HID), F32),
            pltpu.VMEM((2, GWH_HALF, HID), F32),
            dma((6,)), dma((NB,)), dma, dma, dma((21,)), dma((8,)), dma((42,)), dma((8,)),
            dma((3,)), dma((9,)), dma((3,)), dma((9,)),
        ],
        compiler_params=pltpu.CompilerParams(collective_id=0, has_side_effects=True, vmem_limit_bytes=67043328),
    )(adj_rows, feat_rows.T, w_hidden, w_output.T, labels[None, :], train_mask[None, :], block_mask)
    gwh, gwot, loss = pl.pallas_call(
        split_kernel,
        name='split_sums',
        out_shape=(jax.ShapeDtypeStruct((F_IN, HID), F32), jax.ShapeDtypeStruct((CLS, HID), F32),
                   jax.ShapeDtypeStruct((1, 1), F32)),
        in_specs=[vmem],
        out_specs=(vmem, vmem, vmem),
    )(sums)
    return loss[0, 0], gwh, gwot.T


def solution(mesh):
    row_spec = P(AXIS_NAME, None)
    vec_spec = P(AXIS_NAME)
    return jax.shard_map(device_step, mesh=mesh, in_specs=(row_spec, row_spec, P(), P(), vec_spec, vec_spec, P()), out_specs=(P(), P(), P()), check_vma=False)
```

```python
import jax
import jax.numpy as jnp
from jax import lax
from jax.experimental import pallas as pl
from jax.experimental.pallas import tpu as pltpu
from jax.sharding import PartitionSpec as P

AXIS_NAME = 'nodes'
MESH = pl.DeviceIdType.MESH
F32, BF16 = jnp.float32, jnp.bfloat16
BLK = 1024
NB = 16
F_IN, F_PAD = 100, 104
HID = 128
CLS, CLS_PAD = 47, 48
QS = [0, 1, 2, 4, 3, 5, 6, 7]
QI = {q: i for i, q in enumerate(QS)}
ORDERS = [(1, 2, 4), (2, 4, 1), (4, 1, 2)]
X_CHUNKS = [(0, 40), (40, 32), (72, 32)]
Y_CHUNKS = [(0, 16), (16, 16), (32, 16)]
D2_CHUNKS = [(lo, n, 0, BLK, k) for k, (lo, n) in enumerate(Y_CHUNKS)]
D1_CHUNKS = [(0, 40, 0, BLK, 0), (40, 40, 0, BLK, 1), (80, 40, 0, BLK, 2),
             (120, 8, 0, 384, 0), (120, 8, 384, 384, 1), (120, 8, 768, 256, 2)]
GWO_HALF, GWH_HALF = 24, 56
OUT_ROWS = F_PAD + CLS_PAD
M_TILE = 256
A_AHEAD = 5


def forwards(q, k):
    first, second, third = ORDERS[k]
    if k == 2 and q == first:
        return [(first, second)]
    if k == 2 and q == second:
        return [(second, third), (first, third)]
    order = ORDERS[k]
    return [(q, d) for d in order[1 + max(order.index(d) for d in order if q & d):]]


def last_dim(q, k):
    return max((d for d in ORDERS[k] if q & d), key=ORDERS[k].index)


def plan_gather(sizes, cost, max_group):
    link = {1: 0.0, 2: 0.0, 4: 0.0, 0: 0.0}
    ops, arrive, relayed, ready = [], {}, {}, [0]
    now = 0.0

    def send(table, key, dim, size):
        link[dim] = max(now, link[dim]) + size / (46.6 if dim else 600.0)
        table[key] = link[dim] + (2.3 if dim else 0.95)

    for j in range(3):
        for k in range(3):
            send(arrive, (ORDERS[k][j], k), ORDERS[k][j], sizes[k])
    send(relayed, 0, 0, sum(sizes))
    got = {q: 0 for q in range(8)}
    while arrive or relayed or ready:
        key = min(arrive, key=arrive.get, default=None)
        if key is not None and arrive[key] <= now:
            del arrive[key]
            q, k = key
            ops.append(('recv', q, k))
            for src, d in forwards(q, k):
                send(arrive, (src | d, k), d, sizes[k])
            got[q] += 1
            if got[q] == 3:
                ops.append(('relay', q))
                send(relayed, q, 0, sum(sizes))
                ready.append(2 * QI[q])
            continue
        for q in sorted(relayed, key=relayed.get):
            if relayed[q] <= now:
                del relayed[q]
                ops.append(('take', q))
                ready.append(2 * QI[q] + 1)
        if ready:
            ops.append(('dot', ready[:max_group]))
            now += cost(len(ready[:max_group]))
            ready = ready[max_group:]
        else:
            now = min(list(arrive.values()) + list(relayed.values()))
    return ops


def dot_last(lhs, rhs):
    return lax.dot_general(lhs, rhs, (((1,), (1,)), ((), ())), preferred_element_type=F32)


def dot_first(lhs, rhs):
    return lax.dot_general(lhs, rhs, (((0,), (0,)), ((), ())), preferred_element_type=F32)


def step_kernel(adj_hbm, x_hbm, wh_hbm, wot_hbm, lab_hbm, msk_hbm, bm_hbm, out_ref,
                x_ref, wh_ref, wot_ref, lab_ref, msk_ref, bm_ref,
                adj, xall, yall, y1b, z1, z1t, z2, hid, gt, et, con, part2, part1, rb2, rb1, whs, wos, macc, lossv,
                gwos, gwop, gwor, gwog, gwof, gwhs, gwhp, gwhr, gwhg, gwhf,
                io_sem, a_sem, ici_send, d2d_send, recv_a, d2d_a, recv_b, d2d_b,
                gwo_send, gwo_recv, gwh_send, gwh_recv):
    me = lax.axis_index(AXIS_NAME)
    coords = [me % 2, (me // 2) % 2, (me // 4) % 2, me // 8]

    def dev(rel):
        total = 0
        for bit in range(4):
            total = total + ((coords[bit] + ((rel >> bit) & 1)) % 2) * (1 << bit)
        return total

    def rel_of(slot):
        return 2 * QS[slot // 2] + slot % 2

    def rcopy(src, dst, send_sem, recv_sem, rel):
        return pltpu.make_async_remote_copy(src_ref=src, dst_ref=dst, send_sem=send_sem, recv_sem=recv_sem,
                                            device_id=(dev(rel),), device_id_type=MESH)

    def a_copy(slot, blk=0):
        return pltpu.make_async_copy(adj_hbm.at[:, pl.ds(pl.multiple_of(blk * BLK, BLK), BLK)], adj.at[slot], a_sem.at[slot])

    plan1 = plan_gather([n * 2.048 for _, n in X_CHUNKS], lambda n: 0.2 + 0.54 * n, 2)
    a_order = [slot for op in plan1 if op[0] == 'dot' for slot in op[1]]

    def start_a(lo, hi):
        for slot in a_order[lo:hi]:
            a_copy(slot, dev(rel_of(slot))).start()

    loads = [pltpu.make_async_copy(src, dst, io_sem.at[n]) for n, (src, dst) in enumerate(
        [(x_hbm, x_ref), (wh_hbm, wh_ref), (wot_hbm, wot_ref), (lab_hbm, lab_ref), (msk_hbm, msk_ref), (bm_hbm, bm_ref)])]
    barrier = pltpu.get_barrier_semaphore()
    peers = [1, 2, 4, 8]
    for rel in peers:
        pl.semaphore_signal(barrier, inc=1, device_id=(dev(rel),), device_id_type=MESH)

    for load in loads:
        load.start()
    start_a(0, A_AHEAD)
    macc[...] = jnp.zeros_like(macc)
    z1[...] = jnp.zeros_like(z1)
    z2[...] = jnp.zeros_like(z2)
    whs[...] = jnp.zeros_like(whs)
    wos[...] = jnp.zeros_like(wos)
    for load in loads:
        load.wait()
    xall[0, 0:F_PAD - 8, :] = x_ref[0:F_PAD - 8, :]
    xall[0, F_PAD - 8:F_PAD, :] = jnp.concatenate([x_ref[F_PAD - 8:F_IN, :], jnp.zeros((F_PAD - F_IN, BLK), BF16)], axis=0)
    whs[0:F_IN, :] = wh_ref[...].astype(BF16)
    wos[0:CLS, :] = wot_ref[...].astype(BF16)
    pl.semaphore_wait(barrier, len(peers))

    def mask_of(slot):
        if isinstance(slot, int):
            return bm_ref[me, dev(rel_of(slot))]
        i = slot // 2
        c = slot % 2
        bits = []
        for bit in (1, 2, 4):
            b = 0
            for pos, q in enumerate(QS):
                if q & bit:
                    d = (i - pos) * (i - pos)
                    b = b + 1 // (1 + d)
            bits.append(b)
        total = ((coords[0] + c) % 2)
        for n, b in enumerate(bits):
            total = total + ((coords[n + 1] + b) % 2) * (2 << n)
        return bm_ref[me, total]


    def gather_product(buf, chunks, recv, recv_d2d, ops, first, dots):
        def ici(src_q, dim, k):
            dst_q = src_q ^ dim
            lo, n = chunks[k]
            return rcopy(buf.at[2 * QI[src_q], pl.ds(lo, n), :], buf.at[2 * QI[dst_q], pl.ds(lo, n), :],
                         ici_send, recv.at[k * 7 + QI[dst_q] - 1], 2 * dim)

        def relay(q):
            return rcopy(buf.at[2 * QI[q]], buf.at[2 * QI[q] + 1], d2d_send, recv_d2d.at[QI[q]], 1)

        for j in range(3):
            for k in range(3):
                ici(0, ORDERS[k][j], k).start()
        relay(0).start()
        first()
        for op, q, *k in ops:
            if op == 'dot':
                dots(q)
            elif op == 'take':
                relay(q).wait_recv()
            elif op == 'relay':
                relay(q).start()
            else:
                d = last_dim(q, k[0])
                ici(q ^ d, d, k[0]).wait_recv()
                for src, d in forwards(q, k[0]):
                    ici(src, d, k[0]).start()
        for count, sem, rel in ((7, ici_send, 2), (8, d2d_send, 1)):
            sent = buf.at[pl.ds(0, count)]
            rcopy(sent, sent, sem, recv.at[0], rel).wait_send()

    def accumulate(out, slots, blocks):
        for lo in range(0, BLK, M_TILE):
            acc = out[lo:lo + M_TILE, :]
            for slot, block in zip(slots, blocks):
                acc = acc + dot_last(adj[slot, lo:lo + M_TILE, :], block)
            out[lo:lo + M_TILE, :] = acc

    def dots1(slots):
        for slot in slots:
            a_copy(slot).wait()
            ahead = a_order.index(slot) + A_AHEAD
            start_a(ahead, ahead + 1)
        for j, slot in enumerate(slots):
            yt = dot_first(whs[...], xall[slot]).astype(BF16)
            y1b[j] = (yt.astype(F32) * mask_of(slot).astype(F32)).astype(BF16)
        accumulate(z1, slots, [y1b[j] for j in range(len(slots))])

    gather_product(xall, X_CHUNKS, recv_a, d2d_a, plan1, lambda: None, dots1)

    cls_id = lax.broadcasted_iota(jnp.int32, (CLS_PAD, BLK), 0)
    weight = msk_ref[...].astype(F32)
    hid[...] = jnp.maximum(z1[...], 0.0).astype(BF16)
    yall[0] = jnp.where(cls_id == CLS, weight, dot_last(wos[...], hid[...])).astype(BF16)

    def dots2(slots):
        blocks = []
        for slot in slots:
            macc[...] += yall[slot, CLS_PAD - 16:CLS_PAD, :].astype(F32)
            blocks.append((yall[slot].astype(F32) * mask_of(slot).astype(F32)).astype(BF16))
        accumulate(z2, slots, blocks)

    def keep_sign():
        z1t[...] = jnp.transpose(z1[...])

    plan2 = plan_gather([n * 2.048 for _, n in Y_CHUNKS], lambda n: 0.13 + 0.54 * n, 2)
    gather_product(yall, Y_CHUNKS, recv_b, d2d_b, plan2, keep_sign, dots2)
    label_count = jnp.sum(macc[15:16, :])

    zt = jnp.transpose(z2[...])
    valid = cls_id < CLS
    top = jnp.max(jnp.where(valid, zt, -jnp.inf), axis=0, keepdims=True)
    expz = jnp.where(valid, jnp.exp(zt - top), 0.0)
    log_norm = jnp.log(jnp.sum(expz, axis=0, keepdims=True)) + top
    one_hot = cls_id == lab_ref[...]
    picked = jnp.sum(jnp.where(one_hot, zt, 0.0), axis=0, keepdims=True)
    loss_terms = weight * (log_norm - picked)
    acc = loss_terms[:, 0:128]
    for n in range(1, BLK // 128):
        acc = acc + loss_terms[:, 128 * n:128 * (n + 1)]
    lossv[...] = acc
    prob = jnp.exp(zt - log_norm)
    grad = (prob - one_hot.astype(F32)) * (weight / label_count)
    gt[...] = jnp.where(valid, grad, 0.0).astype(BF16)


    def reduce_pass(lhs_ref, rows, chunks, part, rb, recv, recv_d2d, early, hooks):
        parts = range(len(chunks))

        def order_of(k):
            return ORDERS[chunks[k][4]]

        def dim_of(q, k):
            return next(d for d in reversed(order_of(k)) if q & d)

        def ici(q, k):
            lo, n, lane, lanes, _ = chunks[k]
            idx = k * 7 + QI[q] - 1
            return rcopy(con.at[2 * QI[q], pl.ds(lo, n), pl.ds(lane, lanes)],
                         rb.at[QI[q] - 1, pl.ds(lo, n), pl.ds(lane, lanes)], ici_send,
                         recv.at[idx], 2 * dim_of(q, k))

        def d2d(i):
            return rcopy(con.at[2 * i + 1, pl.ds(0, rows), :], part.at[i], d2d_send, recv_d2d.at[i], 1)

        def sources(q, k):
            out = []
            for d in reversed(order_of(k)):
                if q & d:
                    break
                out.append(q ^ d)
            return out

        def compute(slot):
            lhs = (lhs_ref[...].astype(F32) * mask_of(slot).astype(F32)).astype(BF16)
            con[slot, 0:rows, :] = jnp.dot(lhs, adj[slot], preferred_element_type=F32)

        waiting = {(q, k): set(sources(q, k)) for q in range(8) for k in parts}

        def pair_sum(q):
            i = QI[q]
            d2d(i).wait_recv()
            con[2 * i, 0:rows, :] += part[i]
            for k in parts:
                if q and not waiting[q, k]:
                    ici(q, k).start()

        def take(src, k):
            d = dim_of(src, k)
            q = src ^ d
            lo, n, lane, lanes, _ = chunks[k]
            ici(src, k).wait_recv()
            con[2 * QI[q], lo:lo + n, lane:lane + lanes] += rb[QI[src] - 1, lo:lo + n, lane:lane + lanes]
            waiting[q, k].discard(src)
            if q and not waiting[q, k]:
                ici(q, k).start()

        def body(n, carry):
            i = 7 - n
            compute(2 * i + 1)
            d2d(i).start()
            compute(2 * i)
            for m in range(8):
                @pl.when(n == m)
                def _(m=m):
                    if m:
                        pair_sum(QS[8 - m])
                    for r in early.get(m, ()):
                        take_rank(r)
                    for hook in hooks.get(m, ()):
                        hook()
            return carry

        rank = {q: r for r, q in enumerate(reversed(QS))}
        taken = set()

        def sources_of(k, phase):
            d = order_of(k)[2 - phase]
            later = order_of(k)[3 - phase:]
            return sorted((q for q in range(1, 8) if q & d and not any(q & e for e in later)), key=rank.get)

        def take_rank(r, phase=0):
            for k in parts:
                take(sources_of(k, phase)[r], k)
                taken.add((phase, r))

        lax.fori_loop(0, 8, body, 0)
        for r in range(4):
            if (0, r) not in taken:
                take_rank(r)
            if r == 2:
                for hook in hooks.get('mid', ()):
                    hook()
                pair_sum(0)
        take_rank(0, 1)
        take_rank(1, 1)
        for hook in hooks.get('late', ()):
            hook()
        take_rank(0, 2)
        for count, sem, rel in ((7, ici_send, 2), (8, d2d_send, 1)):
            sent = con.at[pl.ds(0, count), pl.ds(0, rows), :]
            rcopy(sent, sent, sem, recv.at[0], rel).wait_send()

    reduce_pass(gt, CLS_PAD, D2_CHUNKS, part2, rb2, recv_a, d2d_a, {6: [0], 7: [1]}, {})
    d2t = con[0, 0:CLS_PAD, :].astype(BF16)
    gwo = jnp.dot(d2t, hid[...], preferred_element_type=F32)
    et[...] = jnp.where(z1t[...] > 0, dot_first(wos[...], d2t), 0.0).astype(BF16)
    row_id = lax.broadcasted_iota(jnp.int32, (CLS_PAD, HID), 0)
    gwos[...] = jnp.where(row_id == CLS, lossv[...], gwo)

    core = coords[0]

    def all_sum(rows, total_rows, src, halves, other, own, gathered, final, send, recv):
        def prepare():
            halves[0] = src[0:rows, :]
            halves[1, 0:total_rows - rows, :] = src[rows:total_rows, :]
            if total_rows < 2 * rows:
                halves[1, total_rows - rows:rows, :] = jnp.zeros((2 * rows - total_rows, HID), F32)

        pair = rcopy(halves.at[1 - core], other, send.at[0], recv.at[0], 1)
        sends = [rcopy(gathered.at[0], gathered.at[q], send.at[1], recv.at[q], 2 * q) for q in range(1, 8)]
        back = rcopy(own, final, send.at[2], recv.at[8], 1)

        def start():
            prepare()
            pair.start()

        def spread():
            pair.wait()
            gathered[0] = halves[core] + other[...]
            for q in (7, 6, 5, 3, 4, 2, 1):
                sends[q - 1].start()

        def collect():
            for cp in sends:
                cp.wait_recv()
            rcopy(gathered.at[pl.ds(0, 7)], gathered.at[pl.ds(0, 7)], send.at[1], recv.at[0], 2).wait_send()
            g = gathered
            own[...] = ((g[0] + g[1]) + (g[2] + g[3])) + ((g[4] + g[5]) + (g[6] + g[7]))
            back.start()

        def finish():
            halves[core] = own[...]
            back.wait()
            halves[1 - core] = final[...]

        return start, spread, collect, finish

    gwo_start, gwo_spread, gwo_collect, gwo_finish = all_sum(GWO_HALF, CLS_PAD, gwos, gwop, gwof.at[0], gwor, gwog,
                                                             gwof.at[1], gwo_send, gwo_recv)
    gwh_start, gwh_spread, gwh_collect, gwh_finish = all_sum(GWH_HALF, F_PAD, gwhs, gwhp, gwhf.at[0], gwhr, gwhg,
                                                             gwhf.at[1], gwh_send, gwh_recv)
    gwo_start()

    def gwo_out():
        gwo_finish()
        out_ref[F_PAD:F_PAD + GWO_HALF, :] = gwop[0]
        out_ref[F_PAD + GWO_HALF:OUT_ROWS, :] = gwop[1]
        loss = jnp.sum(gwop[1, GWO_HALF - 1:GWO_HALF, :], axis=1, keepdims=True) / label_count
        out_ref[OUT_ROWS - 1:OUT_ROWS, :] = jnp.broadcast_to(loss, (1, HID))

    reduce_pass(et, HID, D1_CHUNKS, part1, rb1, recv_b, d2d_b, {},
                {0: [gwo_spread], 'mid': [gwo_collect], 'late': [gwo_out]})
    gwhs[...] = dot_last(xall[0], con[0].astype(BF16))
    gwh_start()
    gwh_spread()
    gwh_collect()
    gwh_finish()
    out_ref[0:GWH_HALF, :] = gwhp[0]
    out_ref[GWH_HALF:F_PAD, :] = gwhp[1, 0:F_PAD - GWH_HALF, :]


def split_kernel(sums_ref, gwh_ref, gwot_ref, loss_ref):
    gwh_ref[...] = sums_ref[0:F_IN, :]
    gwot_ref[...] = sums_ref[F_PAD:F_PAD + CLS, :]
    loss_ref[...] = sums_ref[OUT_ROWS - 1:OUT_ROWS, 0:1]


def device_step(adj_rows, feat_rows, w_hidden, w_output, labels, train_mask, block_mask):
    dma = pltpu.SemaphoreType.DMA
    vmem = pl.BlockSpec(memory_space=pltpu.VMEM)
    hbm = pl.BlockSpec(memory_space=pl.ANY)
    sums = pl.pallas_call(
        step_kernel,
        name='gcn_step',
        out_shape=pltpu.VMEM((OUT_ROWS, HID), F32),
        in_specs=[hbm] * 7,
        out_specs=vmem,
        scratch_shapes=[
            pltpu.VMEM((F_IN, BLK), BF16),
            pltpu.VMEM((F_IN, HID), F32),
            pltpu.VMEM((CLS, HID), F32),
            pltpu.VMEM((1, BLK), jnp.int32),
            pltpu.VMEM((1, BLK), jnp.int32),
            pltpu.SMEM((NB, NB), jnp.int32),
            pltpu.VMEM((NB, BLK, BLK), BF16),
            pltpu.VMEM((NB, F_PAD, BLK), BF16),
            pltpu.VMEM((NB, CLS_PAD, BLK), BF16),
            pltpu.VMEM((2, HID, BLK), BF16),
            pltpu.VMEM((BLK, HID), F32),
            pltpu.VMEM((HID, BLK), F32),
            pltpu.VMEM((BLK, CLS_PAD), F32),
            pltpu.VMEM((BLK, HID), BF16),
            pltpu.VMEM((CLS_PAD, BLK), BF16),
            pltpu.VMEM((HID, BLK), BF16),
            pltpu.VMEM((NB, HID, BLK), F32),
            pltpu.VMEM((8, CLS_PAD, BLK), F32),
            pltpu.VMEM((8, HID, BLK), F32),
            pltpu.VMEM((7, CLS_PAD, BLK), F32),
            pltpu.VMEM((7, HID, BLK), F32),
            pltpu.VMEM((F_PAD, HID), BF16),
            pltpu.VMEM((CLS_PAD, HID), BF16),
            pltpu.VMEM((16, BLK), F32),
            pltpu.VMEM((1, 128), F32),
            pltpu.VMEM((CLS_PAD, HID), F32),
            pltpu.VMEM((2, GWO_HALF, HID), F32),
            pltpu.VMEM((GWO_HALF, HID), F32),
            pltpu.VMEM((8, GWO_HALF, HID), F32),
            pltpu.VMEM((2, GWO_HALF, HID), F32),
            pltpu.VMEM((F_PAD, HID), F32),
            pltpu.VMEM((2, GWH_HALF, HID), F32),
            pltpu.VMEM((GWH_HALF, HID), F32),
            pltpu.VMEM((8, GWH_HALF, HID), F32),
            pltpu.VMEM((2, GWH_HALF, HID), F32),
            dma((6,)), dma((NB,)), dma, dma, dma((21,)), dma((8,)), dma((42,)), dma((8,)),
            dma((3,)), dma((9,)), dma((3,)), dma((9,)),
        ],
        compiler_params=pltpu.CompilerParams(collective_id=0, has_side_effects=True, vmem_limit_bytes=62000000),
    )(adj_rows, feat_rows.T, w_hidden, w_output.T, labels[None, :], train_mask[None, :], block_mask)
    gwh, gwot, loss = pl.pallas_call(
        split_kernel,
        name='split_sums',
        out_shape=(jax.ShapeDtypeStruct((F_IN, HID), F32), jax.ShapeDtypeStruct((CLS, HID), F32),
                   jax.ShapeDtypeStruct((1, 1), F32)),
        in_specs=[vmem],
        out_specs=(vmem, vmem, vmem),
    )(pltpu.with_memory_space_constraint(sums, pltpu.VMEM))
    return loss[0, 0], gwh, gwot.T


def solution(mesh):
    row_spec = P(AXIS_NAME, None)
    vec_spec = P(AXIS_NAME)
    return jax.shard_map(device_step, mesh=mesh, in_specs=(row_spec, row_spec, P(), P(), vec_spec, vec_spec, P()), out_specs=(P(), P(), P()), check_vma=False)
```

```python
import jax
import jax.numpy as jnp
from jax import lax
from jax.experimental import pallas as pl
from jax.experimental.pallas import tpu as pltpu
from jax.sharding import PartitionSpec as P

AXIS_NAME = 'nodes'
MESH = pl.DeviceIdType.MESH
F32, BF16 = jnp.float32, jnp.bfloat16
BLK = 1024
NB = 16
F_IN, F_PAD = 100, 104
HID = 128
CLS, CLS_PAD = 47, 48
QS = [0, 2, 4, 1, 3, 6, 5, 7]
QI = {q: i for i, q in enumerate(QS)}
ORDERS = [(1, 2, 4), (2, 4, 1), (4, 1, 2)]
X_CHUNKS = [(0, 40), (40, 32), (72, 32)]
Y_CHUNKS = [(0, 16), (16, 16), (32, 16)]
D2_CHUNKS = [(lo, n, 0, BLK, k) for k, (lo, n) in enumerate(Y_CHUNKS)]
D1_CHUNKS = [(0, 40, 0, BLK, 0), (40, 40, 0, BLK, 1), (80, 40, 0, BLK, 2),
             (120, 8, 0, 384, 0), (120, 8, 384, 384, 1), (120, 8, 768, 256, 2)]
GWO_HALF, GWH_HALF = 24, 56
OUT_ROWS = F_PAD + CLS_PAD
M_TILE = 256
A_AHEAD = 5


def forwards(q, k, swapped):
    first, second, third = ORDERS[k]
    if k in swapped and q == first:
        return [(first, second)]
    if k in swapped and q == second:
        return [(second, third), (first, third)]
    order = ORDERS[k]
    return [(q, d) for d in order[1 + max(order.index(d) for d in order if q & d):]]


def last_dim(q, k):
    return max((d for d in ORDERS[k] if q & d), key=ORDERS[k].index)


def plan_gather(sizes, cost, max_group, swapped):
    link = {1: 0.0, 2: 0.0, 4: 0.0, 0: 0.0}
    ops, arrive, relayed, ready = [], {}, {}, [0]
    now = 0.0

    def send(table, key, dim, size):
        link[dim] = max(now, link[dim]) + size / (46.6 if dim else 600.0)
        table[key] = link[dim] + (2.3 if dim else 0.95)

    for j in range(3):
        for k in range(3):
            send(arrive, (ORDERS[k][j], k), ORDERS[k][j], sizes[k])
    send(relayed, 0, 0, sum(sizes))
    got = {q: 0 for q in range(8)}
    while arrive or relayed or ready:
        key = min(arrive, key=arrive.get, default=None)
        if key is not None and arrive[key] <= now:
            del arrive[key]
            q, k = key
            ops.append(('recv', q, k))
            for src, d in forwards(q, k, swapped):
                send(arrive, (src | d, k), d, sizes[k])
            got[q] += 1
            if got[q] == 3:
                ops.append(('relay', q))
                send(relayed, q, 0, sum(sizes))
                ready.append(2 * QI[q])
            continue
        for q in sorted(relayed, key=relayed.get):
            if relayed[q] <= now:
                del relayed[q]
                ops.append(('take', q))
                ready.append(2 * QI[q] + 1)
        if ready:
            ops.append(('dot', ready[:max_group]))
            now += cost(len(ready[:max_group]))
            ready = ready[max_group:]
        else:
            now = min(list(arrive.values()) + list(relayed.values()))
    return ops


def dot_last(lhs, rhs):
    return lax.dot_general(lhs, rhs, (((1,), (1,)), ((), ())), preferred_element_type=F32)


def dot_first(lhs, rhs):
    return lax.dot_general(lhs, rhs, (((0,), (0,)), ((), ())), preferred_element_type=F32)


def step_kernel(adj_hbm, x_hbm, wh_hbm, wot_hbm, lab_hbm, msk_hbm, bm_hbm, out_ref,
                x_ref, wh_ref, wot_ref, lab_ref, msk_ref, bm_ref,
                adj, xall, yall, y1b, z1, z1t, z2, z2t, turned, hid, gt, et, con, part2, part1, rb2, rb1, whs, wos, macc, lossv,
                gwos, gwop, gwor, gwog, gwof, gwhs, gwhp, gwhr, gwhg, gwhf,
                io_sem, a_sem, ici_send, d2d_send, recv_a, d2d_a, recv_b, d2d_b,
                gwo_send, gwo_recv, gwh_send, gwh_recv):
    me = lax.axis_index(AXIS_NAME)
    coords = [me % 2, (me // 2) % 2, (me // 4) % 2, me // 8]

    def dev(rel):
        total = 0
        for bit in range(4):
            total = total + ((coords[bit] + ((rel >> bit) & 1)) % 2) * (1 << bit)
        return total

    def rel_of(slot):
        return 2 * QS[slot // 2] + slot % 2

    def rcopy(src, dst, send_sem, recv_sem, rel):
        return pltpu.make_async_remote_copy(src_ref=src, dst_ref=dst, send_sem=send_sem, recv_sem=recv_sem,
                                            device_id=(dev(rel),), device_id_type=MESH)

    def a_copy(slot, blk=0):
        return pltpu.make_async_copy(adj_hbm.at[:, pl.ds(pl.multiple_of(blk * BLK, BLK), BLK)], adj.at[slot], a_sem.at[slot])

    plan1 = plan_gather([n * 2.048 for _, n in X_CHUNKS], lambda n: 0.2 + 0.54 * n, 2, (2,))
    a_order = [slot for op in plan1 if op[0] == 'dot' for slot in op[1]]

    def start_a(lo, hi):
        for slot in a_order[lo:hi]:
            a_copy(slot, dev(rel_of(slot))).start()

    loads = [pltpu.make_async_copy(src, dst, io_sem.at[n]) for n, (src, dst) in enumerate(
        [(x_hbm, x_ref), (wh_hbm, wh_ref), (wot_hbm, wot_ref), (lab_hbm, lab_ref), (msk_hbm, msk_ref), (bm_hbm, bm_ref)])]
    barrier = pltpu.get_barrier_semaphore()
    peers = [1, 2, 4, 8]
    for rel in peers:
        pl.semaphore_signal(barrier, inc=1, device_id=(dev(rel),), device_id_type=MESH)

    for load in loads:
        load.start()
    start_a(0, A_AHEAD)
    macc[...] = jnp.zeros_like(macc)
    z1[...] = jnp.zeros_like(z1)
    z2[...] = jnp.zeros_like(z2)
    z2t[...] = jnp.zeros_like(z2t)
    whs[...] = jnp.zeros_like(whs)
    wos[...] = jnp.zeros_like(wos)
    for load in loads:
        load.wait()
    xall[0, 0:F_PAD - 8, :] = x_ref[0:F_PAD - 8, :]
    xall[0, F_PAD - 8:F_PAD, :] = jnp.concatenate([x_ref[F_PAD - 8:F_IN, :], jnp.zeros((F_PAD - F_IN, BLK), BF16)], axis=0)
    whs[0:F_IN, :] = wh_ref[...].astype(BF16)
    wos[0:CLS, :] = wot_ref[...].astype(BF16)
    pl.semaphore_wait(barrier, len(peers))

    def mask_of(slot):
        if isinstance(slot, int):
            return bm_ref[me, dev(rel_of(slot))]
        i = slot // 2
        c = slot % 2
        bits = []
        for bit in (1, 2, 4):
            b = 0
            for pos, q in enumerate(QS):
                if q & bit:
                    d = (i - pos) * (i - pos)
                    b = b + 1 // (1 + d)
            bits.append(b)
        total = ((coords[0] + c) % 2)
        for n, b in enumerate(bits):
            total = total + ((coords[n + 1] + b) % 2) * (2 << n)
        return bm_ref[me, total]


    def gather_product(buf, chunks, recv, recv_d2d, ops, swapped, first, dots):
        def ici(src_q, dim, k):
            dst_q = src_q ^ dim
            lo, n = chunks[k]
            return rcopy(buf.at[2 * QI[src_q], pl.ds(lo, n), :], buf.at[2 * QI[dst_q], pl.ds(lo, n), :],
                         ici_send, recv.at[k * 7 + QI[dst_q] - 1], 2 * dim)

        def relay(q):
            return rcopy(buf.at[2 * QI[q]], buf.at[2 * QI[q] + 1], d2d_send, recv_d2d.at[QI[q]], 1)

        for j in range(3):
            for k in range(3):
                ici(0, ORDERS[k][j], k).start()
        relay(0).start()
        first()
        for op, q, *k in ops:
            if op == 'dot':
                dots(q)
            elif op == 'take':
                relay(q).wait_recv()
            elif op == 'relay':
                relay(q).start()
            else:
                d = last_dim(q, k[0])
                ici(q ^ d, d, k[0]).wait_recv()
                for src, d in forwards(q, k[0], swapped):
                    ici(src, d, k[0]).start()
        for count, sem, rel in ((7, ici_send, 2), (8, d2d_send, 1)):
            sent = buf.at[pl.ds(0, count)]
            rcopy(sent, sent, sem, recv.at[0], rel).wait_send()

    def accumulate(out, slots, blocks):
        for lo in range(0, BLK, M_TILE):
            acc = out[lo:lo + M_TILE, :]
            for slot, block in zip(slots, blocks):
                acc = acc + dot_last(adj[slot, lo:lo + M_TILE, :], block)
            out[lo:lo + M_TILE, :] = acc

    def dots1(slots):
        for slot in slots:
            a_copy(slot).wait()
            ahead = a_order.index(slot) + A_AHEAD
            start_a(ahead, ahead + 1)
        for j, slot in enumerate(slots):
            yt = dot_first(whs[...], xall[slot]).astype(BF16)
            y1b[j] = (yt.astype(F32) * mask_of(slot).astype(F32)).astype(BF16)
        accumulate(z1, slots, [y1b[j] for j in range(len(slots))])

    gather_product(xall, X_CHUNKS, recv_a, d2d_a, plan1, (2,), lambda: None, dots1)

    cls_id = lax.broadcasted_iota(jnp.int32, (CLS_PAD, BLK), 0)
    weight = msk_ref[...].astype(F32)
    hid[...] = jnp.maximum(z1[...], 0.0).astype(BF16)
    yall[0] = jnp.where(cls_id == CLS, weight, dot_last(wos[...], hid[...])).astype(BF16)

    def dots2(slots):
        blocks = []
        for slot in slots:
            macc[...] += yall[slot, CLS_PAD - 16:CLS_PAD, :].astype(F32)
            blocks.append((yall[slot].astype(F32) * mask_of(slot).astype(F32)).astype(BF16))
        if len(slots) == 1:
            accumulate(z2, slots, blocks)
            return
        stream, held = slots
        turned[0] = jnp.transpose(adj[held, 0:M_TILE, :])
        for n in range(BLK // M_TILE):
            tile = slice(M_TILE * n, M_TILE * (n + 1))
            if n + 1 < BLK // M_TILE:
                turned[(n + 1) % 2] = jnp.transpose(adj[held, M_TILE * (n + 1):M_TILE * (n + 2), :])
            z2[tile, :] += dot_last(adj[stream, tile, :], blocks[0])
            z2t[:, tile] += jnp.dot(blocks[1], turned[n % 2], preferred_element_type=F32)

    def keep_sign():
        z1t[...] = jnp.transpose(z1[...])

    plan2 = plan_gather([n * 2.048 for _, n in Y_CHUNKS], lambda n: 0.43 + 0.25 * n, 2, (0, 1))
    gather_product(yall, Y_CHUNKS, recv_b, d2d_b, plan2, (0, 1), keep_sign, dots2)
    label_count = jnp.sum(macc[15:16, :])

    zt = jnp.transpose(z2[...]) + z2t[...]
    valid = cls_id < CLS
    top = jnp.max(jnp.where(valid, zt, -jnp.inf), axis=0, keepdims=True)
    expz = jnp.where(valid, jnp.exp(zt - top), 0.0)
    log_norm = jnp.log(jnp.sum(expz, axis=0, keepdims=True)) + top
    one_hot = cls_id == lab_ref[...]
    picked = jnp.sum(jnp.where(one_hot, zt, 0.0), axis=0, keepdims=True)
    loss_terms = weight * (log_norm - picked)
    acc = loss_terms[:, 0:128]
    for n in range(1, BLK // 128):
        acc = acc + loss_terms[:, 128 * n:128 * (n + 1)]
    lossv[...] = acc
    prob = jnp.exp(zt - log_norm)
    grad = (prob - one_hot.astype(F32)) * (weight / label_count)
    gt[...] = jnp.where(valid, grad, 0.0).astype(BF16)


    def reduce_pass(lhs_ref, rows, chunks, part, rb, recv, recv_d2d, early, tail, hooks):
        parts = range(len(chunks))

        def order_of(k):
            return ORDERS[chunks[k][4]]

        def dim_of(q, k):
            return next(d for d in reversed(order_of(k)) if q & d)

        def ici(q, k):
            lo, n, lane, lanes, _ = chunks[k]
            idx = k * 7 + QI[q] - 1
            return rcopy(con.at[2 * QI[q], pl.ds(lo, n), pl.ds(lane, lanes)],
                         rb.at[QI[q] - 1, pl.ds(lo, n), pl.ds(lane, lanes)], ici_send,
                         recv.at[idx], 2 * dim_of(q, k))

        def d2d(i):
            return rcopy(con.at[2 * i + 1, pl.ds(0, rows), :], part.at[i], d2d_send, recv_d2d.at[i], 1)

        def sources(q, k):
            out = []
            for d in reversed(order_of(k)):
                if q & d:
                    break
                out.append(q ^ d)
            return out

        def compute(slot):
            lhs = (lhs_ref[...].astype(F32) * mask_of(slot).astype(F32)).astype(BF16)
            con[slot, 0:rows, :] = jnp.dot(lhs, adj[slot], preferred_element_type=F32)

        waiting = {(q, k): set(sources(q, k)) for q in range(8) for k in parts}

        def pair_sum(q):
            i = QI[q]
            d2d(i).wait_recv()
            con[2 * i, 0:rows, :] += part[i]
            for k in parts:
                if q and not waiting[q, k]:
                    ici(q, k).start()

        def take(src, k):
            d = dim_of(src, k)
            q = src ^ d
            lo, n, lane, lanes, _ = chunks[k]
            ici(src, k).wait_recv()
            con[2 * QI[q], lo:lo + n, lane:lane + lanes] += rb[QI[src] - 1, lo:lo + n, lane:lane + lanes]
            waiting[q, k].discard(src)
            if q and not waiting[q, k]:
                ici(q, k).start()

        def body(n, carry):
            i = 7 - n
            compute(2 * i + 1)
            d2d(i).start()
            compute(2 * i)
            for m in range(8):
                @pl.when(n == m)
                def _(m=m):
                    if m:
                        pair_sum(QS[8 - m])
                    for r in early.get(m, ()):
                        take_rank(r)
                    for hook in hooks.get(m, ()):
                        hook()
            return carry

        rank = {q: r for r, q in enumerate(reversed(QS))}

        def sources_of(k, phase):
            d = order_of(k)[2 - phase]
            later = order_of(k)[3 - phase:]
            return sorted((q for q in range(1, 8) if q & d and not any(q & e for e in later)), key=rank.get)

        def take_rank(r, phase=0):
            for k in parts:
                take(sources_of(k, phase)[r], k)

        lax.fori_loop(0, 8, body, 0)
        for step in tail:
            if step is None:
                pair_sum(0)
            elif isinstance(step, str):
                for hook in hooks[step]:
                    hook()
            else:
                take_rank(step[1], step[0])
        for count, sem, rel in ((7, ici_send, 2), (8, d2d_send, 1)):
            sent = con.at[pl.ds(0, count), pl.ds(0, rows), :]
            rcopy(sent, sent, sem, recv.at[0], rel).wait_send()

    reduce_pass(gt, CLS_PAD, D2_CHUNKS, part2, rb2, recv_a, d2d_a, {5: [0], 6: [1], 7: [2]}, [None, (1, 0), (0, 3), (1, 1), (2, 0)], {})
    d2t = con[0, 0:CLS_PAD, :].astype(BF16)
    gwo = jnp.dot(d2t, hid[...], preferred_element_type=F32)
    et[...] = jnp.where(z1t[...] > 0, dot_first(wos[...], d2t), 0.0).astype(BF16)
    row_id = lax.broadcasted_iota(jnp.int32, (CLS_PAD, HID), 0)
    gwos[...] = jnp.where(row_id == CLS, lossv[...], gwo)

    core = coords[0]

    def all_sum(rows, total_rows, src, halves, other, own, gathered, final, send, recv):
        def prepare():
            halves[0] = src[0:rows, :]
            halves[1, 0:total_rows - rows, :] = src[rows:total_rows, :]
            if total_rows < 2 * rows:
                halves[1, total_rows - rows:rows, :] = jnp.zeros((2 * rows - total_rows, HID), F32)

        pair = rcopy(halves.at[1 - core], other, send.at[0], recv.at[0], 1)
        sends = [rcopy(gathered.at[0], gathered.at[q], send.at[1], recv.at[q], 2 * q) for q in range(1, 8)]
        back = rcopy(own, final, send.at[2], recv.at[8], 1)

        def start():
            prepare()
            pair.start()

        def spread():
            pair.wait()
            gathered[0] = halves[core] + other[...]
            for q in (7, 6, 5, 3, 4, 2, 1):
                sends[q - 1].start()

        def collect():
            for cp in sends:
                cp.wait_recv()
            rcopy(gathered.at[pl.ds(0, 7)], gathered.at[pl.ds(0, 7)], send.at[1], recv.at[0], 2).wait_send()
            g = gathered
            own[...] = ((g[0] + g[1]) + (g[2] + g[3])) + ((g[4] + g[5]) + (g[6] + g[7]))
            back.start()

        def finish():
            halves[core] = own[...]
            back.wait()
            halves[1 - core] = final[...]

        return start, spread, collect, finish

    gwo_start, gwo_spread, gwo_collect, gwo_finish = all_sum(GWO_HALF, CLS_PAD, gwos, gwop, gwof.at[0], gwor, gwog,
                                                             gwof.at[1], gwo_send, gwo_recv)
    gwh_start, gwh_spread, gwh_collect, gwh_finish = all_sum(GWH_HALF, F_PAD, gwhs, gwhp, gwhf.at[0], gwhr, gwhg,
                                                             gwhf.at[1], gwh_send, gwh_recv)
    gwo_start()

    def gwo_out():
        gwo_finish()
        out_ref[F_PAD:F_PAD + GWO_HALF, :] = gwop[0]
        out_ref[F_PAD + GWO_HALF:OUT_ROWS, :] = gwop[1]
        loss = jnp.sum(gwop[1, GWO_HALF - 1:GWO_HALF, :], axis=1, keepdims=True) / label_count
        out_ref[OUT_ROWS - 1:OUT_ROWS, :] = jnp.broadcast_to(loss, (1, HID))

    reduce_pass(et, HID, D1_CHUNKS, part1, rb1, recv_b, d2d_b, {},
                [(0, 0), (0, 1), (0, 2), 'mid', None, (0, 3), (1, 0), (1, 1), 'late', (2, 0)],
                {0: [gwo_spread], 'mid': [gwo_collect], 'late': [gwo_out]})
    gwhs[...] = dot_last(xall[0], con[0].astype(BF16))
    gwh_start()
    gwh_spread()
    gwh_collect()
    gwh_finish()
    out_ref[0:GWH_HALF, :] = gwhp[0]
    out_ref[GWH_HALF:F_PAD, :] = gwhp[1, 0:F_PAD - GWH_HALF, :]


def split_kernel(sums_ref, gwh_ref, gwot_ref, loss_ref):
    gwh_ref[...] = sums_ref[0:F_IN, :]
    gwot_ref[...] = sums_ref[F_PAD:F_PAD + CLS, :]
    loss_ref[...] = sums_ref[OUT_ROWS - 1:OUT_ROWS, 0:1]


def device_step(adj_rows, feat_rows, w_hidden, w_output, labels, train_mask, block_mask):
    dma = pltpu.SemaphoreType.DMA
    vmem = pl.BlockSpec(memory_space=pltpu.VMEM)
    hbm = pl.BlockSpec(memory_space=pl.ANY)
    sums = pl.pallas_call(
        step_kernel,
        name='gcn_step',
        out_shape=pltpu.VMEM((OUT_ROWS, HID), F32),
        in_specs=[hbm] * 7,
        out_specs=vmem,
        scratch_shapes=[
            pltpu.VMEM((F_IN, BLK), BF16),
            pltpu.VMEM((F_IN, HID), F32),
            pltpu.VMEM((CLS, HID), F32),
            pltpu.VMEM((1, BLK), jnp.int32),
            pltpu.VMEM((1, BLK), jnp.int32),
            pltpu.SMEM((NB, NB), jnp.int32),
            pltpu.VMEM((NB, BLK, BLK), BF16),
            pltpu.VMEM((NB, F_PAD, BLK), BF16),
            pltpu.VMEM((NB, CLS_PAD, BLK), BF16),
            pltpu.VMEM((2, HID, BLK), BF16),
            pltpu.VMEM((BLK, HID), F32),
            pltpu.VMEM((HID, BLK), F32),
            pltpu.VMEM((BLK, CLS_PAD), F32),
            pltpu.VMEM((CLS_PAD, BLK), F32),
            pltpu.VMEM((2, BLK, M_TILE), BF16),
            pltpu.VMEM((BLK, HID), BF16),
            pltpu.VMEM((CLS_PAD, BLK), BF16),
            pltpu.VMEM((HID, BLK), BF16),
            pltpu.VMEM((NB, HID, BLK), F32),
            pltpu.VMEM((8, CLS_PAD, BLK), F32),
            pltpu.VMEM((8, HID, BLK), F32),
            pltpu.VMEM((7, CLS_PAD, BLK), F32),
            pltpu.VMEM((7, HID, BLK), F32),
            pltpu.VMEM((F_PAD, HID), BF16),
            pltpu.VMEM((CLS_PAD, HID), BF16),
            pltpu.VMEM((16, BLK), F32),
            pltpu.VMEM((1, 128), F32),
            pltpu.VMEM((CLS_PAD, HID), F32),
            pltpu.VMEM((2, GWO_HALF, HID), F32),
            pltpu.VMEM((GWO_HALF, HID), F32),
            pltpu.VMEM((8, GWO_HALF, HID), F32),
            pltpu.VMEM((2, GWO_HALF, HID), F32),
            pltpu.VMEM((F_PAD, HID), F32),
            pltpu.VMEM((2, GWH_HALF, HID), F32),
            pltpu.VMEM((GWH_HALF, HID), F32),
            pltpu.VMEM((8, GWH_HALF, HID), F32),
            pltpu.VMEM((2, GWH_HALF, HID), F32),
            dma((6,)), dma((NB,)), dma, dma, dma((21,)), dma((8,)), dma((42,)), dma((8,)),
            dma((3,)), dma((9,)), dma((3,)), dma((9,)),
        ],
        compiler_params=pltpu.CompilerParams(collective_id=0, has_side_effects=True, vmem_limit_bytes=64000000),
    )(adj_rows, feat_rows.T, w_hidden, w_output.T, labels[None, :], train_mask[None, :], block_mask)
    gwh, gwot, loss = pl.pallas_call(
        split_kernel,
        name='split_sums',
        out_shape=(jax.ShapeDtypeStruct((F_IN, HID), F32), jax.ShapeDtypeStruct((CLS, HID), F32),
                   jax.ShapeDtypeStruct((1, 1), F32)),
        in_specs=[vmem],
        out_specs=(vmem, vmem, vmem),
    )(pltpu.with_memory_space_constraint(sums, pltpu.VMEM))
    return loss[0, 0], gwh, gwot.T


def solution(mesh):
    row_spec = P(AXIS_NAME, None)
    vec_spec = P(AXIS_NAME)
    return jax.shard_map(device_step, mesh=mesh, in_specs=(row_spec, row_spec, P(), P(), vec_spec, vec_spec, P()), out_specs=(P(), P(), P()), check_vma=False)
```

```python
import jax
import jax.numpy as jnp
from jax import lax
from jax.experimental import pallas as pl
from jax.experimental.pallas import tpu as pltpu
from jax.sharding import PartitionSpec as P

AXIS_NAME = 'nodes'
MESH = pl.DeviceIdType.MESH
F32, BF16 = jnp.float32, jnp.bfloat16
BLK = 1024
NB = 16
F_IN, F_PAD = 100, 104
HID = 128
CLS, CLS_PAD = 47, 48
QS = [0, 2, 4, 1, 3, 6, 5, 7]
QI = {q: i for i, q in enumerate(QS)}
ORDERS = [(1, 2, 4), (2, 4, 1), (4, 1, 2)]
X_CHUNKS = [(0, 32, 0, BLK, 0), (32, 32, 0, BLK, 1), (64, 32, 0, BLK, 2),
            (96, 8, 0, 384, 0), (96, 8, 384, 384, 1), (96, 8, 768, 256, 2)]
Y_CHUNKS = [(0, 16, 0, BLK, 0), (16, 16, 0, BLK, 1), (32, 16, 0, BLK, 2)]
D1_CHUNKS = [(0, 40, 0, BLK, 0), (40, 40, 0, BLK, 1), (80, 40, 0, BLK, 2),
             (120, 8, 0, 384, 0), (120, 8, 384, 384, 1), (120, 8, 768, 256, 2)]
GWO_HALF, GWH_HALF = 24, 56
OUT_ROWS = F_PAD + CLS_PAD
M_TILE = 256
A_AHEAD = 5


def forwards(q, order_id, swapped):
    first, second, third = order = ORDERS[order_id]
    if order_id in swapped and q == first:
        return [(first, second)]
    if order_id in swapped and q == second:
        return [(second, third), (first, third)]
    return [(q, d) for d in order[1 + max(order.index(d) for d in order if q & d):]]


def last_dim(q, order_id):
    return max((d for d in ORDERS[order_id] if q & d), key=ORDERS[order_id].index)


def plan_gather(chunks, cost, max_group, swapped):
    sizes = [n * lanes * 0.002 for _, n, _, lanes, _ in chunks]
    link = {1: 0.0, 2: 0.0, 4: 0.0, 0: 0.0}
    ops, arrive, relayed, ready = [], {}, {}, [0]
    now = 0.0

    def send(table, key, dim, size):
        link[dim] = max(now, link[dim]) + size / (46.6 if dim else 600.0)
        table[key] = link[dim] + (2.3 if dim else 0.95)

    for j in range(3):
        for k, chunk in enumerate(chunks):
            d = ORDERS[chunk[4]][j]
            send(arrive, (d, k), d, sizes[k])
    send(relayed, 0, 0, sum(sizes))
    got = {q: 0 for q in range(8)}
    while arrive or relayed or ready:
        key = min(arrive, key=arrive.get, default=None)
        if key is not None and arrive[key] <= now:
            del arrive[key]
            q, k = key
            ops.append(('recv', q, k))
            for src, d in forwards(q, chunks[k][4], swapped):
                send(arrive, (src | d, k), d, sizes[k])
            got[q] += 1
            if got[q] == len(chunks):
                ops.append(('relay', q))
                send(relayed, q, 0, sum(sizes))
                ready.append(2 * QI[q])
            continue
        for q in sorted(relayed, key=relayed.get):
            if relayed[q] <= now:
                del relayed[q]
                ops.append(('take', q))
                ready.append(2 * QI[q] + 1)
        if ready:
            ops.append(('dot', ready[:max_group]))
            now += cost(len(ready[:max_group]))
            ready = ready[max_group:]
        else:
            now = min(list(arrive.values()) + list(relayed.values()))
    return ops


def dot_last(lhs, rhs):
    return lax.dot_general(lhs, rhs, (((1,), (1,)), ((), ())), preferred_element_type=F32)


def dot_first(lhs, rhs):
    return lax.dot_general(lhs, rhs, (((0,), (0,)), ((), ())), preferred_element_type=F32)


def step_kernel(adj_hbm, x_hbm, wh_hbm, wot_hbm, lab_hbm, msk_hbm, bm_hbm, out_ref,
                x_ref, wh_ref, wot_ref, lab_ref, msk_ref, bm_ref,
                adj, xall, yall, y1b, z1, z1t, z2, z2t, turned, hid, gt, et, con, part2, part1, rb2, rb1, whs, wos, macc, lossv,
                gwos, gwop, gwor, gwog, gwof, gwhs, gwhp, gwhr, gwhg, gwhf,
                io_sem, a_sem, ici_send, d2d_send, recv_a, d2d_a, recv_b, d2d_b,
                gwo_send, gwo_recv, gwh_send, gwh_recv):
    me = lax.axis_index(AXIS_NAME)
    coords = [me % 2, (me // 2) % 2, (me // 4) % 2, me // 8]

    def dev(rel):
        total = 0
        for bit in range(4):
            total = total + ((coords[bit] + ((rel >> bit) & 1)) % 2) * (1 << bit)
        return total

    def rel_of(slot):
        return 2 * QS[slot // 2] + slot % 2

    def rcopy(src, dst, send_sem, recv_sem, rel):
        return pltpu.make_async_remote_copy(src_ref=src, dst_ref=dst, send_sem=send_sem, recv_sem=recv_sem,
                                            device_id=(dev(rel),), device_id_type=MESH)

    def a_copy(slot, blk=0):
        return pltpu.make_async_copy(adj_hbm.at[:, pl.ds(pl.multiple_of(blk * BLK, BLK), BLK)], adj.at[slot], a_sem.at[slot])

    plan1 = plan_gather(X_CHUNKS, lambda n: 0.2 + 0.54 * n, 2, (2,))
    a_order = [slot for op in plan1 if op[0] == 'dot' for slot in op[1]]

    def start_a(lo, hi):
        for slot in a_order[lo:hi]:
            a_copy(slot, dev(rel_of(slot))).start()

    loads = [pltpu.make_async_copy(src, dst, io_sem.at[n]) for n, (src, dst) in enumerate(
        [(x_hbm, x_ref), (wh_hbm, wh_ref), (wot_hbm, wot_ref), (lab_hbm, lab_ref), (msk_hbm, msk_ref), (bm_hbm, bm_ref)])]
    barrier = pltpu.get_barrier_semaphore()
    peers = [1, 2, 4, 8]
    for rel in peers:
        pl.semaphore_signal(barrier, inc=1, device_id=(dev(rel),), device_id_type=MESH)

    for load in loads:
        load.start()
    start_a(0, A_AHEAD)
    macc[...] = jnp.zeros_like(macc)
    z1[...] = jnp.zeros_like(z1)
    z2[...] = jnp.zeros_like(z2)
    z2t[...] = jnp.zeros_like(z2t)
    whs[...] = jnp.zeros_like(whs)
    wos[...] = jnp.zeros_like(wos)
    for load in loads:
        load.wait()
    xall[0, 0:F_PAD - 8, :] = x_ref[0:F_PAD - 8, :]
    xall[0, F_PAD - 8:F_PAD, :] = jnp.concatenate([x_ref[F_PAD - 8:F_IN, :], jnp.zeros((F_PAD - F_IN, BLK), BF16)], axis=0)
    whs[0:F_IN, :] = wh_ref[...].astype(BF16)
    wos[0:CLS, :] = wot_ref[...].astype(BF16)
    pl.semaphore_wait(barrier, len(peers))

    def mask_of(slot):
        if isinstance(slot, int):
            return bm_ref[me, dev(rel_of(slot))]
        i = slot // 2
        c = slot % 2
        bits = []
        for bit in (1, 2, 4):
            b = 0
            for pos, q in enumerate(QS):
                if q & bit:
                    d = (i - pos) * (i - pos)
                    b = b + 1 // (1 + d)
            bits.append(b)
        total = ((coords[0] + c) % 2)
        for n, b in enumerate(bits):
            total = total + ((coords[n + 1] + b) % 2) * (2 << n)
        return bm_ref[me, total]


    def gather_product(buf, chunks, recv, recv_d2d, ops, swapped, first, dots):
        def ici(src_q, dim, k):
            dst_q = src_q ^ dim
            lo, n, lane, lanes, _ = chunks[k]
            return rcopy(buf.at[2 * QI[src_q], pl.ds(lo, n), pl.ds(lane, lanes)],
                         buf.at[2 * QI[dst_q], pl.ds(lo, n), pl.ds(lane, lanes)],
                         ici_send, recv.at[k * 7 + QI[dst_q] - 1], 2 * dim)

        def relay(q):
            return rcopy(buf.at[2 * QI[q]], buf.at[2 * QI[q] + 1], d2d_send, recv_d2d.at[QI[q]], 1)

        for j in range(3):
            for k, chunk in enumerate(chunks):
                ici(0, ORDERS[chunk[4]][j], k).start()
        relay(0).start()
        first()
        for op, q, *k in ops:
            if op == 'dot':
                dots(q)
            elif op == 'take':
                relay(q).wait_recv()
            elif op == 'relay':
                relay(q).start()
            else:
                order_id = chunks[k[0]][4]
                d = last_dim(q, order_id)
                ici(q ^ d, d, k[0]).wait_recv()
                for src, d in forwards(q, order_id, swapped):
                    ici(src, d, k[0]).start()
        for count, sem, rel in ((7, ici_send, 2), (8, d2d_send, 1)):
            sent = buf.at[pl.ds(0, count)]
            rcopy(sent, sent, sem, recv.at[0], rel).wait_send()

    def accumulate(out, slots, blocks):
        for lo in range(0, BLK, M_TILE):
            acc = out[lo:lo + M_TILE, :]
            for slot, block in zip(slots, blocks):
                acc = acc + dot_last(adj[slot, lo:lo + M_TILE, :], block)
            out[lo:lo + M_TILE, :] = acc

    def dots1(slots):
        for slot in slots:
            a_copy(slot).wait()
            ahead = a_order.index(slot) + A_AHEAD
            start_a(ahead, ahead + 1)
        for j, slot in enumerate(slots):
            yt = dot_first(whs[...], xall[slot]).astype(BF16)
            y1b[j] = (yt.astype(F32) * mask_of(slot).astype(F32)).astype(BF16)
        accumulate(z1, slots, [y1b[j] for j in range(len(slots))])

    gather_product(xall, X_CHUNKS, recv_a, d2d_a, plan1, (2,), lambda: None, dots1)

    cls_id = lax.broadcasted_iota(jnp.int32, (CLS_PAD, BLK), 0)
    weight = msk_ref[...].astype(F32)
    hid[...] = jnp.maximum(z1[...], 0.0).astype(BF16)
    yall[0] = jnp.where(cls_id == CLS, weight, dot_last(wos[...], hid[...])).astype(BF16)

    def dots2(slots):
        blocks = []
        for slot in slots:
            macc[...] += yall[slot, CLS_PAD - 16:CLS_PAD, :].astype(F32)
            blocks.append((yall[slot].astype(F32) * mask_of(slot).astype(F32)).astype(BF16))
        if len(slots) == 1:
            accumulate(z2, slots, blocks)
            return
        stream, held = slots
        turned[0] = jnp.transpose(adj[held, 0:M_TILE, :])
        for n in range(BLK // M_TILE):
            tile = slice(M_TILE * n, M_TILE * (n + 1))
            if n + 1 < BLK // M_TILE:
                turned[(n + 1) % 2] = jnp.transpose(adj[held, M_TILE * (n + 1):M_TILE * (n + 2), :])
            z2[tile, :] += dot_last(adj[stream, tile, :], blocks[0])
            z2t[:, tile] += jnp.dot(blocks[1], turned[n % 2], preferred_element_type=F32)

    def keep_sign():
        z1t[...] = jnp.transpose(z1[...])

    plan2 = plan_gather(Y_CHUNKS, lambda n: 0.43 + 0.25 * n, 2, (0, 1))
    gather_product(yall, Y_CHUNKS, recv_b, d2d_b, plan2, (0, 1), keep_sign, dots2)
    label_count = jnp.sum(macc[15:16, :])

    zt = jnp.transpose(z2[...]) + z2t[...]
    valid = cls_id < CLS
    top = jnp.max(jnp.where(valid, zt, -jnp.inf), axis=0, keepdims=True)
    expz = jnp.where(valid, jnp.exp(zt - top), 0.0)
    log_norm = jnp.log(jnp.sum(expz, axis=0, keepdims=True)) + top
    one_hot = cls_id == lab_ref[...]
    picked = jnp.sum(jnp.where(one_hot, zt, 0.0), axis=0, keepdims=True)
    loss_terms = weight * (log_norm - picked)
    acc = loss_terms[:, 0:128]
    for n in range(1, BLK // 128):
        acc = acc + loss_terms[:, 128 * n:128 * (n + 1)]
    lossv[...] = acc
    prob = jnp.exp(zt - log_norm)
    grad = (prob - one_hot.astype(F32)) * (weight / label_count)
    gt[...] = jnp.where(valid, grad, 0.0).astype(BF16)


    def reduce_pass(lhs_ref, rows, chunks, part, rb, recv, recv_d2d, early, tail, hooks):
        parts = range(len(chunks))

        def order_of(k):
            return ORDERS[chunks[k][4]]

        def dim_of(q, k):
            return next(d for d in reversed(order_of(k)) if q & d)

        def ici(q, k):
            lo, n, lane, lanes, _ = chunks[k]
            idx = k * 7 + QI[q] - 1
            return rcopy(con.at[2 * QI[q], pl.ds(lo, n), pl.ds(lane, lanes)],
                         rb.at[QI[q] - 1, pl.ds(lo, n), pl.ds(lane, lanes)], ici_send,
                         recv.at[idx], 2 * dim_of(q, k))

        def d2d(i):
            return rcopy(con.at[2 * i + 1, pl.ds(0, rows), :], part.at[i], d2d_send, recv_d2d.at[i], 1)

        cuts = [chunks[0][0], chunks[1][0], chunks[2][0], rows]

        def d2d_part(p):
            span = pl.ds(cuts[p], cuts[p + 1] - cuts[p])
            return rcopy(con.at[15, span, :], part.at[7, span, :], d2d_send, recv_d2d.at[8 + p if p else 7], 1)

        def sources(q, k):
            out = []
            for d in reversed(order_of(k)):
                if q & d:
                    break
                out.append(q ^ d)
            return out

        def compute(slot):
            lhs = (lhs_ref[...].astype(F32) * mask_of(slot).astype(F32)).astype(BF16)
            con[slot, 0:rows, :] = jnp.dot(lhs, adj[slot], preferred_element_type=F32)

        waiting = {(q, k): set(sources(q, k)) for q in range(8) for k in parts}

        def pair_sum(q):
            i = QI[q]
            for p in range(3) if i == 7 else [None]:
                lo, hi = (0, rows) if p is None else (cuts[p], cuts[p + 1])
                (d2d(i) if p is None else d2d_part(p)).wait_recv()
                con[2 * i, lo:hi, :] += part[i, lo:hi, :]
                for k in parts:
                    if q and not waiting[q, k] and lo <= chunks[k][0] < hi:
                        ici(q, k).start()

        def take(src, k):
            d = dim_of(src, k)
            q = src ^ d
            lo, n, lane, lanes, _ = chunks[k]
            ici(src, k).wait_recv()
            con[2 * QI[q], lo:lo + n, lane:lane + lanes] += rb[QI[src] - 1, lo:lo + n, lane:lane + lanes]
            waiting[q, k].discard(src)
            if q and not waiting[q, k]:
                ici(q, k).start()

        def body(n, carry):
            i = 7 - n
            compute(2 * i + 1)

            @pl.when(n == 0)
            def _():
                for p in range(3):
                    d2d_part(p).start()

            @pl.when(n > 0)
            def _():
                d2d(i).start()

            compute(2 * i)
            for m in range(8):
                @pl.when(n == m)
                def _(m=m):
                    if m:
                        pair_sum(QS[8 - m])
                    for r in early.get(m, ()):
                        take_rank(r)
                    for hook in hooks.get(m, ()):
                        hook()
            return carry

        rank = {q: r for r, q in enumerate(reversed(QS))}

        def sources_of(k, phase):
            d = order_of(k)[2 - phase]
            later = order_of(k)[3 - phase:]
            return sorted((q for q in range(1, 8) if q & d and not any(q & e for e in later)), key=rank.get)

        def take_rank(r, phase=0):
            for k in parts:
                take(sources_of(k, phase)[r], k)

        lax.fori_loop(0, 8, body, 0)
        for step in tail:
            if step is None:
                pair_sum(0)
            elif isinstance(step, str):
                for hook in hooks[step]:
                    hook()
            else:
                take_rank(step[1], step[0])
        for count, sem, rel in ((7, ici_send, 2), (8, d2d_send, 1)):
            sent = con.at[pl.ds(0, count), pl.ds(0, rows), :]
            rcopy(sent, sent, sem, recv.at[0], rel).wait_send()

    reduce_pass(gt, CLS_PAD, Y_CHUNKS, part2, rb2, recv_a, d2d_a, {5: [0], 6: [1], 7: [2]}, [None, (1, 0), (0, 3), (1, 1), (2, 0)], {})
    d2t = con[0, 0:CLS_PAD, :].astype(BF16)
    gwo = jnp.dot(d2t, hid[...], preferred_element_type=F32)
    et[...] = jnp.where(z1t[...] > 0, dot_first(wos[...], d2t), 0.0).astype(BF16)
    row_id = lax.broadcasted_iota(jnp.int32, (CLS_PAD, HID), 0)
    gwos[...] = jnp.where(row_id == CLS, lossv[...], gwo)

    core = coords[0]

    def all_sum(rows, total_rows, src, halves, other, own, gathered, final, send, recv):
        def prepare():
            halves[0] = src[0:rows, :]
            halves[1, 0:total_rows - rows, :] = src[rows:total_rows, :]
            if total_rows < 2 * rows:
                halves[1, total_rows - rows:rows, :] = jnp.zeros((2 * rows - total_rows, HID), F32)

        pair = rcopy(halves.at[1 - core], other, send.at[0], recv.at[0], 1)
        sends = [rcopy(gathered.at[0], gathered.at[q], send.at[1], recv.at[q], 2 * q) for q in range(1, 8)]
        back = rcopy(own, final, send.at[2], recv.at[8], 1)

        def start():
            prepare()
            pair.start()

        def spread():
            pair.wait()
            gathered[0] = halves[core] + other[...]
            for q in (7, 6, 5, 3, 4, 2, 1):
                sends[q - 1].start()

        def collect():
            for cp in sends:
                cp.wait_recv()
            rcopy(gathered.at[pl.ds(0, 7)], gathered.at[pl.ds(0, 7)], send.at[1], recv.at[0], 2).wait_send()
            g = gathered
            own[...] = ((g[0] + g[1]) + (g[2] + g[3])) + ((g[4] + g[5]) + (g[6] + g[7]))
            back.start()

        def finish():
            halves[core] = own[...]
            back.wait()
            halves[1 - core] = final[...]

        return start, spread, collect, finish

    gwo_start, gwo_spread, gwo_collect, gwo_finish = all_sum(GWO_HALF, CLS_PAD, gwos, gwop, gwof.at[0], gwor, gwog,
                                                             gwof.at[1], gwo_send, gwo_recv)
    gwh_start, gwh_spread, gwh_collect, gwh_finish = all_sum(GWH_HALF, F_PAD, gwhs, gwhp, gwhf.at[0], gwhr, gwhg,
                                                             gwhf.at[1], gwh_send, gwh_recv)
    gwo_start()

    def gwo_out():
        gwo_finish()
        out_ref[F_PAD:F_PAD + GWO_HALF, :] = gwop[0]
        out_ref[F_PAD + GWO_HALF:OUT_ROWS, :] = gwop[1]
        loss = jnp.sum(gwop[1, GWO_HALF - 1:GWO_HALF, :], axis=1, keepdims=True) / label_count
        out_ref[OUT_ROWS - 1:OUT_ROWS, :] = jnp.broadcast_to(loss, (1, HID))

    reduce_pass(et, HID, D1_CHUNKS, part1, rb1, recv_b, d2d_b, {},
                [(0, 0), (0, 1), (0, 2), 'mid', None, (0, 3), (1, 0), (1, 1), 'late', (2, 0)],
                {0: [gwo_spread], 'mid': [gwo_collect], 'late': [gwo_out]})
    gwhs[...] = dot_last(xall[0], con[0].astype(BF16))
    gwh_start()
    gwh_spread()
    gwh_collect()
    gwh_finish()
    out_ref[0:GWH_HALF, :] = gwhp[0]
    out_ref[GWH_HALF:F_PAD, :] = gwhp[1, 0:F_PAD - GWH_HALF, :]


def split_kernel(sums_ref, gwh_ref, gwot_ref, loss_ref):
    gwh_ref[...] = sums_ref[0:F_IN, :]
    gwot_ref[...] = sums_ref[F_PAD:F_PAD + CLS, :]
    loss_ref[...] = sums_ref[OUT_ROWS - 1:OUT_ROWS, 0:1]


def device_step(adj_rows, feat_rows, w_hidden, w_output, labels, train_mask, block_mask):
    dma = pltpu.SemaphoreType.DMA
    vmem = pl.BlockSpec(memory_space=pltpu.VMEM)
    hbm = pl.BlockSpec(memory_space=pl.ANY)
    sums = pl.pallas_call(
        step_kernel,
        name='gcn_step',
        out_shape=pltpu.VMEM((OUT_ROWS, HID), F32),
        in_specs=[hbm] * 7,
        out_specs=vmem,
        scratch_shapes=[
            pltpu.VMEM((F_IN, BLK), BF16),
            pltpu.VMEM((F_IN, HID), F32),
            pltpu.VMEM((CLS, HID), F32),
            pltpu.VMEM((1, BLK), jnp.int32),
            pltpu.VMEM((1, BLK), jnp.int32),
            pltpu.SMEM((NB, NB), jnp.int32),
            pltpu.VMEM((NB, BLK, BLK), BF16),
            pltpu.VMEM((NB, F_PAD, BLK), BF16),
            pltpu.VMEM((NB, CLS_PAD, BLK), BF16),
            pltpu.VMEM((2, HID, BLK), BF16),
            pltpu.VMEM((BLK, HID), F32),
            pltpu.VMEM((HID, BLK), F32),
            pltpu.VMEM((BLK, CLS_PAD), F32),
            pltpu.VMEM((CLS_PAD, BLK), F32),
            pltpu.VMEM((2, BLK, M_TILE), BF16),
            pltpu.VMEM((BLK, HID), BF16),
            pltpu.VMEM((CLS_PAD, BLK), BF16),
            pltpu.VMEM((HID, BLK), BF16),
            pltpu.VMEM((NB, HID, BLK), F32),
            pltpu.VMEM((8, CLS_PAD, BLK), F32),
            pltpu.VMEM((8, HID, BLK), F32),
            pltpu.VMEM((7, CLS_PAD, BLK), F32),
            pltpu.VMEM((7, HID, BLK), F32),
            pltpu.VMEM((F_PAD, HID), BF16),
            pltpu.VMEM((CLS_PAD, HID), BF16),
            pltpu.VMEM((16, BLK), F32),
            pltpu.VMEM((1, 128), F32),
            pltpu.VMEM((CLS_PAD, HID), F32),
            pltpu.VMEM((2, GWO_HALF, HID), F32),
            pltpu.VMEM((GWO_HALF, HID), F32),
            pltpu.VMEM((8, GWO_HALF, HID), F32),
            pltpu.VMEM((2, GWO_HALF, HID), F32),
            pltpu.VMEM((F_PAD, HID), F32),
            pltpu.VMEM((2, GWH_HALF, HID), F32),
            pltpu.VMEM((GWH_HALF, HID), F32),
            pltpu.VMEM((8, GWH_HALF, HID), F32),
            pltpu.VMEM((2, GWH_HALF, HID), F32),
            dma((6,)), dma((NB,)), dma, dma, dma((42,)), dma((11,)), dma((42,)), dma((11,)),
            dma((3,)), dma((9,)), dma((3,)), dma((9,)),
        ],
        compiler_params=pltpu.CompilerParams(collective_id=0, has_side_effects=True, vmem_limit_bytes=64000000),
    )(adj_rows, feat_rows.T, w_hidden, w_output.T, labels[None, :], train_mask[None, :], block_mask)
    gwh, gwot, loss = pl.pallas_call(
        split_kernel,
        name='split_sums',
        out_shape=(jax.ShapeDtypeStruct((F_IN, HID), F32), jax.ShapeDtypeStruct((CLS, HID), F32),
                   jax.ShapeDtypeStruct((1, 1), F32)),
        in_specs=[vmem],
        out_specs=(vmem, vmem, vmem),
    )(pltpu.with_memory_space_constraint(sums, pltpu.VMEM))
    return loss[0, 0], gwh, gwot.T


def solution(mesh):
    row_spec = P(AXIS_NAME, None)
    vec_spec = P(AXIS_NAME)
    return jax.shard_map(device_step, mesh=mesh, in_specs=(row_spec, row_spec, P(), P(), vec_spec, vec_spec, P()), out_specs=(P(), P(), P()), check_vma=False)
```

```python
import jax
import jax.numpy as jnp
from jax import lax
from jax.experimental import pallas as pl
from jax.experimental.pallas import tpu as pltpu
from jax.sharding import PartitionSpec as P

AXIS_NAME = 'nodes'
MESH = pl.DeviceIdType.MESH
F32, BF16 = jnp.float32, jnp.bfloat16
BLK = 1024
NB = 16
F_IN, F_PAD = 100, 104
HID = 128
CLS, CLS_PAD = 47, 48
QS = [0, 2, 4, 1, 3, 6, 5, 7]
QI = {q: i for i, q in enumerate(QS)}
ORDERS = [(1, 2, 4), (2, 4, 1), (4, 1, 2)]
X_CHUNKS = [(0, 40, 0, BLK, 0), (40, 32, 0, BLK, 1), (72, 32, 0, BLK, 2)]
Y_CHUNKS = [(0, 16, 0, BLK, 0), (16, 16, 0, BLK, 1), (32, 16, 0, BLK, 2)]
D1_CHUNKS = [(0, 40, 0, BLK, 0), (40, 40, 0, BLK, 1), (80, 40, 0, BLK, 2),
             (120, 8, 0, 384, 0), (120, 8, 384, 384, 1), (120, 8, 768, 256, 2)]
GWO_HALF, GWH_HALF = 24, 56
OUT_ROWS = F_PAD + CLS_PAD
M_TILE = 256
A_AHEAD = 5


def forwards(q, order_id, swapped):
    first, second, third = order = ORDERS[order_id]
    if order_id in swapped and q == first:
        return [(first, second)]
    if order_id in swapped and q == second:
        return [(second, third), (first, third)]
    return [(q, d) for d in order[1 + max(order.index(d) for d in order if q & d):]]


def last_dim(q, order_id):
    return max((d for d in ORDERS[order_id] if q & d), key=ORDERS[order_id].index)


def plan_gather(chunks, cost, max_group, swapped):
    sizes = [n * lanes * 0.002 for _, n, _, lanes, _ in chunks]
    link = {1: 0.0, 2: 0.0, 4: 0.0, 0: 0.0}
    ops, arrive, relayed, ready = [], {}, {}, [0]
    now = 0.0

    def send(table, key, dim, size):
        link[dim] = max(now, link[dim]) + size / (46.6 if dim else 600.0)
        table[key] = link[dim] + (2.3 if dim else 0.95)

    for j in range(3):
        for k, chunk in enumerate(chunks):
            d = ORDERS[chunk[4]][j]
            send(arrive, (d, k), d, sizes[k])
    send(relayed, 0, 0, sum(sizes))
    got = {q: 0 for q in range(8)}
    while arrive or relayed or ready:
        key = min(arrive, key=arrive.get, default=None)
        if key is not None and arrive[key] <= now:
            del arrive[key]
            q, k = key
            ops.append(('recv', q, k))
            for src, d in forwards(q, chunks[k][4], swapped):
                send(arrive, (src | d, k), d, sizes[k])
            got[q] += 1
            if got[q] == len(chunks):
                ops.append(('relay', q))
                send(relayed, q, 0, sum(sizes))
                ready.append(2 * QI[q])
            continue
        for q in sorted(relayed, key=relayed.get):
            if relayed[q] <= now:
                del relayed[q]
                ops.append(('take', q))
                ready.append(2 * QI[q] + 1)
        if ready:
            ops.append(('dot', ready[:max_group]))
            now += cost(len(ready[:max_group]))
            ready = ready[max_group:]
        else:
            now = min(list(arrive.values()) + list(relayed.values()))
    return ops


def dot_last(lhs, rhs):
    return lax.dot_general(lhs, rhs, (((1,), (1,)), ((), ())), preferred_element_type=F32)


def dot_first(lhs, rhs):
    return lax.dot_general(lhs, rhs, (((0,), (0,)), ((), ())), preferred_element_type=F32)


def step_kernel(adj_hbm, x_hbm, wh_hbm, wot_hbm, lab_hbm, msk_hbm, bm_hbm, out_ref,
                x_ref, wh_ref, wot_ref, lab_ref, msk_ref, bm_ref,
                adj, xall, yall, y1b, z1, z1t, z2, z2t, turned, hid, gt, et, con, part2, part1, rb2, rb1, whs, wos, macc, lossv,
                gwos, gwop, gwor, gwog, gwof, gwhs, gwhp, gwhr, gwhg, gwhf,
                io_sem, a_sem, ici_send, d2d_send, recv_a, d2d_a, recv_b, d2d_b,
                gwo_send, gwo_recv, gwh_send, gwh_recv):
    me = lax.axis_index(AXIS_NAME)
    coords = [me % 2, (me // 2) % 2, (me // 4) % 2, me // 8]

    def dev(rel):
        total = 0
        for bit in range(4):
            total = total + ((coords[bit] + ((rel >> bit) & 1)) % 2) * (1 << bit)
        return total

    def rel_of(slot):
        return 2 * QS[slot // 2] + slot % 2

    def rcopy(src, dst, send_sem, recv_sem, rel):
        return pltpu.make_async_remote_copy(src_ref=src, dst_ref=dst, send_sem=send_sem, recv_sem=recv_sem,
                                            device_id=(dev(rel),), device_id_type=MESH)

    def a_copy(slot, blk=0):
        return pltpu.make_async_copy(adj_hbm.at[:, pl.ds(pl.multiple_of(blk * BLK, BLK), BLK)], adj.at[slot], a_sem.at[slot])

    plan1 = plan_gather(X_CHUNKS, lambda n: 0.2 + 0.54 * n, 2, (2,))
    a_order = [slot for op in plan1 if op[0] == 'dot' for slot in op[1]]

    def start_a(lo, hi):
        for slot in a_order[lo:hi]:
            a_copy(slot, dev(rel_of(slot))).start()

    loads = [pltpu.make_async_copy(src, dst, io_sem.at[n]) for n, (src, dst) in enumerate(
        [(x_hbm, x_ref), (wh_hbm, wh_ref), (wot_hbm, wot_ref), (lab_hbm, lab_ref), (msk_hbm, msk_ref), (bm_hbm, bm_ref)])]
    barrier = pltpu.get_barrier_semaphore()
    peers = [1, 2, 4, 8]
    for rel in peers:
        pl.semaphore_signal(barrier, inc=1, device_id=(dev(rel),), device_id_type=MESH)

    for load in loads:
        load.start()
    start_a(0, A_AHEAD)
    macc[...] = jnp.zeros_like(macc)
    z1[...] = jnp.zeros_like(z1)
    z2[...] = jnp.zeros_like(z2)
    z2t[...] = jnp.zeros_like(z2t)
    whs[...] = jnp.zeros_like(whs)
    wos[...] = jnp.zeros_like(wos)
    for load in loads:
        load.wait()
    xall[0, 0:F_PAD - 8, :] = x_ref[0:F_PAD - 8, :]
    xall[0, F_PAD - 8:F_PAD, :] = jnp.concatenate([x_ref[F_PAD - 8:F_IN, :], jnp.zeros((F_PAD - F_IN, BLK), BF16)], axis=0)
    whs[0:F_IN, :] = wh_ref[...].astype(BF16)
    wos[0:CLS, :] = wot_ref[...].astype(BF16)
    pl.semaphore_wait(barrier, len(peers))

    def mask_of(slot):
        if isinstance(slot, int):
            return bm_ref[me, dev(rel_of(slot))]
        i = slot // 2
        c = slot % 2
        bits = []
        for bit in (1, 2, 4):
            b = 0
            for pos, q in enumerate(QS):
                if q & bit:
                    d = (i - pos) * (i - pos)
                    b = b + 1 // (1 + d)
            bits.append(b)
        total = ((coords[0] + c) % 2)
        for n, b in enumerate(bits):
            total = total + ((coords[n + 1] + b) % 2) * (2 << n)
        return bm_ref[me, total]


    def gather_product(buf, chunks, recv, recv_d2d, ops, swapped, first, dots):
        def ici(src_q, dim, k):
            dst_q = src_q ^ dim
            lo, n, lane, lanes, _ = chunks[k]
            return rcopy(buf.at[2 * QI[src_q], pl.ds(lo, n), pl.ds(lane, lanes)],
                         buf.at[2 * QI[dst_q], pl.ds(lo, n), pl.ds(lane, lanes)],
                         ici_send, recv.at[k * 7 + QI[dst_q] - 1], 2 * dim)

        def relay(q):
            return rcopy(buf.at[2 * QI[q]], buf.at[2 * QI[q] + 1], d2d_send, recv_d2d.at[QI[q]], 1)

        for j in range(3):
            for k, chunk in enumerate(chunks):
                ici(0, ORDERS[chunk[4]][j], k).start()
        relay(0).start()
        first()
        for op, q, *k in ops:
            if op == 'dot':
                dots(q)
            elif op == 'take':
                relay(q).wait_recv()
            elif op == 'relay':
                relay(q).start()
            else:
                order_id = chunks[k[0]][4]
                d = last_dim(q, order_id)
                ici(q ^ d, d, k[0]).wait_recv()
                for src, d in forwards(q, order_id, swapped):
                    ici(src, d, k[0]).start()
        for count, sem, rel in ((7, ici_send, 2), (8, d2d_send, 1)):
            sent = buf.at[pl.ds(0, count)]
            rcopy(sent, sent, sem, recv.at[0], rel).wait_send()

    def accumulate(out, slots, blocks):
        for lo in range(0, BLK, M_TILE):
            acc = out[lo:lo + M_TILE, :]
            for slot, block in zip(slots, blocks):
                acc = acc + dot_last(adj[slot, lo:lo + M_TILE, :], block)
            out[lo:lo + M_TILE, :] = acc

    def dots1(slots):
        for slot in slots:
            a_copy(slot).wait()
            ahead = a_order.index(slot) + A_AHEAD
            start_a(ahead, ahead + 1)
        for j, slot in enumerate(slots):
            yt = dot_first(whs[...], xall[slot]).astype(BF16)
            y1b[j] = (yt.astype(F32) * mask_of(slot).astype(F32)).astype(BF16)
        accumulate(z1, slots, [y1b[j] for j in range(len(slots))])

    gather_product(xall, X_CHUNKS, recv_a, d2d_a, plan1, (2,), lambda: None, dots1)

    cls_id = lax.broadcasted_iota(jnp.int32, (CLS_PAD, BLK), 0)
    weight = msk_ref[...].astype(F32)
    hid[...] = jnp.maximum(z1[...], 0.0).astype(BF16)
    yall[0] = jnp.where(cls_id == CLS, weight, dot_last(wos[...], hid[...])).astype(BF16)

    def dots2(slots):
        blocks = []
        for slot in slots:
            macc[...] += yall[slot, CLS_PAD - 16:CLS_PAD, :].astype(F32)
            blocks.append((yall[slot].astype(F32) * mask_of(slot).astype(F32)).astype(BF16))
        if len(slots) == 1:
            accumulate(z2, slots, blocks)
            return
        stream, held = slots
        turned[0] = jnp.transpose(adj[held, 0:M_TILE, :])
        for n in range(BLK // M_TILE):
            tile = slice(M_TILE * n, M_TILE * (n + 1))
            if n + 1 < BLK // M_TILE:
                turned[(n + 1) % 2] = jnp.transpose(adj[held, M_TILE * (n + 1):M_TILE * (n + 2), :])
            z2[tile, :] += dot_last(adj[stream, tile, :], blocks[0])
            z2t[:, tile] += jnp.dot(blocks[1], turned[n % 2], preferred_element_type=F32)

    def keep_sign():
        z1t[...] = jnp.transpose(z1[...])

    plan2 = plan_gather(Y_CHUNKS, lambda n: 0.43 + 0.25 * n, 2, (0, 1))
    gather_product(yall, Y_CHUNKS, recv_b, d2d_b, plan2, (0, 1), keep_sign, dots2)
    label_count = jnp.sum(macc[15:16, :])

    zt = jnp.transpose(z2[...]) + z2t[...]
    valid = cls_id < CLS
    top = jnp.max(jnp.where(valid, zt, -jnp.inf), axis=0, keepdims=True)
    expz = jnp.where(valid, jnp.exp(zt - top), 0.0)
    log_norm = jnp.log(jnp.sum(expz, axis=0, keepdims=True)) + top
    one_hot = cls_id == lab_ref[...]
    picked = jnp.sum(jnp.where(one_hot, zt, 0.0), axis=0, keepdims=True)
    loss_terms = weight * (log_norm - picked)
    acc = loss_terms[:, 0:128]
    for n in range(1, BLK // 128):
        acc = acc + loss_terms[:, 128 * n:128 * (n + 1)]
    lossv[...] = acc
    prob = jnp.exp(zt - log_norm)
    grad = (prob - one_hot.astype(F32)) * (weight / label_count)
    gt[...] = jnp.where(valid, grad, 0.0).astype(BF16)


    def reduce_pass(lhs_ref, rows, chunks, part, rb, recv, recv_d2d, early, tail, hooks):
        parts = range(len(chunks))

        def order_of(k):
            return ORDERS[chunks[k][4]]

        def dim_of(q, k):
            return next(d for d in reversed(order_of(k)) if q & d)

        def ici(q, k):
            lo, n, lane, lanes, _ = chunks[k]
            idx = k * 7 + QI[q] - 1
            return rcopy(con.at[2 * QI[q], pl.ds(lo, n), pl.ds(lane, lanes)],
                         rb.at[QI[q] - 1, pl.ds(lo, n), pl.ds(lane, lanes)], ici_send,
                         recv.at[idx], 2 * dim_of(q, k))

        def d2d(i):
            return rcopy(con.at[2 * i + 1, pl.ds(0, rows), :], part.at[i], d2d_send, recv_d2d.at[i], 1)

        cuts = [chunks[0][0], chunks[1][0], chunks[2][0], rows]

        def d2d_part(p):
            span = pl.ds(cuts[p], cuts[p + 1] - cuts[p])
            return rcopy(con.at[15, span, :], part.at[7, span, :], d2d_send, recv_d2d.at[8 + p if p else 7], 1)

        def sources(q, k):
            out = []
            for d in reversed(order_of(k)):
                if q & d:
                    break
                out.append(q ^ d)
            return out

        def compute(slot):
            lhs = (lhs_ref[...].astype(F32) * mask_of(slot).astype(F32)).astype(BF16)
            con[slot, 0:rows, :] = jnp.dot(lhs, adj[slot], preferred_element_type=F32)

        waiting = {(q, k): set(sources(q, k)) for q in range(8) for k in parts}

        def pair_sum(q):
            i = QI[q]
            for p in range(3) if i == 7 else [None]:
                lo, hi = (0, rows) if p is None else (cuts[p], cuts[p + 1])
                (d2d(i) if p is None else d2d_part(p)).wait_recv()
                con[2 * i, lo:hi, :] += part[i, lo:hi, :]
                for k in parts:
                    if q and not waiting[q, k] and lo <= chunks[k][0] < hi:
                        ici(q, k).start()

        def take(src, k):
            d = dim_of(src, k)
            q = src ^ d
            lo, n, lane, lanes, _ = chunks[k]
            ici(src, k).wait_recv()
            con[2 * QI[q], lo:lo + n, lane:lane + lanes] += rb[QI[src] - 1, lo:lo + n, lane:lane + lanes]
            waiting[q, k].discard(src)
            if q and not waiting[q, k]:
                ici(q, k).start()

        def body(n, carry):
            i = 7 - n
            compute(2 * i + 1)

            @pl.when(n == 0)
            def _():
                for p in range(3):
                    d2d_part(p).start()

            @pl.when(n > 0)
            def _():
                d2d(i).start()

            compute(2 * i)
            for m in range(8):
                @pl.when(n == m)
                def _(m=m):
                    if m:
                        pair_sum(QS[8 - m])
                    for r in early.get(m, ()):
                        take_rank(r)
                    for hook in hooks.get(m, ()):
                        hook()
            return carry

        rank = {q: r for r, q in enumerate(reversed(QS))}

        def sources_of(k, phase):
            d = order_of(k)[2 - phase]
            later = order_of(k)[3 - phase:]
            return sorted((q for q in range(1, 8) if q & d and not any(q & e for e in later)), key=rank.get)

        def take_rank(r, phase=0):
            for k in parts:
                take(sources_of(k, phase)[r], k)

        lax.fori_loop(0, 8, body, 0)
        for step in tail:
            if step is None:
                pair_sum(0)
            elif isinstance(step, str):
                for hook in hooks[step]:
                    hook()
            else:
                take_rank(step[1], step[0])
        for count, sem, rel in ((7, ici_send, 2), (8, d2d_send, 1)):
            sent = con.at[pl.ds(0, count), pl.ds(0, rows), :]
            rcopy(sent, sent, sem, recv.at[0], rel).wait_send()

    reduce_pass(gt, CLS_PAD, Y_CHUNKS, part2, rb2, recv_a, d2d_a, {5: [0], 6: [1], 7: [2]}, [None, (1, 0), (0, 3), (1, 1), (2, 0)], {})
    d2t = con[0, 0:CLS_PAD, :].astype(BF16)
    gwo = jnp.dot(d2t, hid[...], preferred_element_type=F32)
    et[...] = jnp.where(z1t[...] > 0, dot_first(wos[...], d2t), 0.0).astype(BF16)
    row_id = lax.broadcasted_iota(jnp.int32, (CLS_PAD, HID), 0)
    gwos[...] = jnp.where(row_id == CLS, lossv[...], gwo)

    core = coords[0]

    def all_sum(rows, total_rows, src, halves, other, own, gathered, final, send, recv):
        def prepare():
            halves[0] = src[0:rows, :]
            halves[1, 0:total_rows - rows, :] = src[rows:total_rows, :]
            if total_rows < 2 * rows:
                halves[1, total_rows - rows:rows, :] = jnp.zeros((2 * rows - total_rows, HID), F32)

        pair = rcopy(halves.at[1 - core], other, send.at[0], recv.at[0], 1)
        sends = [rcopy(gathered.at[0], gathered.at[q], send.at[1], recv.at[q], 2 * q) for q in range(1, 8)]
        back = rcopy(own, final, send.at[2], recv.at[8], 1)

        def start():
            prepare()
            pair.start()

        def spread():
            pair.wait()
            gathered[0] = halves[core] + other[...]
            for q in (7, 6, 5, 3, 4, 2, 1):
                sends[q - 1].start()

        def collect():
            for cp in sends:
                cp.wait_recv()
            rcopy(gathered.at[pl.ds(0, 7)], gathered.at[pl.ds(0, 7)], send.at[1], recv.at[0], 2).wait_send()
            g = gathered
            own[...] = ((g[0] + g[1]) + (g[2] + g[3])) + ((g[4] + g[5]) + (g[6] + g[7]))
            back.start()

        def finish():
            halves[core] = own[...]
            back.wait()
            halves[1 - core] = final[...]

        return start, spread, collect, finish

    gwo_start, gwo_spread, gwo_collect, gwo_finish = all_sum(GWO_HALF, CLS_PAD, gwos, gwop, gwof.at[0], gwor, gwog,
                                                             gwof.at[1], gwo_send, gwo_recv)
    gwh_start, gwh_spread, gwh_collect, gwh_finish = all_sum(GWH_HALF, F_PAD, gwhs, gwhp, gwhf.at[0], gwhr, gwhg,
                                                             gwhf.at[1], gwh_send, gwh_recv)
    gwo_start()

    def gwo_out():
        gwo_finish()
        out_ref[F_PAD:F_PAD + GWO_HALF, :] = gwop[0]
        out_ref[F_PAD + GWO_HALF:OUT_ROWS, :] = gwop[1]
        loss = jnp.sum(gwop[1, GWO_HALF - 1:GWO_HALF, :], axis=1, keepdims=True) / label_count
        out_ref[OUT_ROWS - 1:OUT_ROWS, :] = jnp.broadcast_to(loss, (1, HID))

    reduce_pass(et, HID, D1_CHUNKS, part1, rb1, recv_b, d2d_b, {},
                [(0, 0), (0, 1), (0, 2), 'mid', None, (0, 3), (1, 0), (1, 1), 'late', (2, 0)],
                {0: [gwo_spread], 'mid': [gwo_collect], 'late': [gwo_out]})
    gwhs[...] = dot_last(xall[0], con[0].astype(BF16))
    gwh_start()
    gwh_spread()
    gwh_collect()
    gwh_finish()
    out_ref[0:GWH_HALF, :] = gwhp[0]
    out_ref[GWH_HALF:F_PAD, :] = gwhp[1, 0:F_PAD - GWH_HALF, :]


def split_kernel(sums_ref, gwh_ref, gwot_ref, loss_ref):
    gwh_ref[...] = sums_ref[0:F_IN, :]
    gwot_ref[...] = sums_ref[F_PAD:F_PAD + CLS, :]
    loss_ref[...] = sums_ref[OUT_ROWS - 1:OUT_ROWS, 0:1]


def device_step(adj_rows, feat_rows, w_hidden, w_output, labels, train_mask, block_mask):
    dma = pltpu.SemaphoreType.DMA
    vmem = pl.BlockSpec(memory_space=pltpu.VMEM)
    hbm = pl.BlockSpec(memory_space=pl.ANY)
    sums = pl.pallas_call(
        step_kernel,
        name='gcn_step',
        out_shape=pltpu.VMEM((OUT_ROWS, HID), F32),
        in_specs=[hbm] * 7,
        out_specs=vmem,
        scratch_shapes=[
            pltpu.VMEM((F_IN, BLK), BF16),
            pltpu.VMEM((F_IN, HID), F32),
            pltpu.VMEM((CLS, HID), F32),
            pltpu.VMEM((1, BLK), jnp.int32),
            pltpu.VMEM((1, BLK), jnp.int32),
            pltpu.SMEM((NB, NB), jnp.int32),
            pltpu.VMEM((NB, BLK, BLK), BF16),
            pltpu.VMEM((NB, F_PAD, BLK), BF16),
            pltpu.VMEM((NB, CLS_PAD, BLK), BF16),
            pltpu.VMEM((2, HID, BLK), BF16),
            pltpu.VMEM((BLK, HID), F32),
            pltpu.VMEM((HID, BLK), F32),
            pltpu.VMEM((BLK, CLS_PAD), F32),
            pltpu.VMEM((CLS_PAD, BLK), F32),
            pltpu.VMEM((2, BLK, M_TILE), BF16),
            pltpu.VMEM((BLK, HID), BF16),
            pltpu.VMEM((CLS_PAD, BLK), BF16),
            pltpu.VMEM((HID, BLK), BF16),
            pltpu.VMEM((NB, HID, BLK), F32),
            pltpu.VMEM((8, CLS_PAD, BLK), F32),
            pltpu.VMEM((8, HID, BLK), F32),
            pltpu.VMEM((7, CLS_PAD, BLK), F32),
            pltpu.VMEM((7, HID, BLK), F32),
            pltpu.VMEM((F_PAD, HID), BF16),
            pltpu.VMEM((CLS_PAD, HID), BF16),
            pltpu.VMEM((16, BLK), F32),
            pltpu.VMEM((1, 128), F32),
            pltpu.VMEM((CLS_PAD, HID), F32),
            pltpu.VMEM((2, GWO_HALF, HID), F32),
            pltpu.VMEM((GWO_HALF, HID), F32),
            pltpu.VMEM((8, GWO_HALF, HID), F32),
            pltpu.VMEM((2, GWO_HALF, HID), F32),
            pltpu.VMEM((F_PAD, HID), F32),
            pltpu.VMEM((2, GWH_HALF, HID), F32),
            pltpu.VMEM((GWH_HALF, HID), F32),
            pltpu.VMEM((8, GWH_HALF, HID), F32),
            pltpu.VMEM((2, GWH_HALF, HID), F32),
            dma((6,)), dma((NB,)), dma, dma, dma((21,)), dma((11,)), dma((42,)), dma((11,)),
            dma((3,)), dma((9,)), dma((3,)), dma((9,)),
        ],
        compiler_params=pltpu.CompilerParams(collective_id=0, has_side_effects=True, vmem_limit_bytes=64000000),
    )(adj_rows, feat_rows.T, w_hidden, w_output.T, labels[None, :], train_mask[None, :], block_mask)
    gwh, gwot, loss = pl.pallas_call(
        split_kernel,
        name='split_sums',
        out_shape=(jax.ShapeDtypeStruct((F_IN, HID), F32), jax.ShapeDtypeStruct((CLS, HID), F32),
                   jax.ShapeDtypeStruct((1, 1), F32)),
        in_specs=[vmem],
        out_specs=(vmem, vmem, vmem),
    )(pltpu.with_memory_space_constraint(sums, pltpu.VMEM))
    return loss[0, 0], gwh, gwot.T


def solution(mesh):
    row_spec = P(AXIS_NAME, None)
    vec_spec = P(AXIS_NAME)
    return jax.shard_map(device_step, mesh=mesh, in_specs=(row_spec, row_spec, P(), P(), vec_spec, vec_spec, P()), out_specs=(P(), P(), P()), check_vma=False)
```

```python
import jax
import jax.numpy as jnp
from jax import lax
from jax.experimental import pallas as pl
from jax.experimental.pallas import tpu as pltpu
from jax.sharding import PartitionSpec as P

AXIS_NAME = 'nodes'
MESH = pl.DeviceIdType.MESH
F32, BF16 = jnp.float32, jnp.bfloat16
BLK = 1024
NB = 16
F_IN, F_PAD = 100, 104
HID = 128
CLS, CLS_PAD = 47, 48
QS = [0, 2, 4, 1, 3, 6, 5, 7]
QI = {q: i for i, q in enumerate(QS)}
ORDERS = [(1, 2, 4), (2, 4, 1), (4, 1, 2)]
X_CHUNKS = [(0, 40, 0, BLK, 0), (40, 32, 0, BLK, 1), (72, 32, 0, BLK, 2)]
Y_CHUNKS = [(0, 16, 0, BLK, 0), (16, 16, 0, BLK, 1), (32, 16, 0, BLK, 2)]
D1_CHUNKS = [(0, 40, 0, BLK, 0), (40, 40, 0, BLK, 1), (80, 40, 0, BLK, 2),
             (120, 8, 0, 384, 0), (120, 8, 384, 384, 1), (120, 8, 768, 256, 2)]
GWO_HALF, GWH_HALF = 24, 56
OUT_ROWS = F_PAD + CLS_PAD
M_TILE = 256
A_AHEAD = 5


def forwards(q, order_id, swapped):
    first, second, third = order = ORDERS[order_id]
    if order_id in swapped and q == first:
        return [(first, second)]
    if order_id in swapped and q == second:
        return [(second, third), (first, third)]
    return [(q, d) for d in order[1 + max(order.index(d) for d in order if q & d):]]


def last_dim(q, order_id):
    return max((d for d in ORDERS[order_id] if q & d), key=ORDERS[order_id].index)


def plan_gather(chunks, cost, max_group, swapped):
    sizes = [n * lanes * 0.002 for _, n, _, lanes, _ in chunks]
    link = {1: 0.0, 2: 0.0, 4: 0.0, 0: 0.0}
    ops, arrive, relayed, ready = [], {}, {}, [0]
    now = 0.0

    def send(table, key, dim, size):
        link[dim] = max(now, link[dim]) + size / (46.6 if dim else 600.0)
        table[key] = link[dim] + (2.3 if dim else 0.95)

    for j in range(3):
        for k, chunk in enumerate(chunks):
            d = ORDERS[chunk[4]][j]
            send(arrive, (d, k), d, sizes[k])
    send(relayed, 0, 0, sum(sizes))
    got = {q: 0 for q in range(8)}
    while arrive or relayed or ready:
        key = min(arrive, key=arrive.get, default=None)
        if key is not None and arrive[key] <= now:
            del arrive[key]
            q, k = key
            ops.append(('recv', q, k))
            for src, d in forwards(q, chunks[k][4], swapped):
                send(arrive, (src | d, k), d, sizes[k])
            got[q] += 1
            if got[q] == len(chunks):
                ops.append(('relay', q))
                send(relayed, q, 0, sum(sizes))
                ready.append(2 * QI[q])
            continue
        for q in sorted(relayed, key=relayed.get):
            if relayed[q] <= now:
                del relayed[q]
                ops.append(('take', q))
                ready.append(2 * QI[q] + 1)
        if ready:
            ops.append(('dot', ready[:max_group]))
            now += cost(len(ready[:max_group]))
            ready = ready[max_group:]
        else:
            now = min(list(arrive.values()) + list(relayed.values()))
    return ops


def dot_last(lhs, rhs):
    return lax.dot_general(lhs, rhs, (((1,), (1,)), ((), ())), preferred_element_type=F32)


def dot_first(lhs, rhs):
    return lax.dot_general(lhs, rhs, (((0,), (0,)), ((), ())), preferred_element_type=F32)


def step_kernel(adj_hbm, x_hbm, wh_hbm, wot_hbm, lab_hbm, msk_hbm, bm_hbm, out_ref,
                x_ref, wh_ref, wot_ref, lab_ref, msk_ref, bm_ref,
                adj, xall, yall, y1b, z1, z1t, z2, z2t, turned, hidt, gt, et, con, part2, part1, rb2, rb1, whs, wos, macc, lossv,
                gwos, gwop, gwor, gwog, gwof, gwhs, gwhp, gwhr, gwhg, gwhf,
                io_sem, a_sem, ici_send, d2d_send, recv_a, d2d_a, recv_b, d2d_b,
                gwo_send, gwo_recv, gwh_send, gwh_recv):
    me = lax.axis_index(AXIS_NAME)
    coords = [me % 2, (me // 2) % 2, (me // 4) % 2, me // 8]

    def dev(rel):
        total = 0
        for bit in range(4):
            total = total + ((coords[bit] + ((rel >> bit) & 1)) % 2) * (1 << bit)
        return total

    def rel_of(slot):
        return 2 * QS[slot // 2] + slot % 2

    def rcopy(src, dst, send_sem, recv_sem, rel):
        return pltpu.make_async_remote_copy(src_ref=src, dst_ref=dst, send_sem=send_sem, recv_sem=recv_sem,
                                            device_id=(dev(rel),), device_id_type=MESH)

    def a_copy(slot, blk=0):
        return pltpu.make_async_copy(adj_hbm.at[:, pl.ds(pl.multiple_of(blk * BLK, BLK), BLK)], adj.at[slot], a_sem.at[slot])

    plan1 = plan_gather(X_CHUNKS, lambda n: 0.42 + 0.32 * n, 2, (2,))
    a_order = [slot for op in plan1 if op[0] == 'dot' for slot in op[1]]

    def start_a(lo, hi):
        for slot in a_order[lo:hi]:
            a_copy(slot, dev(rel_of(slot))).start()

    loads = [pltpu.make_async_copy(src, dst, io_sem.at[n]) for n, (src, dst) in enumerate(
        [(x_hbm, x_ref), (wh_hbm, wh_ref), (wot_hbm, wot_ref), (lab_hbm, lab_ref), (msk_hbm, msk_ref), (bm_hbm, bm_ref)])]
    barrier = pltpu.get_barrier_semaphore()
    peers = [1, 2, 4, 8]
    for rel in peers:
        pl.semaphore_signal(barrier, inc=1, device_id=(dev(rel),), device_id_type=MESH)

    for load in loads:
        load.start()
    start_a(0, A_AHEAD)
    macc[...] = jnp.zeros_like(macc)
    z1[...] = jnp.zeros_like(z1)
    z1t[...] = jnp.zeros_like(z1t)
    z2[...] = jnp.zeros_like(z2)
    z2t[...] = jnp.zeros_like(z2t)
    whs[...] = jnp.zeros_like(whs)
    wos[...] = jnp.zeros_like(wos)
    for load in loads:
        load.wait()
    xall[0, 0:F_PAD - 8, :] = x_ref[0:F_PAD - 8, :]
    xall[0, F_PAD - 8:F_PAD, :] = jnp.concatenate([x_ref[F_PAD - 8:F_IN, :], jnp.zeros((F_PAD - F_IN, BLK), BF16)], axis=0)
    whs[0:F_IN, :] = wh_ref[...].astype(BF16)
    wos[0:CLS, :] = wot_ref[...].astype(BF16)
    pl.semaphore_wait(barrier, len(peers))

    def mask_of(slot):
        if isinstance(slot, int):
            return bm_ref[me, dev(rel_of(slot))]
        i = slot // 2
        c = slot % 2
        bits = []
        for bit in (1, 2, 4):
            b = 0
            for pos, q in enumerate(QS):
                if q & bit:
                    d = (i - pos) * (i - pos)
                    b = b + 1 // (1 + d)
            bits.append(b)
        total = ((coords[0] + c) % 2)
        for n, b in enumerate(bits):
            total = total + ((coords[n + 1] + b) % 2) * (2 << n)
        return bm_ref[me, total]


    def gather_product(buf, chunks, recv, recv_d2d, ops, swapped, first, dots):
        def ici(src_q, dim, k):
            dst_q = src_q ^ dim
            lo, n, lane, lanes, _ = chunks[k]
            return rcopy(buf.at[2 * QI[src_q], pl.ds(lo, n), pl.ds(lane, lanes)],
                         buf.at[2 * QI[dst_q], pl.ds(lo, n), pl.ds(lane, lanes)],
                         ici_send, recv.at[k * 7 + QI[dst_q] - 1], 2 * dim)

        def relay(q):
            return rcopy(buf.at[2 * QI[q]], buf.at[2 * QI[q] + 1], d2d_send, recv_d2d.at[QI[q]], 1)

        for j in range(3):
            for k, chunk in enumerate(chunks):
                ici(0, ORDERS[chunk[4]][j], k).start()
        relay(0).start()
        first()
        for op, q, *k in ops:
            if op == 'dot':
                dots(q)
            elif op == 'take':
                relay(q).wait_recv()
            elif op == 'relay':
                relay(q).start()
            else:
                order_id = chunks[k[0]][4]
                d = last_dim(q, order_id)
                ici(q ^ d, d, k[0]).wait_recv()
                for src, d in forwards(q, order_id, swapped):
                    ici(src, d, k[0]).start()
        for count, sem, rel in ((7, ici_send, 2), (8, d2d_send, 1)):
            sent = buf.at[pl.ds(0, count)]
            rcopy(sent, sent, sem, recv.at[0], rel).wait_send()

    def products(out, out_t, slots, blocks):
        if len(slots) == 1:
            for lo in range(0, BLK, M_TILE):
                out[lo:lo + M_TILE, :] += dot_last(adj[slots[0], lo:lo + M_TILE, :], blocks[0])
            return
        stream, held = slots
        turned[0] = jnp.transpose(adj[held, 0:M_TILE, :])
        for n in range(BLK // M_TILE):
            tile = slice(M_TILE * n, M_TILE * (n + 1))
            if n + 1 < BLK // M_TILE:
                turned[(n + 1) % 2] = jnp.transpose(adj[held, M_TILE * (n + 1):M_TILE * (n + 2), :])
            out[tile, :] += dot_last(adj[stream, tile, :], blocks[0])
            out_t[:, tile] += jnp.dot(blocks[1], turned[n % 2], preferred_element_type=F32)

    def dots1(slots):
        for slot in slots:
            a_copy(slot).wait()
            ahead = a_order.index(slot) + A_AHEAD
            start_a(ahead, ahead + 1)
        for j, slot in enumerate(slots):
            yt = dot_first(whs[...], xall[slot]).astype(BF16)
            y1b[j] = (yt.astype(F32) * mask_of(slot).astype(F32)).astype(BF16)
        products(z1, z1t, slots, [y1b[j] for j in range(len(slots))])

    gather_product(xall, X_CHUNKS, recv_a, d2d_a, plan1, (2,), lambda: None, dots1)

    cls_id = lax.broadcasted_iota(jnp.int32, (CLS_PAD, BLK), 0)
    weight = msk_ref[...].astype(F32)
    z1t[...] += jnp.transpose(z1[...])
    hidt[...] = jnp.maximum(z1t[...], 0.0).astype(BF16)
    yall[0] = jnp.where(cls_id == CLS, weight, jnp.dot(wos[...], hidt[...], preferred_element_type=F32)).astype(BF16)

    def dots2(slots):
        blocks = []
        for slot in slots:
            macc[...] += yall[slot, CLS_PAD - 16:CLS_PAD, :].astype(F32)
            blocks.append((yall[slot].astype(F32) * mask_of(slot).astype(F32)).astype(BF16))
        products(z2, z2t, slots, blocks)

    plan2 = plan_gather(Y_CHUNKS, lambda n: 0.43 + 0.25 * n, 2, (0, 1))
    gather_product(yall, Y_CHUNKS, recv_b, d2d_b, plan2, (0, 1), lambda: None, dots2)
    label_count = jnp.sum(macc[15:16, :])

    zt = jnp.transpose(z2[...]) + z2t[...]
    valid = cls_id < CLS
    top = jnp.max(jnp.where(valid, zt, -jnp.inf), axis=0, keepdims=True)
    expz = jnp.where(valid, jnp.exp(zt - top), 0.0)
    log_norm = jnp.log(jnp.sum(expz, axis=0, keepdims=True)) + top
    one_hot = cls_id == lab_ref[...]
    picked = jnp.sum(jnp.where(one_hot, zt, 0.0), axis=0, keepdims=True)
    loss_terms = weight * (log_norm - picked)
    acc = loss_terms[:, 0:128]
    for n in range(1, BLK // 128):
        acc = acc + loss_terms[:, 128 * n:128 * (n + 1)]
    lossv[...] = acc
    prob = jnp.exp(zt - log_norm)
    grad = (prob - one_hot.astype(F32)) * (weight / label_count)
    gt[...] = jnp.where(valid, grad, 0.0).astype(BF16)


    def reduce_pass(lhs_ref, rows, chunks, part, rb, recv, recv_d2d, early, tail, hooks):
        parts = range(len(chunks))

        def order_of(k):
            return ORDERS[chunks[k][4]]

        def dim_of(q, k):
            return next(d for d in reversed(order_of(k)) if q & d)

        def ici(q, k):
            lo, n, lane, lanes, _ = chunks[k]
            idx = k * 7 + QI[q] - 1
            return rcopy(con.at[2 * QI[q], pl.ds(lo, n), pl.ds(lane, lanes)],
                         rb.at[QI[q] - 1, pl.ds(lo, n), pl.ds(lane, lanes)], ici_send,
                         recv.at[idx], 2 * dim_of(q, k))

        def d2d(i):
            return rcopy(con.at[2 * i + 1, pl.ds(0, rows), :], part.at[i], d2d_send, recv_d2d.at[i], 1)

        cuts = [chunks[0][0], chunks[1][0], chunks[2][0], rows]

        def d2d_part(p):
            span = pl.ds(cuts[p], cuts[p + 1] - cuts[p])
            return rcopy(con.at[15, span, :], part.at[7, span, :], d2d_send, recv_d2d.at[8 + p if p else 7], 1)

        def sources(q, k):
            out = []
            for d in reversed(order_of(k)):
                if q & d:
                    break
                out.append(q ^ d)
            return out

        def compute(slot):
            lhs = (lhs_ref[...].astype(F32) * mask_of(slot).astype(F32)).astype(BF16)
            con[slot, 0:rows, :] = jnp.dot(lhs, adj[slot], preferred_element_type=F32)

        waiting = {(q, k): set(sources(q, k)) for q in range(8) for k in parts}

        def pair_sum(q):
            i = QI[q]
            for p in range(3) if i == 7 else [None]:
                lo, hi = (0, rows) if p is None else (cuts[p], cuts[p + 1])
                (d2d(i) if p is None else d2d_part(p)).wait_recv()
                con[2 * i, lo:hi, :] += part[i, lo:hi, :]
                for k in parts:
                    if q and not waiting[q, k] and lo <= chunks[k][0] < hi:
                        ici(q, k).start()

        def take(src, k):
            d = dim_of(src, k)
            q = src ^ d
            lo, n, lane, lanes, _ = chunks[k]
            ici(src, k).wait_recv()
            con[2 * QI[q], lo:lo + n, lane:lane + lanes] += rb[QI[src] - 1, lo:lo + n, lane:lane + lanes]
            waiting[q, k].discard(src)
            if q and not waiting[q, k]:
                ici(q, k).start()

        def body(n, carry):
            i = 7 - n
            compute(2 * i + 1)

            @pl.when(n == 0)
            def _():
                for p in range(3):
                    d2d_part(p).start()

            @pl.when(n > 0)
            def _():
                d2d(i).start()

            compute(2 * i)
            for m in range(8):
                @pl.when(n == m)
                def _(m=m):
                    if m:
                        pair_sum(QS[8 - m])
                    for r in early.get(m, ()):
                        take_rank(r)
                    for hook in hooks.get(m, ()):
                        hook()
            return carry

        rank = {q: r for r, q in enumerate(reversed(QS))}

        def sources_of(k, phase):
            d = order_of(k)[2 - phase]
            later = order_of(k)[3 - phase:]
            return sorted((q for q in range(1, 8) if q & d and not any(q & e for e in later)), key=rank.get)

        def take_rank(r, phase=0):
            for k in parts:
                take(sources_of(k, phase)[r], k)

        lax.fori_loop(0, 8, body, 0)
        for step in tail:
            if step is None:
                pair_sum(0)
            elif isinstance(step, str):
                for hook in hooks[step]:
                    hook()
            else:
                take_rank(step[1], step[0])
        for count, sem, rel in ((7, ici_send, 2), (8, d2d_send, 1)):
            sent = con.at[pl.ds(0, count), pl.ds(0, rows), :]
            rcopy(sent, sent, sem, recv.at[0], rel).wait_send()

    reduce_pass(gt, CLS_PAD, Y_CHUNKS, part2, rb2, recv_a, d2d_a, {5: [0], 6: [1], 7: [2]}, [None, (1, 0), (0, 3), (1, 1), (2, 0)], {})
    d2t = con[0, 0:CLS_PAD, :].astype(BF16)
    gwo = dot_last(d2t, hidt[...])
    row_id = lax.broadcasted_iota(jnp.int32, (CLS_PAD, HID), 0)
    gwos[...] = jnp.where(row_id == CLS, lossv[...], gwo)

    core = coords[0]

    def all_sum(rows, total_rows, src, halves, other, own, gathered, final, send, recv):
        def prepare():
            halves[0] = src[0:rows, :]
            halves[1, 0:total_rows - rows, :] = src[rows:total_rows, :]
            if total_rows < 2 * rows:
                halves[1, total_rows - rows:rows, :] = jnp.zeros((2 * rows - total_rows, HID), F32)

        pair = rcopy(halves.at[1 - core], other, send.at[0], recv.at[0], 1)
        sends = [rcopy(gathered.at[0], gathered.at[q], send.at[1], recv.at[q], 2 * q) for q in range(1, 8)]
        back = rcopy(own, final, send.at[2], recv.at[8], 1)

        def start():
            prepare()
            pair.start()

        def spread():
            pair.wait()
            gathered[0] = halves[core] + other[...]
            for q in (7, 6, 5, 3, 4, 2, 1):
                sends[q - 1].start()

        def collect():
            for cp in sends:
                cp.wait_recv()
            rcopy(gathered.at[pl.ds(0, 7)], gathered.at[pl.ds(0, 7)], send.at[1], recv.at[0], 2).wait_send()
            g = gathered
            own[...] = ((g[0] + g[1]) + (g[2] + g[3])) + ((g[4] + g[5]) + (g[6] + g[7]))
            back.start()

        def finish():
            halves[core] = own[...]
            back.wait()
            halves[1 - core] = final[...]

        return start, spread, collect, finish

    gwo_start, gwo_spread, gwo_collect, gwo_finish = all_sum(GWO_HALF, CLS_PAD, gwos, gwop, gwof.at[0], gwor, gwog,
                                                             gwof.at[1], gwo_send, gwo_recv)
    gwh_start, gwh_spread, gwh_collect, gwh_finish = all_sum(GWH_HALF, F_PAD, gwhs, gwhp, gwhf.at[0], gwhr, gwhg,
                                                             gwhf.at[1], gwh_send, gwh_recv)
    gwo_start()
    et[...] = jnp.where(z1t[...] > 0, dot_first(wos[...], d2t), 0.0).astype(BF16)

    def gwo_out():
        gwo_finish()
        out_ref[F_PAD:F_PAD + GWO_HALF, :] = gwop[0]
        out_ref[F_PAD + GWO_HALF:OUT_ROWS, :] = gwop[1]
        loss = jnp.sum(gwop[1, GWO_HALF - 1:GWO_HALF, :], axis=1, keepdims=True) / label_count
        out_ref[OUT_ROWS - 1:OUT_ROWS, :] = jnp.broadcast_to(loss, (1, HID))

    reduce_pass(et, HID, D1_CHUNKS, part1, rb1, recv_b, d2d_b, {},
                [(0, 0), (0, 1), (0, 2), 'mid', None, (0, 3), (1, 0), (1, 1), 'late', (2, 0)],
                {0: [gwo_spread], 'mid': [gwo_collect], 'late': [gwo_out]})
    gwhs[...] = dot_last(xall[0], con[0].astype(BF16))
    gwh_start()
    gwh_spread()
    gwh_collect()
    gwh_finish()
    out_ref[0:GWH_HALF, :] = gwhp[0]
    out_ref[GWH_HALF:F_PAD, :] = gwhp[1, 0:F_PAD - GWH_HALF, :]


def split_kernel(sums_ref, gwh_ref, gwot_ref, loss_ref):
    gwh_ref[...] = sums_ref[0:F_IN, :]
    gwot_ref[...] = sums_ref[F_PAD:F_PAD + CLS, :]
    loss_ref[...] = sums_ref[OUT_ROWS - 1:OUT_ROWS, 0:1]


def device_step(adj_rows, feat_rows, w_hidden, w_output, labels, train_mask, block_mask):
    dma = pltpu.SemaphoreType.DMA
    vmem = pl.BlockSpec(memory_space=pltpu.VMEM)
    hbm = pl.BlockSpec(memory_space=pl.ANY)
    sums = pl.pallas_call(
        step_kernel,
        name='gcn_step',
        out_shape=pltpu.VMEM((OUT_ROWS, HID), F32),
        in_specs=[hbm] * 7,
        out_specs=vmem,
        scratch_shapes=[
            pltpu.VMEM((F_IN, BLK), BF16),
            pltpu.VMEM((F_IN, HID), F32),
            pltpu.VMEM((CLS, HID), F32),
            pltpu.VMEM((1, BLK), jnp.int32),
            pltpu.VMEM((1, BLK), jnp.int32),
            pltpu.SMEM((NB, NB), jnp.int32),
            pltpu.VMEM((NB, BLK, BLK), BF16),
            pltpu.VMEM((NB, F_PAD, BLK), BF16),
            pltpu.VMEM((NB, CLS_PAD, BLK), BF16),
            pltpu.VMEM((2, HID, BLK), BF16),
            pltpu.VMEM((BLK, HID), F32),
            pltpu.VMEM((HID, BLK), F32),
            pltpu.VMEM((BLK, CLS_PAD), F32),
            pltpu.VMEM((CLS_PAD, BLK), F32),
            pltpu.VMEM((2, BLK, M_TILE), BF16),
            pltpu.VMEM((HID, BLK), BF16),
            pltpu.VMEM((CLS_PAD, BLK), BF16),
            pltpu.VMEM((HID, BLK), BF16),
            pltpu.VMEM((NB, HID, BLK), F32),
            pltpu.VMEM((8, CLS_PAD, BLK), F32),
            pltpu.VMEM((8, HID, BLK), F32),
            pltpu.VMEM((7, CLS_PAD, BLK), F32),
            pltpu.VMEM((7, HID, BLK), F32),
            pltpu.VMEM((F_PAD, HID), BF16),
            pltpu.VMEM((CLS_PAD, HID), BF16),
            pltpu.VMEM((16, BLK), F32),
            pltpu.VMEM((1, 128), F32),
            pltpu.VMEM((CLS_PAD, HID), F32),
            pltpu.VMEM((2, GWO_HALF, HID), F32),
            pltpu.VMEM((GWO_HALF, HID), F32),
            pltpu.VMEM((8, GWO_HALF, HID), F32),
            pltpu.VMEM((2, GWO_HALF, HID), F32),
            pltpu.VMEM((F_PAD, HID), F32),
            pltpu.VMEM((2, GWH_HALF, HID), F32),
            pltpu.VMEM((GWH_HALF, HID), F32),
            pltpu.VMEM((8, GWH_HALF, HID), F32),
            pltpu.VMEM((2, GWH_HALF, HID), F32),
            dma((6,)), dma((NB,)), dma, dma, dma((21,)), dma((11,)), dma((42,)), dma((11,)),
            dma((3,)), dma((9,)), dma((3,)), dma((9,)),
        ],
        compiler_params=pltpu.CompilerParams(collective_id=0, has_side_effects=True, vmem_limit_bytes=64000000),
    )(adj_rows, feat_rows.T, w_hidden, w_output.T, labels[None, :], train_mask[None, :], block_mask)
    gwh, gwot, loss = pl.pallas_call(
        split_kernel,
        name='split_sums',
        out_shape=(jax.ShapeDtypeStruct((F_IN, HID), F32), jax.ShapeDtypeStruct((CLS, HID), F32),
                   jax.ShapeDtypeStruct((1, 1), F32)),
        in_specs=[vmem],
        out_specs=(vmem, vmem, vmem),
    )(pltpu.with_memory_space_constraint(sums, pltpu.VMEM))
    return loss[0, 0], gwh, gwot.T


def solution(mesh):
    row_spec = P(AXIS_NAME, None)
    vec_spec = P(AXIS_NAME)
    return jax.shard_map(device_step, mesh=mesh, in_specs=(row_spec, row_spec, P(), P(), vec_spec, vec_spec, P()), out_specs=(P(), P(), P()), check_vma=False)
```

```python
import jax
import jax.numpy as jnp
from jax import lax
from jax.experimental import pallas as pl
from jax.experimental.pallas import tpu as pltpu
from jax.sharding import PartitionSpec as P

AXIS_NAME = 'nodes'
MESH = pl.DeviceIdType.MESH
F32, BF16 = jnp.float32, jnp.bfloat16
BLK = 1024
NB = 16
F_IN, F_PAD = 100, 104
HID = 128
CLS, CLS_PAD = 47, 48
QS = [0, 2, 4, 1, 3, 6, 5, 7]
QI = {q: i for i, q in enumerate(QS)}
ORDERS = [(1, 2, 4), (2, 4, 1), (4, 1, 2)]
X_CHUNKS = [(0, 40, 0, BLK, 0), (40, 32, 0, BLK, 1), (72, 32, 0, BLK, 2)]
Y_CHUNKS = [(0, 16, 0, BLK, 0), (16, 16, 0, BLK, 1), (32, 16, 0, BLK, 2)]
D2_CHUNKS = [(8 * n, 8, 0, BLK, n % 3) for n in range(6)]
D1_CHUNKS = [(0, 40, 0, BLK, 0), (40, 40, 0, BLK, 1), (80, 40, 0, BLK, 2),
             (120, 8, 0, 384, 0), (120, 8, 384, 384, 1), (120, 8, 768, 256, 2)]
GWO_HALF, GWH_HALF = 24, 56
OUT_ROWS = F_PAD + CLS_PAD
M_TILE = 256
A_AHEAD = 5


def forwards(q, order_id, swapped):
    first, second, third = order = ORDERS[order_id]
    if order_id in swapped and q == first:
        return [(first, second)]
    if order_id in swapped and q == second:
        return [(second, third), (first, third)]
    return [(q, d) for d in order[1 + max(order.index(d) for d in order if q & d):]]


def last_dim(q, order_id):
    return max((d for d in ORDERS[order_id] if q & d), key=ORDERS[order_id].index)


def plan_gather(chunks, cost, max_group, swapped):
    sizes = [n * lanes * 0.002 for _, n, _, lanes, _ in chunks]
    link = {1: 0.0, 2: 0.0, 4: 0.0, 0: 0.0}
    ops, arrive, relayed, ready = [], {}, {}, [0]
    now = 0.0

    def send(table, key, dim, size):
        link[dim] = max(now, link[dim]) + size / (46.6 if dim else 600.0)
        table[key] = link[dim] + (2.3 if dim else 0.95)

    for j in range(3):
        for k, chunk in enumerate(chunks):
            d = ORDERS[chunk[4]][j]
            send(arrive, (d, k), d, sizes[k])
    send(relayed, 0, 0, sum(sizes))
    got = {q: 0 for q in range(8)}
    while arrive or relayed or ready:
        key = min(arrive, key=arrive.get, default=None)
        if key is not None and arrive[key] <= now:
            del arrive[key]
            q, k = key
            ops.append(('recv', q, k))
            for src, d in forwards(q, chunks[k][4], swapped):
                send(arrive, (src | d, k), d, sizes[k])
            got[q] += 1
            if got[q] == len(chunks):
                ops.append(('relay', q))
                send(relayed, q, 0, sum(sizes))
                ready.append(2 * QI[q])
            continue
        for q in sorted(relayed, key=relayed.get):
            if relayed[q] <= now:
                del relayed[q]
                ops.append(('take', q))
                ready.append(2 * QI[q] + 1)
        if ready:
            ops.append(('dot', ready[:max_group]))
            now += cost(len(ready[:max_group]))
            ready = ready[max_group:]
        else:
            now = min(list(arrive.values()) + list(relayed.values()))
    return ops


def dot_last(lhs, rhs):
    return lax.dot_general(lhs, rhs, (((1,), (1,)), ((), ())), preferred_element_type=F32)


def dot_first(lhs, rhs):
    return lax.dot_general(lhs, rhs, (((0,), (0,)), ((), ())), preferred_element_type=F32)


def step_kernel(adj_hbm, x_hbm, wh_hbm, wot_hbm, lab_hbm, msk_hbm, bm_hbm, out_ref,
                x_ref, wh_ref, wot_ref, lab_ref, msk_ref, bm_ref,
                adj, xall, yall, y1b, z1, z1t, z2, z2t, turned, hid, gt, et, con, part2, part1, rb2, rb1, whs, wos, macc, lossv,
                gwos, gwop, gwor, gwog, gwof, gwhs, gwhp, gwhr, gwhg, gwhf,
                io_sem, a_sem, ici_send, d2d_send, recv_a, d2d_a, recv_b, d2d_b,
                gwo_send, gwo_recv, gwh_send, gwh_recv):
    me = lax.axis_index(AXIS_NAME)
    coords = [me % 2, (me // 2) % 2, (me // 4) % 2, me // 8]

    def dev(rel):
        total = 0
        for bit in range(4):
            total = total + ((coords[bit] + ((rel >> bit) & 1)) % 2) * (1 << bit)
        return total

    def rel_of(slot):
        return 2 * QS[slot // 2] + slot % 2

    def rcopy(src, dst, send_sem, recv_sem, rel):
        return pltpu.make_async_remote_copy(src_ref=src, dst_ref=dst, send_sem=send_sem, recv_sem=recv_sem,
                                            device_id=(dev(rel),), device_id_type=MESH)

    def a_copy(slot, blk=0):
        return pltpu.make_async_copy(adj_hbm.at[:, pl.ds(pl.multiple_of(blk * BLK, BLK), BLK)], adj.at[slot], a_sem.at[slot])

    plan1 = plan_gather(X_CHUNKS, lambda n: 0.2 + 0.54 * n, 2, (2,))
    a_order = [slot for op in plan1 if op[0] == 'dot' for slot in op[1]]

    def start_a(lo, hi):
        for slot in a_order[lo:hi]:
            a_copy(slot, dev(rel_of(slot))).start()

    loads = [pltpu.make_async_copy(src, dst, io_sem.at[n]) for n, (src, dst) in enumerate(
        [(x_hbm, x_ref), (wh_hbm, wh_ref), (wot_hbm, wot_ref), (lab_hbm, lab_ref), (msk_hbm, msk_ref), (bm_hbm, bm_ref)])]
    barrier = pltpu.get_barrier_semaphore()
    peers = [1, 2, 4, 8]
    for rel in peers:
        pl.semaphore_signal(barrier, inc=1, device_id=(dev(rel),), device_id_type=MESH)

    for load in loads:
        load.start()
    start_a(0, A_AHEAD)
    macc[...] = jnp.zeros_like(macc)
    z1[...] = jnp.zeros_like(z1)
    z2[...] = jnp.zeros_like(z2)
    z2t[...] = jnp.zeros_like(z2t)
    whs[...] = jnp.zeros_like(whs)
    wos[...] = jnp.zeros_like(wos)
    for load in loads:
        load.wait()
    xall[0, 0:F_PAD - 8, :] = x_ref[0:F_PAD - 8, :]
    xall[0, F_PAD - 8:F_PAD, :] = jnp.concatenate([x_ref[F_PAD - 8:F_IN, :], jnp.zeros((F_PAD - F_IN, BLK), BF16)], axis=0)
    whs[0:F_IN, :] = wh_ref[...].astype(BF16)
    wos[0:CLS, :] = wot_ref[...].astype(BF16)
    pl.semaphore_wait(barrier, len(peers))

    def mask_of(slot):
        if isinstance(slot, int):
            return bm_ref[me, dev(rel_of(slot))]
        i = slot // 2
        c = slot % 2
        bits = []
        for bit in (1, 2, 4):
            b = 0
            for pos, q in enumerate(QS):
                if q & bit:
                    d = (i - pos) * (i - pos)
                    b = b + 1 // (1 + d)
            bits.append(b)
        total = ((coords[0] + c) % 2)
        for n, b in enumerate(bits):
            total = total + ((coords[n + 1] + b) % 2) * (2 << n)
        return bm_ref[me, total]


    def gather_product(buf, chunks, recv, recv_d2d, ops, swapped, first, dots):
        def ici(src_q, dim, k):
            dst_q = src_q ^ dim
            lo, n, lane, lanes, _ = chunks[k]
            return rcopy(buf.at[2 * QI[src_q], pl.ds(lo, n), pl.ds(lane, lanes)],
                         buf.at[2 * QI[dst_q], pl.ds(lo, n), pl.ds(lane, lanes)],
                         ici_send, recv.at[k * 7 + QI[dst_q] - 1], 2 * dim)

        def relay(q):
            return rcopy(buf.at[2 * QI[q]], buf.at[2 * QI[q] + 1], d2d_send, recv_d2d.at[QI[q]], 1)

        for j in range(3):
            for k, chunk in enumerate(chunks):
                ici(0, ORDERS[chunk[4]][j], k).start()
        relay(0).start()
        first()
        for op, q, *k in ops:
            if op == 'dot':
                dots(q)
            elif op == 'take':
                relay(q).wait_recv()
            elif op == 'relay':
                relay(q).start()
            else:
                order_id = chunks[k[0]][4]
                d = last_dim(q, order_id)
                ici(q ^ d, d, k[0]).wait_recv()
                for src, d in forwards(q, order_id, swapped):
                    ici(src, d, k[0]).start()
        for count, sem, rel in ((7, ici_send, 2), (8, d2d_send, 1)):
            sent = buf.at[pl.ds(0, count)]
            rcopy(sent, sent, sem, recv.at[0], rel).wait_send()

    def accumulate(out, slots, blocks):
        for lo in range(0, BLK, M_TILE):
            acc = out[lo:lo + M_TILE, :]
            for slot, block in zip(slots, blocks):
                acc = acc + dot_last(adj[slot, lo:lo + M_TILE, :], block)
            out[lo:lo + M_TILE, :] = acc

    def dots1(slots):
        for slot in slots:
            a_copy(slot).wait()
            ahead = a_order.index(slot) + A_AHEAD
            start_a(ahead, ahead + 1)
        for j, slot in enumerate(slots):
            yt = dot_first(whs[...], xall[slot]).astype(BF16)
            y1b[j] = (yt.astype(F32) * mask_of(slot).astype(F32)).astype(BF16)
        accumulate(z1, slots, [y1b[j] for j in range(len(slots))])

    gather_product(xall, X_CHUNKS, recv_a, d2d_a, plan1, (2,), lambda: None, dots1)

    cls_id = lax.broadcasted_iota(jnp.int32, (CLS_PAD, BLK), 0)
    weight = msk_ref[...].astype(F32)
    hid[...] = jnp.maximum(z1[...], 0.0).astype(BF16)
    yall[0] = jnp.where(cls_id == CLS, weight, dot_last(wos[...], hid[...])).astype(BF16)

    def dots2(slots):
        blocks = []
        for slot in slots:
            macc[...] += yall[slot, CLS_PAD - 16:CLS_PAD, :].astype(F32)
            blocks.append((yall[slot].astype(F32) * mask_of(slot).astype(F32)).astype(BF16))
        if len(slots) == 1:
            accumulate(z2, slots, blocks)
            return
        stream, held = slots
        turned[0] = jnp.transpose(adj[held, 0:M_TILE, :])
        for n in range(BLK // M_TILE):
            tile = slice(M_TILE * n, M_TILE * (n + 1))
            if n + 1 < BLK // M_TILE:
                turned[(n + 1) % 2] = jnp.transpose(adj[held, M_TILE * (n + 1):M_TILE * (n + 2), :])
            z2[tile, :] += dot_last(adj[stream, tile, :], blocks[0])
            z2t[:, tile] += jnp.dot(blocks[1], turned[n % 2], preferred_element_type=F32)

    def keep_sign():
        z1t[...] = jnp.transpose(z1[...])

    plan2 = plan_gather(Y_CHUNKS, lambda n: 0.43 + 0.25 * n, 2, (0, 1))
    gather_product(yall, Y_CHUNKS, recv_b, d2d_b, plan2, (0, 1), keep_sign, dots2)
    label_count = jnp.sum(macc[15:16, :])

    zt = jnp.transpose(z2[...]) + z2t[...]
    valid = cls_id < CLS
    top = jnp.max(jnp.where(valid, zt, -jnp.inf), axis=0, keepdims=True)
    expz = jnp.where(valid, jnp.exp(zt - top), 0.0)
    log_norm = jnp.log(jnp.sum(expz, axis=0, keepdims=True)) + top
    one_hot = cls_id == lab_ref[...]
    picked = jnp.sum(jnp.where(one_hot, zt, 0.0), axis=0, keepdims=True)
    loss_terms = weight * (log_norm - picked)
    acc = loss_terms[:, 0:128]
    for n in range(1, BLK // 128):
        acc = acc + loss_terms[:, 128 * n:128 * (n + 1)]
    lossv[...] = acc
    prob = jnp.exp(zt - log_norm)
    grad = (prob - one_hot.astype(F32)) * (weight / label_count)
    gt[...] = jnp.where(valid, grad, 0.0).astype(BF16)


    def reduce_pass(lhs_ref, rows, chunks, part, rb, recv, recv_d2d, early, tail, hooks):
        parts = range(len(chunks))

        def order_of(k):
            return ORDERS[chunks[k][4]]

        def dim_of(q, k):
            return next(d for d in reversed(order_of(k)) if q & d)

        def ici(q, k):
            lo, n, lane, lanes, _ = chunks[k]
            idx = k * 7 + QI[q] - 1
            return rcopy(con.at[2 * QI[q], pl.ds(lo, n), pl.ds(lane, lanes)],
                         rb.at[QI[q] - 1, pl.ds(lo, n), pl.ds(lane, lanes)], ici_send,
                         recv.at[idx], 2 * dim_of(q, k))

        def d2d(i):
            return rcopy(con.at[2 * i + 1, pl.ds(0, rows), :], part.at[i], d2d_send, recv_d2d.at[i], 1)

        cuts = [0, rows // 24 * 8, rows // 24 * 16, rows]

        def d2d_part(p):
            span = pl.ds(cuts[p], cuts[p + 1] - cuts[p])
            return rcopy(con.at[15, span, :], part.at[7, span, :], d2d_send, recv_d2d.at[8 + p if p else 7], 1)

        def sources(q, k):
            out = []
            for d in reversed(order_of(k)):
                if q & d:
                    break
                out.append(q ^ d)
            return out

        def compute(slot):
            lhs = (lhs_ref[...].astype(F32) * mask_of(slot).astype(F32)).astype(BF16)
            con[slot, 0:rows, :] = jnp.dot(lhs, adj[slot], preferred_element_type=F32)

        waiting = {(q, k): set(sources(q, k)) for q in range(8) for k in parts}

        def pair_sum(q):
            i = QI[q]
            for p in range(3) if i == 7 else [None]:
                lo, hi = (0, rows) if p is None else (cuts[p], cuts[p + 1])
                (d2d(i) if p is None else d2d_part(p)).wait_recv()
                con[2 * i, lo:hi, :] += part[i, lo:hi, :]
                for k in parts:
                    if q and not waiting[q, k] and lo <= chunks[k][0] < hi:
                        ici(q, k).start()

        def take(src, k):
            d = dim_of(src, k)
            q = src ^ d
            lo, n, lane, lanes, _ = chunks[k]
            ici(src, k).wait_recv()
            con[2 * QI[q], lo:lo + n, lane:lane + lanes] += rb[QI[src] - 1, lo:lo + n, lane:lane + lanes]
            waiting[q, k].discard(src)
            if q and not waiting[q, k]:
                ici(q, k).start()

        def body(n, carry):
            i = 7 - n
            compute(2 * i + 1)

            @pl.when(n == 0)
            def _():
                for p in range(3):
                    d2d_part(p).start()

            @pl.when(n > 0)
            def _():
                d2d(i).start()

            compute(2 * i)
            for m in range(8):
                @pl.when(n == m)
                def _(m=m):
                    if m:
                        pair_sum(QS[8 - m])
                    for r in early.get(m, ()):
                        take_rank(r)
                    for hook in hooks.get(m, ()):
                        hook()
            return carry

        rank = {q: r for r, q in enumerate(reversed(QS))}

        def sources_of(k, phase):
            d = order_of(k)[2 - phase]
            later = order_of(k)[3 - phase:]
            return sorted((q for q in range(1, 8) if q & d and not any(q & e for e in later)), key=rank.get)

        def take_rank(r, phase=0):
            for k in parts:
                take(sources_of(k, phase)[r], k)

        lax.fori_loop(0, 8, body, 0)
        for step in tail:
            if step is None:
                pair_sum(0)
            elif isinstance(step, str):
                for hook in hooks[step]:
                    hook()
            else:
                take_rank(step[1], step[0])
        for count, sem, rel in ((7, ici_send, 2), (8, d2d_send, 1)):
            sent = con.at[pl.ds(0, count), pl.ds(0, rows), :]
            rcopy(sent, sent, sem, recv.at[0], rel).wait_send()

    reduce_pass(gt, CLS_PAD, D2_CHUNKS, part2, rb2, recv_a, d2d_a, {6: [0], 7: [1]},
                [None, (0, 2), (1, 0), (0, 3), (1, 1), (2, 0)], {})
    d2t = con[0, 0:CLS_PAD, :].astype(BF16)
    gwo = jnp.dot(d2t, hid[...], preferred_element_type=F32)
    et[...] = jnp.where(z1t[...] > 0, dot_first(wos[...], d2t), 0.0).astype(BF16)
    row_id = lax.broadcasted_iota(jnp.int32, (CLS_PAD, HID), 0)
    gwos[...] = jnp.where(row_id == CLS, lossv[...], gwo)

    core = coords[0]

    def all_sum(rows, total_rows, src, halves, other, own, gathered, final, send, recv):
        def prepare():
            halves[0] = src[0:rows, :]
            halves[1, 0:total_rows - rows, :] = src[rows:total_rows, :]
            if total_rows < 2 * rows:
                halves[1, total_rows - rows:rows, :] = jnp.zeros((2 * rows - total_rows, HID), F32)

        pair = rcopy(halves.at[1 - core], other, send.at[0], recv.at[0], 1)
        sends = [rcopy(gathered.at[0], gathered.at[q], send.at[1], recv.at[q], 2 * q) for q in range(1, 8)]
        back = rcopy(own, final, send.at[2], recv.at[8], 1)

        def start():
            prepare()
            pair.start()

        def spread():
            pair.wait()
            gathered[0] = halves[core] + other[...]
            for q in (7, 6, 5, 3, 4, 2, 1):
                sends[q - 1].start()

        def collect():
            for cp in sends:
                cp.wait_recv()
            rcopy(gathered.at[pl.ds(0, 7)], gathered.at[pl.ds(0, 7)], send.at[1], recv.at[0], 2).wait_send()
            g = gathered
            own[...] = ((g[0] + g[1]) + (g[2] + g[3])) + ((g[4] + g[5]) + (g[6] + g[7]))
            back.start()

        def finish():
            halves[core] = own[...]
            back.wait()
            halves[1 - core] = final[...]

        return start, spread, collect, finish

    gwo_start, gwo_spread, gwo_collect, gwo_finish = all_sum(GWO_HALF, CLS_PAD, gwos, gwop, gwof.at[0], gwor, gwog,
                                                             gwof.at[1], gwo_send, gwo_recv)
    gwh_start, gwh_spread, gwh_collect, gwh_finish = all_sum(GWH_HALF, F_PAD, gwhs, gwhp, gwhf.at[0], gwhr, gwhg,
                                                             gwhf.at[1], gwh_send, gwh_recv)
    gwo_start()

    def gwo_out():
        gwo_finish()
        out_ref[F_PAD:F_PAD + GWO_HALF, :] = gwop[0]
        out_ref[F_PAD + GWO_HALF:OUT_ROWS, :] = gwop[1]
        loss = jnp.sum(gwop[1, GWO_HALF - 1:GWO_HALF, :], axis=1, keepdims=True) / label_count
        out_ref[OUT_ROWS - 1:OUT_ROWS, :] = jnp.broadcast_to(loss, (1, HID))

    reduce_pass(et, HID, D1_CHUNKS, part1, rb1, recv_b, d2d_b, {},
                [(0, 0), (0, 1), (0, 2), 'mid', None, (0, 3), (1, 0), (1, 1), 'late', (2, 0)],
                {0: [gwo_spread], 'mid': [gwo_collect], 'late': [gwo_out]})
    gwhs[...] = dot_last(xall[0], con[0].astype(BF16))
    gwh_start()
    gwh_spread()
    gwh_collect()
    gwh_finish()
    out_ref[0:GWH_HALF, :] = gwhp[0]
    out_ref[GWH_HALF:F_PAD, :] = gwhp[1, 0:F_PAD - GWH_HALF, :]


def split_kernel(sums_ref, gwh_ref, gwot_ref, loss_ref):
    gwh_ref[...] = sums_ref[0:F_IN, :]
    gwot_ref[...] = sums_ref[F_PAD:F_PAD + CLS, :]
    loss_ref[...] = sums_ref[OUT_ROWS - 1:OUT_ROWS, 0:1]


def device_step(adj_rows, feat_rows, w_hidden, w_output, labels, train_mask, block_mask):
    dma = pltpu.SemaphoreType.DMA
    vmem = pl.BlockSpec(memory_space=pltpu.VMEM)
    hbm = pl.BlockSpec(memory_space=pl.ANY)
    sums = pl.pallas_call(
        step_kernel,
        name='gcn_step',
        out_shape=pltpu.VMEM((OUT_ROWS, HID), F32),
        in_specs=[hbm] * 7,
        out_specs=vmem,
        scratch_shapes=[
            pltpu.VMEM((F_IN, BLK), BF16),
            pltpu.VMEM((F_IN, HID), F32),
            pltpu.VMEM((CLS, HID), F32),
            pltpu.VMEM((1, BLK), jnp.int32),
            pltpu.VMEM((1, BLK), jnp.int32),
            pltpu.SMEM((NB, NB), jnp.int32),
            pltpu.VMEM((NB, BLK, BLK), BF16),
            pltpu.VMEM((NB, F_PAD, BLK), BF16),
            pltpu.VMEM((NB, CLS_PAD, BLK), BF16),
            pltpu.VMEM((2, HID, BLK), BF16),
            pltpu.VMEM((BLK, HID), F32),
            pltpu.VMEM((HID, BLK), F32),
            pltpu.VMEM((BLK, CLS_PAD), F32),
            pltpu.VMEM((CLS_PAD, BLK), F32),
            pltpu.VMEM((2, BLK, M_TILE), BF16),
            pltpu.VMEM((BLK, HID), BF16),
            pltpu.VMEM((CLS_PAD, BLK), BF16),
            pltpu.VMEM((HID, BLK), BF16),
            pltpu.VMEM((NB, HID, BLK), F32),
            pltpu.VMEM((8, CLS_PAD, BLK), F32),
            pltpu.VMEM((8, HID, BLK), F32),
            pltpu.VMEM((7, CLS_PAD, BLK), F32),
            pltpu.VMEM((7, HID, BLK), F32),
            pltpu.VMEM((F_PAD, HID), BF16),
            pltpu.VMEM((CLS_PAD, HID), BF16),
            pltpu.VMEM((16, BLK), F32),
            pltpu.VMEM((1, 128), F32),
            pltpu.VMEM((CLS_PAD, HID), F32),
            pltpu.VMEM((2, GWO_HALF, HID), F32),
            pltpu.VMEM((GWO_HALF, HID), F32),
            pltpu.VMEM((8, GWO_HALF, HID), F32),
            pltpu.VMEM((2, GWO_HALF, HID), F32),
            pltpu.VMEM((F_PAD, HID), F32),
            pltpu.VMEM((2, GWH_HALF, HID), F32),
            pltpu.VMEM((GWH_HALF, HID), F32),
            pltpu.VMEM((8, GWH_HALF, HID), F32),
            pltpu.VMEM((2, GWH_HALF, HID), F32),
            dma((6,)), dma((NB,)), dma, dma, dma((42,)), dma((11,)), dma((42,)), dma((11,)),
            dma((3,)), dma((9,)), dma((3,)), dma((9,)),
        ],
        compiler_params=pltpu.CompilerParams(collective_id=0, has_side_effects=True, vmem_limit_bytes=64000000),
    )(adj_rows, feat_rows.T, w_hidden, w_output.T, labels[None, :], train_mask[None, :], block_mask)
    gwh, gwot, loss = pl.pallas_call(
        split_kernel,
        name='split_sums',
        out_shape=(jax.ShapeDtypeStruct((F_IN, HID), F32), jax.ShapeDtypeStruct((CLS, HID), F32),
                   jax.ShapeDtypeStruct((1, 1), F32)),
        in_specs=[vmem],
        out_specs=(vmem, vmem, vmem),
    )(pltpu.with_memory_space_constraint(sums, pltpu.VMEM))
    return loss[0, 0], gwh, gwot.T


def solution(mesh):
    row_spec = P(AXIS_NAME, None)
    vec_spec = P(AXIS_NAME)
    return jax.shard_map(device_step, mesh=mesh, in_specs=(row_spec, row_spec, P(), P(), vec_spec, vec_spec, P()), out_specs=(P(), P(), P()), check_vma=False)
```

```python
import jax
import jax.numpy as jnp
from jax import lax
from jax.experimental import pallas as pl
from jax.experimental.pallas import tpu as pltpu
from jax.sharding import PartitionSpec as P

AXIS_NAME = 'nodes'
MESH = pl.DeviceIdType.MESH
F32, BF16 = jnp.float32, jnp.bfloat16
BLK = 1024
NB = 16
F_IN, F_PAD = 100, 104
HID = 128
CLS, CLS_PAD = 47, 48
QS = [0, 2, 4, 1, 3, 6, 5, 7]
QI = {q: i for i, q in enumerate(QS)}
ORDERS = [(1, 2, 4), (2, 4, 1), (4, 1, 2)]
X_CHUNKS = [(0, 40, 0, BLK, 0), (40, 32, 0, BLK, 1), (72, 32, 0, BLK, 2)]
Y_CHUNKS = [(0, 16, 0, BLK, 0), (16, 16, 0, BLK, 1), (32, 16, 0, BLK, 2)]
D1_CHUNKS = [(0, 48, 0, BLK, 0), (48, 40, 0, BLK, 1), (88, 40, 0, BLK, 2)]
GWO_HALF, GWH_HALF = 24, 56
OUT_ROWS = F_PAD + CLS_PAD
M_TILE = 256
A_AHEAD = 5


def forwards(q, order_id, swapped):
    first, second, third = order = ORDERS[order_id]
    if order_id in swapped and q == first:
        return [(first, second)]
    if order_id in swapped and q == second:
        return [(second, third), (first, third)]
    return [(q, d) for d in order[1 + max(order.index(d) for d in order if q & d):]]


def last_dim(q, order_id):
    return max((d for d in ORDERS[order_id] if q & d), key=ORDERS[order_id].index)


def plan_gather(chunks, cost, max_group, swapped):
    sizes = [n * lanes * 0.002 for _, n, _, lanes, _ in chunks]
    link = {1: 0.0, 2: 0.0, 4: 0.0, 0: 0.0}
    ops, arrive, relayed, ready = [], {}, {}, [0]
    now = 0.0

    def send(table, key, dim, size):
        link[dim] = max(now, link[dim]) + size / (46.6 if dim else 600.0)
        table[key] = link[dim] + (2.3 if dim else 0.95)

    for j in range(3):
        for k, chunk in enumerate(chunks):
            d = ORDERS[chunk[4]][j]
            send(arrive, (d, k), d, sizes[k])
    send(relayed, 0, 0, sum(sizes))
    got = {q: 0 for q in range(8)}
    while arrive or relayed or ready:
        key = min(arrive, key=arrive.get, default=None)
        if key is not None and arrive[key] <= now:
            del arrive[key]
            q, k = key
            ops.append(('recv', q, k))
            for src, d in forwards(q, chunks[k][4], swapped):
                send(arrive, (src | d, k), d, sizes[k])
            got[q] += 1
            if got[q] == len(chunks):
                ops.append(('relay', q))
                send(relayed, q, 0, sum(sizes))
                ready.append(2 * QI[q])
            continue
        for q in sorted(relayed, key=relayed.get):
            if relayed[q] <= now:
                del relayed[q]
                ops.append(('take', q))
                ready.append(2 * QI[q] + 1)
        if ready:
            ops.append(('dot', ready[:max_group]))
            now += cost(len(ready[:max_group]))
            ready = ready[max_group:]
        else:
            now = min(list(arrive.values()) + list(relayed.values()))
    return ops


def dot_last(lhs, rhs):
    return lax.dot_general(lhs, rhs, (((1,), (1,)), ((), ())), preferred_element_type=F32)


def dot_first(lhs, rhs):
    return lax.dot_general(lhs, rhs, (((0,), (0,)), ((), ())), preferred_element_type=F32)


def step_kernel(adj_hbm, x_hbm, wh_hbm, wot_hbm, lab_hbm, msk_hbm, bm_hbm, out_ref,
                x_ref, wh_ref, wot_ref, lab_ref, msk_ref, bm_ref,
                adj, xall, yall, y1b, z1, z1t, z2, z2t, turned, hid, gt, et, con, part2, part1, rb2, rb1, whs, wos, macc, lossv,
                gwos, gwop, gwor, gwog, gwof, gwhs, gwhp, gwhr, gwhg, gwhf,
                io_sem, a_sem, ici_send, d2d_send, recv_a, d2d_a, recv_b, d2d_b,
                gwo_send, gwo_recv, gwh_send, gwh_recv):
    me = lax.axis_index(AXIS_NAME)
    coords = [me % 2, (me // 2) % 2, (me // 4) % 2, me // 8]

    def dev(rel):
        total = 0
        for bit in range(4):
            total = total + ((coords[bit] + ((rel >> bit) & 1)) % 2) * (1 << bit)
        return total

    def rel_of(slot):
        return 2 * QS[slot // 2] + slot % 2

    def rcopy(src, dst, send_sem, recv_sem, rel):
        return pltpu.make_async_remote_copy(src_ref=src, dst_ref=dst, send_sem=send_sem, recv_sem=recv_sem,
                                            device_id=(dev(rel),), device_id_type=MESH)

    def a_copy(slot, blk=0):
        return pltpu.make_async_copy(adj_hbm.at[:, pl.ds(pl.multiple_of(blk * BLK, BLK), BLK)], adj.at[slot], a_sem.at[slot])

    plan1 = plan_gather(X_CHUNKS, lambda n: 0.2 + 0.54 * n, 2, (2,))
    a_order = [slot for op in plan1 if op[0] == 'dot' for slot in op[1]]

    def start_a(lo, hi):
        for slot in a_order[lo:hi]:
            a_copy(slot, dev(rel_of(slot))).start()

    loads = [pltpu.make_async_copy(src, dst, io_sem.at[n]) for n, (src, dst) in enumerate(
        [(x_hbm, x_ref), (wh_hbm, wh_ref), (wot_hbm, wot_ref), (lab_hbm, lab_ref), (msk_hbm, msk_ref), (bm_hbm, bm_ref)])]
    barrier = pltpu.get_barrier_semaphore()
    peers = [1, 2, 4, 8]
    for rel in peers:
        pl.semaphore_signal(barrier, inc=1, device_id=(dev(rel),), device_id_type=MESH)

    for load in loads:
        load.start()
    start_a(0, A_AHEAD)
    macc[...] = jnp.zeros_like(macc)
    z1[...] = jnp.zeros_like(z1)
    z2[...] = jnp.zeros_like(z2)
    z2t[...] = jnp.zeros_like(z2t)
    whs[...] = jnp.zeros_like(whs)
    wos[...] = jnp.zeros_like(wos)
    for load in loads:
        load.wait()
    xall[0, 0:F_PAD - 8, :] = x_ref[0:F_PAD - 8, :]
    xall[0, F_PAD - 8:F_PAD, :] = jnp.concatenate([x_ref[F_PAD - 8:F_IN, :], jnp.zeros((F_PAD - F_IN, BLK), BF16)], axis=0)
    whs[0:F_IN, :] = wh_ref[...].astype(BF16)
    wos[0:CLS, :] = wot_ref[...].astype(BF16)
    pl.semaphore_wait(barrier, len(peers))

    def mask_of(slot):
        if isinstance(slot, int):
            return bm_ref[me, dev(rel_of(slot))]
        i = slot // 2
        c = slot % 2
        bits = []
        for bit in (1, 2, 4):
            b = 0
            for pos, q in enumerate(QS):
                if q & bit:
                    d = (i - pos) * (i - pos)
                    b = b + 1 // (1 + d)
            bits.append(b)
        total = ((coords[0] + c) % 2)
        for n, b in enumerate(bits):
            total = total + ((coords[n + 1] + b) % 2) * (2 << n)
        return bm_ref[me, total]


    def gather_product(buf, chunks, recv, recv_d2d, ops, swapped, first, dots):
        def ici(src_q, dim, k):
            dst_q = src_q ^ dim
            lo, n, lane, lanes, _ = chunks[k]
            return rcopy(buf.at[2 * QI[src_q], pl.ds(lo, n), pl.ds(lane, lanes)],
                         buf.at[2 * QI[dst_q], pl.ds(lo, n), pl.ds(lane, lanes)],
                         ici_send, recv.at[k * 7 + QI[dst_q] - 1], 2 * dim)

        def relay(q):
            return rcopy(buf.at[2 * QI[q]], buf.at[2 * QI[q] + 1], d2d_send, recv_d2d.at[QI[q]], 1)

        for j in range(3):
            for k, chunk in enumerate(chunks):
                ici(0, ORDERS[chunk[4]][j], k).start()
        relay(0).start()
        first()
        for op, q, *k in ops:
            if op == 'dot':
                dots(q)
            elif op == 'take':
                relay(q).wait_recv()
            elif op == 'relay':
                relay(q).start()
            else:
                order_id = chunks[k[0]][4]
                d = last_dim(q, order_id)
                ici(q ^ d, d, k[0]).wait_recv()
                for src, d in forwards(q, order_id, swapped):
                    ici(src, d, k[0]).start()
        for count, sem, rel in ((7, ici_send, 2), (8, d2d_send, 1)):
            sent = buf.at[pl.ds(0, count)]
            rcopy(sent, sent, sem, recv.at[0], rel).wait_send()

    def accumulate(out, slots, blocks):
        for lo in range(0, BLK, M_TILE):
            acc = out[lo:lo + M_TILE, :]
            for slot, block in zip(slots, blocks):
                acc = acc + dot_last(adj[slot, lo:lo + M_TILE, :], block)
            out[lo:lo + M_TILE, :] = acc

    def dots1(slots):
        for slot in slots:
            a_copy(slot).wait()
            ahead = a_order.index(slot) + A_AHEAD
            start_a(ahead, ahead + 1)
        for j, slot in enumerate(slots):
            yt = dot_first(whs[...], xall[slot]).astype(BF16)
            y1b[j] = (yt.astype(F32) * mask_of(slot).astype(F32)).astype(BF16)
        accumulate(z1, slots, [y1b[j] for j in range(len(slots))])

    gather_product(xall, X_CHUNKS, recv_a, d2d_a, plan1, (2,), lambda: None, dots1)

    cls_id = lax.broadcasted_iota(jnp.int32, (CLS_PAD, BLK), 0)
    weight = msk_ref[...].astype(F32)
    hid[...] = jnp.maximum(z1[...], 0.0).astype(BF16)
    yall[0] = jnp.where(cls_id == CLS, weight, dot_last(wos[...], hid[...])).astype(BF16)

    def dots2(slots):
        blocks = []
        for slot in slots:
            macc[...] += yall[slot, CLS_PAD - 16:CLS_PAD, :].astype(F32)
            blocks.append((yall[slot].astype(F32) * mask_of(slot).astype(F32)).astype(BF16))
        if len(slots) == 1:
            accumulate(z2, slots, blocks)
            return
        stream, held = slots
        turned[0] = jnp.transpose(adj[held, 0:M_TILE, :])
        for n in range(BLK // M_TILE):
            tile = slice(M_TILE * n, M_TILE * (n + 1))
            if n + 1 < BLK // M_TILE:
                turned[(n + 1) % 2] = jnp.transpose(adj[held, M_TILE * (n + 1):M_TILE * (n + 2), :])
            z2[tile, :] += dot_last(adj[stream, tile, :], blocks[0])
            z2t[:, tile] += jnp.dot(blocks[1], turned[n % 2], preferred_element_type=F32)

    def keep_sign():
        z1t[...] = jnp.transpose(z1[...])

    plan2 = plan_gather(Y_CHUNKS, lambda n: 0.43 + 0.25 * n, 2, (0, 1))
    gather_product(yall, Y_CHUNKS, recv_b, d2d_b, plan2, (0, 1), keep_sign, dots2)
    label_count = jnp.sum(macc[15:16, :])

    zt = jnp.transpose(z2[...]) + z2t[...]
    valid = cls_id < CLS
    top = jnp.max(jnp.where(valid, zt, -jnp.inf), axis=0, keepdims=True)
    expz = jnp.where(valid, jnp.exp(zt - top), 0.0)
    log_norm = jnp.log(jnp.sum(expz, axis=0, keepdims=True)) + top
    one_hot = cls_id == lab_ref[...]
    picked = jnp.sum(jnp.where(one_hot, zt, 0.0), axis=0, keepdims=True)
    loss_terms = weight * (log_norm - picked)
    acc = loss_terms[:, 0:128]
    for n in range(1, BLK // 128):
        acc = acc + loss_terms[:, 128 * n:128 * (n + 1)]
    lossv[...] = acc
    prob = jnp.exp(zt - log_norm)
    grad = (prob - one_hot.astype(F32)) * (weight / label_count)
    gt[...] = jnp.where(valid, grad, 0.0).astype(BF16)


    def reduce_pass(lhs_ref, rows, chunks, part, rb, recv, recv_d2d, early, tail, hooks):
        parts = range(len(chunks))

        def order_of(k):
            return ORDERS[chunks[k][4]]

        def dim_of(q, k):
            return next(d for d in reversed(order_of(k)) if q & d)

        def ici(q, k):
            lo, n, lane, lanes, _ = chunks[k]
            idx = k * 7 + QI[q] - 1
            return rcopy(con.at[2 * QI[q], pl.ds(lo, n), pl.ds(lane, lanes)],
                         rb.at[QI[q] - 1, pl.ds(lo, n), pl.ds(lane, lanes)], ici_send,
                         recv.at[idx], 2 * dim_of(q, k))

        def d2d(i):
            return rcopy(con.at[2 * i + 1, pl.ds(0, rows), :], part.at[i], d2d_send, recv_d2d.at[i], 1)

        cuts = [chunks[0][0], chunks[1][0], chunks[2][0], rows]

        def d2d_part(p):
            span = pl.ds(cuts[p], cuts[p + 1] - cuts[p])
            return rcopy(con.at[15, span, :], part.at[7, span, :], d2d_send, recv_d2d.at[8 + p if p else 7], 1)

        def sources(q, k):
            out = []
            for d in reversed(order_of(k)):
                if q & d:
                    break
                out.append(q ^ d)
            return out

        def compute(slot):
            lhs = (lhs_ref[...].astype(F32) * mask_of(slot).astype(F32)).astype(BF16)
            con[slot, 0:rows, :] = jnp.dot(lhs, adj[slot], preferred_element_type=F32)

        waiting = {(q, k): set(sources(q, k)) for q in range(8) for k in parts}

        def pair_sum(q):
            i = QI[q]
            for p in range(3) if i == 7 else [None]:
                lo, hi = (0, rows) if p is None else (cuts[p], cuts[p + 1])
                (d2d(i) if p is None else d2d_part(p)).wait_recv()
                con[2 * i, lo:hi, :] += part[i, lo:hi, :]
                for k in parts:
                    if q and not waiting[q, k] and lo <= chunks[k][0] < hi:
                        ici(q, k).start()

        def take(src, k):
            d = dim_of(src, k)
            q = src ^ d
            lo, n, lane, lanes, _ = chunks[k]
            ici(src, k).wait_recv()
            con[2 * QI[q], lo:lo + n, lane:lane + lanes] += rb[QI[src] - 1, lo:lo + n, lane:lane + lanes]
            waiting[q, k].discard(src)
            if q and not waiting[q, k]:
                ici(q, k).start()

        def body(n, carry):
            i = 7 - n
            compute(2 * i + 1)

            @pl.when(n == 0)
            def _():
                for p in range(3):
                    d2d_part(p).start()

            @pl.when(n > 0)
            def _():
                d2d(i).start()

            compute(2 * i)
            for m in range(8):
                @pl.when(n == m)
                def _(m=m):
                    if m:
                        pair_sum(QS[8 - m])
                    for r in early.get(m, ()):
                        take_rank(r)
                    for hook in hooks.get(m, ()):
                        hook()
            return carry

        rank = {q: r for r, q in enumerate(reversed(QS))}

        def sources_of(k, phase):
            d = order_of(k)[2 - phase]
            later = order_of(k)[3 - phase:]
            return sorted((q for q in range(1, 8) if q & d and not any(q & e for e in later)), key=rank.get)

        def take_rank(r, phase=0):
            for k in parts:
                take(sources_of(k, phase)[r], k)

        lax.fori_loop(0, 8, body, 0)
        for step in tail:
            if step is None:
                pair_sum(0)
            elif isinstance(step, str):
                for hook in hooks[step]:
                    hook()
            else:
                take_rank(step[1], step[0])
        for count, sem, rel in ((7, ici_send, 2), (8, d2d_send, 1)):
            sent = con.at[pl.ds(0, count), pl.ds(0, rows), :]
            rcopy(sent, sent, sem, recv.at[0], rel).wait_send()

    reduce_pass(gt, CLS_PAD, Y_CHUNKS, part2, rb2, recv_a, d2d_a, {5: [0], 6: [1], 7: [2]}, [None, (1, 0), (0, 3), (1, 1), (2, 0)], {})
    d2t = con[0, 0:CLS_PAD, :].astype(BF16)
    gwo = jnp.dot(d2t, hid[...], preferred_element_type=F32)
    et[...] = jnp.where(z1t[...] > 0, dot_first(wos[...], d2t), 0.0).astype(BF16)
    row_id = lax.broadcasted_iota(jnp.int32, (CLS_PAD, HID), 0)
    gwos[...] = jnp.where(row_id == CLS, lossv[...], gwo)

    core = coords[0]

    def all_sum(rows, total_rows, src, halves, other, own, gathered, final, send, recv):
        def prepare():
            halves[0] = src[0:rows, :]
            halves[1, 0:total_rows - rows, :] = src[rows:total_rows, :]
            if total_rows < 2 * rows:
                halves[1, total_rows - rows:rows, :] = jnp.zeros((2 * rows - total_rows, HID), F32)

        pair = rcopy(halves.at[1 - core], other, send.at[0], recv.at[0], 1)
        sends = [rcopy(gathered.at[0], gathered.at[q], send.at[1], recv.at[q], 2 * q) for q in range(1, 8)]
        back = rcopy(own, final, send.at[2], recv.at[8], 1)

        def start():
            prepare()
            pair.start()

        def spread():
            pair.wait()
            gathered[0] = halves[core] + other[...]
            for q in (7, 6, 5, 3, 4, 2, 1):
                sends[q - 1].start()

        def collect():
            for cp in sends:
                cp.wait_recv()
            rcopy(gathered.at[pl.ds(0, 7)], gathered.at[pl.ds(0, 7)], send.at[1], recv.at[0], 2).wait_send()
            g = gathered
            own[...] = ((g[0] + g[1]) + (g[2] + g[3])) + ((g[4] + g[5]) + (g[6] + g[7]))
            back.start()

        def finish():
            halves[core] = own[...]
            back.wait()
            halves[1 - core] = final[...]

        return start, spread, collect, finish

    gwo_start, gwo_spread, gwo_collect, gwo_finish = all_sum(GWO_HALF, CLS_PAD, gwos, gwop, gwof.at[0], gwor, gwog,
                                                             gwof.at[1], gwo_send, gwo_recv)
    gwh_start, gwh_spread, gwh_collect, gwh_finish = all_sum(GWH_HALF, F_PAD, gwhs, gwhp, gwhf.at[0], gwhr, gwhg,
                                                             gwhf.at[1], gwh_send, gwh_recv)
    gwo_start()

    def gwo_out():
        gwo_finish()
        out_ref[F_PAD:F_PAD + GWO_HALF, :] = gwop[0]
        out_ref[F_PAD + GWO_HALF:OUT_ROWS, :] = gwop[1]
        loss = jnp.sum(gwop[1, GWO_HALF - 1:GWO_HALF, :], axis=1, keepdims=True) / label_count
        out_ref[OUT_ROWS - 1:OUT_ROWS, :] = jnp.broadcast_to(loss, (1, HID))

    reduce_pass(et, HID, D1_CHUNKS, part1, rb1, recv_b, d2d_b, {},
                [(0, 0), (0, 1), (0, 2), 'mid', None, (0, 3), (1, 0), (1, 1), 'late', (2, 0)],
                {0: [gwo_spread], 'mid': [gwo_collect], 'late': [gwo_out]})
    gwhs[...] = dot_last(xall[0], con[0].astype(BF16))
    gwh_start()
    gwh_spread()
    gwh_collect()
    gwh_finish()
    out_ref[0:GWH_HALF, :] = gwhp[0]
    out_ref[GWH_HALF:F_PAD, :] = gwhp[1, 0:F_PAD - GWH_HALF, :]


def split_kernel(sums_ref, gwh_ref, gwot_ref, loss_ref):
    gwh_ref[...] = sums_ref[0:F_IN, :]
    gwot_ref[...] = sums_ref[F_PAD:F_PAD + CLS, :]
    loss_ref[...] = sums_ref[OUT_ROWS - 1:OUT_ROWS, 0:1]


def device_step(adj_rows, feat_rows, w_hidden, w_output, labels, train_mask, block_mask):
    dma = pltpu.SemaphoreType.DMA
    vmem = pl.BlockSpec(memory_space=pltpu.VMEM)
    hbm = pl.BlockSpec(memory_space=pl.ANY)
    sums = pl.pallas_call(
        step_kernel,
        name='gcn_step',
        out_shape=pltpu.VMEM((OUT_ROWS, HID), F32),
        in_specs=[hbm] * 7,
        out_specs=vmem,
        scratch_shapes=[
            pltpu.VMEM((F_IN, BLK), BF16),
            pltpu.VMEM((F_IN, HID), F32),
            pltpu.VMEM((CLS, HID), F32),
            pltpu.VMEM((1, BLK), jnp.int32),
            pltpu.VMEM((1, BLK), jnp.int32),
            pltpu.SMEM((NB, NB), jnp.int32),
            pltpu.VMEM((NB, BLK, BLK), BF16),
            pltpu.VMEM((NB, F_PAD, BLK), BF16),
            pltpu.VMEM((NB, CLS_PAD, BLK), BF16),
            pltpu.VMEM((2, HID, BLK), BF16),
            pltpu.VMEM((BLK, HID), F32),
            pltpu.VMEM((HID, BLK), F32),
            pltpu.VMEM((BLK, CLS_PAD), F32),
            pltpu.VMEM((CLS_PAD, BLK), F32),
            pltpu.VMEM((2, BLK, M_TILE), BF16),
            pltpu.VMEM((BLK, HID), BF16),
            pltpu.VMEM((CLS_PAD, BLK), BF16),
            pltpu.VMEM((HID, BLK), BF16),
            pltpu.VMEM((NB, HID, BLK), F32),
            pltpu.VMEM((8, CLS_PAD, BLK), F32),
            pltpu.VMEM((8, HID, BLK), F32),
            pltpu.VMEM((7, CLS_PAD, BLK), F32),
            pltpu.VMEM((7, HID, BLK), F32),
            pltpu.VMEM((F_PAD, HID), BF16),
            pltpu.VMEM((CLS_PAD, HID), BF16),
            pltpu.VMEM((16, BLK), F32),
            pltpu.VMEM((1, 128), F32),
            pltpu.VMEM((CLS_PAD, HID), F32),
            pltpu.VMEM((2, GWO_HALF, HID), F32),
            pltpu.VMEM((GWO_HALF, HID), F32),
            pltpu.VMEM((8, GWO_HALF, HID), F32),
            pltpu.VMEM((2, GWO_HALF, HID), F32),
            pltpu.VMEM((F_PAD, HID), F32),
            pltpu.VMEM((2, GWH_HALF, HID), F32),
            pltpu.VMEM((GWH_HALF, HID), F32),
            pltpu.VMEM((8, GWH_HALF, HID), F32),
            pltpu.VMEM((2, GWH_HALF, HID), F32),
            dma((6,)), dma((NB,)), dma, dma, dma((21,)), dma((11,)), dma((21,)), dma((11,)),
            dma((3,)), dma((9,)), dma((3,)), dma((9,)),
        ],
        compiler_params=pltpu.CompilerParams(collective_id=0, has_side_effects=True, vmem_limit_bytes=64000000),
    )(adj_rows, feat_rows.T, w_hidden, w_output.T, labels[None, :], train_mask[None, :], block_mask)
    gwh, gwot, loss = pl.pallas_call(
        split_kernel,
        name='split_sums',
        out_shape=(jax.ShapeDtypeStruct((F_IN, HID), F32), jax.ShapeDtypeStruct((CLS, HID), F32),
                   jax.ShapeDtypeStruct((1, 1), F32)),
        in_specs=[vmem],
        out_specs=(vmem, vmem, vmem),
    )(pltpu.with_memory_space_constraint(sums, pltpu.VMEM))
    return loss[0, 0], gwh, gwot.T


def solution(mesh):
    row_spec = P(AXIS_NAME, None)
    vec_spec = P(AXIS_NAME)
    return jax.shard_map(device_step, mesh=mesh, in_specs=(row_spec, row_spec, P(), P(), vec_spec, vec_spec, P()), out_specs=(P(), P(), P()), check_vma=False)
```

```python
import jax
import jax.numpy as jnp
from jax import lax
from jax.experimental import pallas as pl
from jax.experimental.pallas import tpu as pltpu
from jax.sharding import PartitionSpec as P

AXIS_NAME = 'nodes'
MESH = pl.DeviceIdType.MESH
F32, BF16 = jnp.float32, jnp.bfloat16
BLK = 1024
NB = 16
F_IN, F_PAD = 100, 104
HID = 128
CLS, CLS_PAD = 47, 48
QS = [0, 2, 4, 1, 3, 6, 5, 7]
QI = {q: i for i, q in enumerate(QS)}
ORDERS = [(1, 2, 4), (2, 4, 1), (4, 1, 2)]
X_CHUNKS = [(0, 40, 0, BLK, 0), (40, 32, 0, BLK, 1), (72, 32, 0, BLK, 2)]
Y_CHUNKS = [(0, 16, 0, BLK, 0), (16, 16, 0, BLK, 1), (32, 16, 0, BLK, 2)]
D1_CHUNKS = [(0, 40, 0, BLK, 0), (40, 40, 0, BLK, 1), (80, 40, 0, BLK, 2),
             (120, 8, 0, 384, 0), (120, 8, 384, 384, 1), (120, 8, 768, 256, 2)]
GWO_HALF, GWH_HALF = 24, 56
OUT_ROWS = F_PAD + CLS_PAD
M_TILE = 256
A_AHEAD = 5


def forwards(q, order_id, swapped):
    first, second, third = order = ORDERS[order_id]
    if order_id in swapped and q == first:
        return [(first, second)]
    if order_id in swapped and q == second:
        return [(second, third), (first, third)]
    return [(q, d) for d in order[1 + max(order.index(d) for d in order if q & d):]]


def last_dim(q, order_id):
    return max((d for d in ORDERS[order_id] if q & d), key=ORDERS[order_id].index)


def plan_gather(chunks, cost, max_group, swapped):
    sizes = [n * lanes * 0.002 for _, n, _, lanes, _ in chunks]
    link = {1: 0.0, 2: 0.0, 4: 0.0, 0: 0.0}
    ops, arrive, relayed, ready = [], {}, {}, [0]
    now = 0.0

    def send(table, key, dim, size):
        link[dim] = max(now, link[dim]) + size / (46.6 if dim else 600.0)
        table[key] = link[dim] + (2.3 if dim else 0.95)

    for j in range(3):
        for k, chunk in enumerate(chunks):
            d = ORDERS[chunk[4]][j]
            send(arrive, (d, k), d, sizes[k])
    send(relayed, 0, 0, sum(sizes))
    got = {q: 0 for q in range(8)}
    while arrive or relayed or ready:
        key = min(arrive, key=arrive.get, default=None)
        if key is not None and arrive[key] <= now:
            del arrive[key]
            q, k = key
            ops.append(('recv', q, k))
            for src, d in forwards(q, chunks[k][4], swapped):
                send(arrive, (src | d, k), d, sizes[k])
            got[q] += 1
            if got[q] == len(chunks):
                ops.append(('relay', q))
                send(relayed, q, 0, sum(sizes))
                ready.append(2 * QI[q])
            continue
        for q in sorted(relayed, key=relayed.get):
            if relayed[q] <= now:
                del relayed[q]
                ops.append(('take', q))
                ready.append(2 * QI[q] + 1)
        if ready:
            ops.append(('dot', ready[:max_group]))
            now += cost(len(ready[:max_group]))
            ready = ready[max_group:]
        else:
            now = min(list(arrive.values()) + list(relayed.values()))
    return ops


def dot_last(lhs, rhs):
    return lax.dot_general(lhs, rhs, (((1,), (1,)), ((), ())), preferred_element_type=F32)


def dot_first(lhs, rhs):
    return lax.dot_general(lhs, rhs, (((0,), (0,)), ((), ())), preferred_element_type=F32)


def step_kernel(adj_hbm, x_hbm, wh_hbm, wot_hbm, lab_hbm, msk_hbm, bm_hbm, out_ref,
                x_ref, wh_ref, wot_ref, lab_ref, msk_ref, bm_ref, mask_tab,
                adj, xall, yall, y1b, z1, z1t, z2, z2t, turned, hid, gt, et, con, part2, part1, rb2, rb1, whs, wos, macc, lossv,
                gwos, gwop, gwor, gwog, gwof, gwhs, gwhp, gwhr, gwhg, gwhf,
                io_sem, a_sem, ici_send, d2d_send, recv_a, d2d_a, recv_b, d2d_b,
                gwo_send, gwo_recv, gwh_send, gwh_recv):
    me = lax.axis_index(AXIS_NAME)
    coords = [me % 2, (me // 2) % 2, (me // 4) % 2, me // 8]

    def device_of(rel):
        total = 0
        for bit in range(4):
            total = total + ((coords[bit] + ((rel >> bit) & 1)) % 2) * (1 << bit)
        return total

    devices = [device_of(rel) for rel in range(NB)]

    def dev(rel):
        return devices[rel]

    def rel_of(slot):
        return 2 * QS[slot // 2] + slot % 2

    def rcopy(src, dst, send_sem, recv_sem, rel):
        return pltpu.make_async_remote_copy(src_ref=src, dst_ref=dst, send_sem=send_sem, recv_sem=recv_sem,
                                            device_id=(dev(rel),), device_id_type=MESH)

    def a_copy(slot, blk=0):
        return pltpu.make_async_copy(adj_hbm.at[:, pl.ds(pl.multiple_of(blk * BLK, BLK), BLK)], adj.at[slot], a_sem.at[slot])

    plan1 = plan_gather(X_CHUNKS, lambda n: 0.2 + 0.54 * n, 2, (2,))
    a_order = [slot for op in plan1 if op[0] == 'dot' for slot in op[1]]

    def start_a(lo, hi):
        for slot in a_order[lo:hi]:
            a_copy(slot, dev(rel_of(slot))).start()

    loads = [pltpu.make_async_copy(src, dst, io_sem.at[n]) for n, (src, dst) in enumerate(
        [(x_hbm, x_ref), (wh_hbm, wh_ref), (wot_hbm, wot_ref), (lab_hbm, lab_ref), (msk_hbm, msk_ref), (bm_hbm, bm_ref)])]
    barrier = pltpu.get_barrier_semaphore()
    peers = [1, 2, 4, 8]
    for rel in peers:
        pl.semaphore_signal(barrier, inc=1, device_id=(dev(rel),), device_id_type=MESH)

    for load in loads:
        load.start()
    start_a(0, A_AHEAD)
    macc[...] = jnp.zeros_like(macc)
    z1[...] = jnp.zeros_like(z1)
    z2[...] = jnp.zeros_like(z2)
    z2t[...] = jnp.zeros_like(z2t)
    whs[...] = jnp.zeros_like(whs)
    wos[...] = jnp.zeros_like(wos)
    for load in loads:
        load.wait()
    xall[0, 0:F_PAD - 8, :] = x_ref[0:F_PAD - 8, :]
    xall[0, F_PAD - 8:F_PAD, :] = jnp.concatenate([x_ref[F_PAD - 8:F_IN, :], jnp.zeros((F_PAD - F_IN, BLK), BF16)], axis=0)
    whs[0:F_IN, :] = wh_ref[...].astype(BF16)
    wos[0:CLS, :] = wot_ref[...].astype(BF16)
    pl.semaphore_wait(barrier, len(peers))

    for n in range(NB):
        mask_tab[n] = bm_ref[me, dev(rel_of(n))]

    def mask_of(slot):
        return mask_tab[slot]


    def gather_product(buf, chunks, recv, recv_d2d, ops, swapped, first, dots):
        def ici(src_q, dim, k):
            dst_q = src_q ^ dim
            lo, n, lane, lanes, _ = chunks[k]
            return rcopy(buf.at[2 * QI[src_q], pl.ds(lo, n), pl.ds(lane, lanes)],
                         buf.at[2 * QI[dst_q], pl.ds(lo, n), pl.ds(lane, lanes)],
                         ici_send, recv.at[k * 7 + QI[dst_q] - 1], 2 * dim)

        def relay(q):
            return rcopy(buf.at[2 * QI[q]], buf.at[2 * QI[q] + 1], d2d_send, recv_d2d.at[QI[q]], 1)

        for j in range(3):
            for k, chunk in enumerate(chunks):
                ici(0, ORDERS[chunk[4]][j], k).start()
        relay(0).start()
        first()
        for op, q, *k in ops:
            if op == 'dot':
                dots(q)
            elif op == 'take':
                relay(q).wait_recv()
            elif op == 'relay':
                relay(q).start()
            else:
                order_id = chunks[k[0]][4]
                d = last_dim(q, order_id)
                ici(q ^ d, d, k[0]).wait_recv()
                for src, d in forwards(q, order_id, swapped):
                    ici(src, d, k[0]).start()
        for count, sem, rel in ((7, ici_send, 2), (8, d2d_send, 1)):
            sent = buf.at[pl.ds(0, count)]
            rcopy(sent, sent, sem, recv.at[0], rel).wait_send()

    def accumulate(out, slots, blocks):
        for lo in range(0, BLK, M_TILE):
            acc = out[lo:lo + M_TILE, :]
            for slot, block in zip(slots, blocks):
                acc = acc + dot_last(adj[slot, lo:lo + M_TILE, :], block)
            out[lo:lo + M_TILE, :] = acc

    def dots1(slots):
        for slot in slots:
            a_copy(slot).wait()
            ahead = a_order.index(slot) + A_AHEAD
            start_a(ahead, ahead + 1)
        for j, slot in enumerate(slots):
            yt = dot_first(whs[...], xall[slot]).astype(BF16)
            y1b[j] = (yt.astype(F32) * mask_of(slot).astype(F32)).astype(BF16)
        accumulate(z1, slots, [y1b[j] for j in range(len(slots))])

    gather_product(xall, X_CHUNKS, recv_a, d2d_a, plan1, (2,), lambda: None, dots1)

    cls_id = lax.broadcasted_iota(jnp.int32, (CLS_PAD, BLK), 0)
    weight = msk_ref[...].astype(F32)
    hid[...] = jnp.maximum(z1[...], 0.0).astype(BF16)
    yall[0] = jnp.where(cls_id == CLS, weight, dot_last(wos[...], hid[...])).astype(BF16)

    def dots2(slots):
        blocks = []
        for slot in slots:
            macc[...] += yall[slot, CLS_PAD - 16:CLS_PAD, :].astype(F32)
            blocks.append((yall[slot].astype(F32) * mask_of(slot).astype(F32)).astype(BF16))
        if len(slots) == 1:
            accumulate(z2, slots, blocks)
            return
        stream, held = slots
        turned[0] = jnp.transpose(adj[held, 0:M_TILE, :])
        for n in range(BLK // M_TILE):
            tile = slice(M_TILE * n, M_TILE * (n + 1))
            if n + 1 < BLK // M_TILE:
                turned[(n + 1) % 2] = jnp.transpose(adj[held, M_TILE * (n + 1):M_TILE * (n + 2), :])
            z2[tile, :] += dot_last(adj[stream, tile, :], blocks[0])
            z2t[:, tile] += jnp.dot(blocks[1], turned[n % 2], preferred_element_type=F32)

    def keep_sign():
        z1t[...] = jnp.transpose(z1[...])

    plan2 = plan_gather(Y_CHUNKS, lambda n: 0.43 + 0.25 * n, 2, (0, 1))
    gather_product(yall, Y_CHUNKS, recv_b, d2d_b, plan2, (0, 1), keep_sign, dots2)
    label_count = jnp.sum(macc[15:16, :])

    zt = jnp.transpose(z2[...]) + z2t[...]
    valid = cls_id < CLS
    top = jnp.max(jnp.where(valid, zt, -jnp.inf), axis=0, keepdims=True)
    expz = jnp.where(valid, jnp.exp(zt - top), 0.0)
    log_norm = jnp.log(jnp.sum(expz, axis=0, keepdims=True)) + top
    one_hot = cls_id == lab_ref[...]
    picked = jnp.sum(jnp.where(one_hot, zt, 0.0), axis=0, keepdims=True)
    loss_terms = weight * (log_norm - picked)
    acc = loss_terms[:, 0:128]
    for n in range(1, BLK // 128):
        acc = acc + loss_terms[:, 128 * n:128 * (n + 1)]
    lossv[...] = acc
    prob = jnp.exp(zt - log_norm)
    grad = (prob - one_hot.astype(F32)) * (weight / label_count)
    gt[...] = jnp.where(valid, grad, 0.0).astype(BF16)


    def reduce_pass(lhs_ref, rows, chunks, part, rb, recv, recv_d2d, early, tail, hooks):
        parts = range(len(chunks))

        def order_of(k):
            return ORDERS[chunks[k][4]]

        def dim_of(q, k):
            return next(d for d in reversed(order_of(k)) if q & d)

        def ici(q, k):
            lo, n, lane, lanes, _ = chunks[k]
            idx = k * 7 + QI[q] - 1
            return rcopy(con.at[2 * QI[q], pl.ds(lo, n), pl.ds(lane, lanes)],
                         rb.at[QI[q] - 1, pl.ds(lo, n), pl.ds(lane, lanes)], ici_send,
                         recv.at[idx], 2 * dim_of(q, k))

        def d2d(i):
            return rcopy(con.at[2 * i + 1, pl.ds(0, rows), :], part.at[i], d2d_send, recv_d2d.at[i], 1)

        cuts = [chunks[0][0], chunks[1][0], chunks[2][0], rows]

        def d2d_part(p):
            span = pl.ds(cuts[p], cuts[p + 1] - cuts[p])
            return rcopy(con.at[15, span, :], part.at[7, span, :], d2d_send, recv_d2d.at[8 + p if p else 7], 1)

        def sources(q, k):
            out = []
            for d in reversed(order_of(k)):
                if q & d:
                    break
                out.append(q ^ d)
            return out

        def compute(slot):
            lhs = (lhs_ref[...].astype(F32) * mask_of(slot).astype(F32)).astype(BF16)
            con[slot, 0:rows, :] = jnp.dot(lhs, adj[slot], preferred_element_type=F32)

        waiting = {(q, k): set(sources(q, k)) for q in range(8) for k in parts}

        def pair_sum(q):
            i = QI[q]
            for p in range(3) if i == 7 else [None]:
                lo, hi = (0, rows) if p is None else (cuts[p], cuts[p + 1])
                (d2d(i) if p is None else d2d_part(p)).wait_recv()
                con[2 * i, lo:hi, :] += part[i, lo:hi, :]
                for k in parts:
                    if q and not waiting[q, k] and lo <= chunks[k][0] < hi:
                        ici(q, k).start()

        def take(src, k):
            d = dim_of(src, k)
            q = src ^ d
            lo, n, lane, lanes, _ = chunks[k]
            ici(src, k).wait_recv()
            con[2 * QI[q], lo:lo + n, lane:lane + lanes] += rb[QI[src] - 1, lo:lo + n, lane:lane + lanes]
            waiting[q, k].discard(src)
            if q and not waiting[q, k]:
                ici(q, k).start()

        def body(n, carry):
            i = 7 - n
            compute(2 * i + 1)

            @pl.when(n == 0)
            def _():
                for p in range(3):
                    d2d_part(p).start()

            @pl.when(n > 0)
            def _():
                d2d(i).start()

            compute(2 * i)
            for m in range(8):
                @pl.when(n == m)
                def _(m=m):
                    if m:
                        pair_sum(QS[8 - m])
                    for r in early.get(m, ()):
                        take_rank(r)
                    for hook in hooks.get(m, ()):
                        hook()
            return carry

        rank = {q: r for r, q in enumerate(reversed(QS))}

        def sources_of(k, phase):
            d = order_of(k)[2 - phase]
            later = order_of(k)[3 - phase:]
            return sorted((q for q in range(1, 8) if q & d and not any(q & e for e in later)), key=rank.get)

        def take_rank(r, phase=0):
            for k in parts:
                take(sources_of(k, phase)[r], k)

        lax.fori_loop(0, 8, body, 0)
        for step in tail:
            if step is None:
                pair_sum(0)
            elif isinstance(step, str):
                for hook in hooks[step]:
                    hook()
            else:
                take_rank(step[1], step[0])
        for count, sem, rel in ((7, ici_send, 2), (8, d2d_send, 1)):
            sent = con.at[pl.ds(0, count), pl.ds(0, rows), :]
            rcopy(sent, sent, sem, recv.at[0], rel).wait_send()

    reduce_pass(gt, CLS_PAD, Y_CHUNKS, part2, rb2, recv_a, d2d_a, {5: [0], 6: [1], 7: [2]}, [None, (1, 0), (0, 3), (1, 1), (2, 0)], {})
    d2t = con[0, 0:CLS_PAD, :].astype(BF16)
    gwo = jnp.dot(d2t, hid[...], preferred_element_type=F32)
    et[...] = jnp.where(z1t[...] > 0, dot_first(wos[...], d2t), 0.0).astype(BF16)
    row_id = lax.broadcasted_iota(jnp.int32, (CLS_PAD, HID), 0)
    gwos[...] = jnp.where(row_id == CLS, lossv[...], gwo)

    core = coords[0]

    def all_sum(rows, total_rows, src, halves, other, own, gathered, final, send, recv):
        def prepare():
            halves[0] = src[0:rows, :]
            halves[1, 0:total_rows - rows, :] = src[rows:total_rows, :]
            if total_rows < 2 * rows:
                halves[1, total_rows - rows:rows, :] = jnp.zeros((2 * rows - total_rows, HID), F32)

        pair = rcopy(halves.at[1 - core], other, send.at[0], recv.at[0], 1)
        sends = [rcopy(gathered.at[0], gathered.at[q], send.at[1], recv.at[q], 2 * q) for q in range(1, 8)]
        back = rcopy(own, final, send.at[2], recv.at[8], 1)

        def start():
            prepare()
            pair.start()

        def spread():
            pair.wait()
            gathered[0] = halves[core] + other[...]
            for q in (7, 6, 5, 3, 4, 2, 1):
                sends[q - 1].start()

        def collect():
            for cp in sends:
                cp.wait_recv()
            rcopy(gathered.at[pl.ds(0, 7)], gathered.at[pl.ds(0, 7)], send.at[1], recv.at[0], 2).wait_send()
            g = gathered
            own[...] = ((g[0] + g[1]) + (g[2] + g[3])) + ((g[4] + g[5]) + (g[6] + g[7]))
            back.start()

        def finish():
            halves[core] = own[...]
            back.wait()
            halves[1 - core] = final[...]

        return start, spread, collect, finish

    gwo_start, gwo_spread, gwo_collect, gwo_finish = all_sum(GWO_HALF, CLS_PAD, gwos, gwop, gwof.at[0], gwor, gwog,
                                                             gwof.at[1], gwo_send, gwo_recv)
    gwh_start, gwh_spread, gwh_collect, gwh_finish = all_sum(GWH_HALF, F_PAD, gwhs, gwhp, gwhf.at[0], gwhr, gwhg,
                                                             gwhf.at[1], gwh_send, gwh_recv)
    gwo_start()

    def gwo_out():
        gwo_finish()
        out_ref[F_PAD:F_PAD + GWO_HALF, :] = gwop[0]
        out_ref[F_PAD + GWO_HALF:OUT_ROWS, :] = gwop[1]
        loss = jnp.sum(gwop[1, GWO_HALF - 1:GWO_HALF, :], axis=1, keepdims=True) / label_count
        out_ref[OUT_ROWS - 1:OUT_ROWS, :] = jnp.broadcast_to(loss, (1, HID))

    reduce_pass(et, HID, D1_CHUNKS, part1, rb1, recv_b, d2d_b, {},
                [(0, 0), (0, 1), (0, 2), 'mid', None, (0, 3), (1, 0), (1, 1), 'late', (2, 0)],
                {0: [gwo_spread], 'mid': [gwo_collect], 'late': [gwo_out]})
    gwhs[...] = dot_last(xall[0], con[0].astype(BF16))
    gwh_start()
    gwh_spread()
    gwh_collect()
    gwh_finish()
    out_ref[0:GWH_HALF, :] = gwhp[0]
    out_ref[GWH_HALF:F_PAD, :] = gwhp[1, 0:F_PAD - GWH_HALF, :]


def split_kernel(sums_ref, gwh_ref, gwot_ref, loss_ref):
    gwh_ref[...] = sums_ref[0:F_IN, :]
    gwot_ref[...] = sums_ref[F_PAD:F_PAD + CLS, :]
    loss_ref[...] = sums_ref[OUT_ROWS - 1:OUT_ROWS, 0:1]


def device_step(adj_rows, feat_rows, w_hidden, w_output, labels, train_mask, block_mask):
    dma = pltpu.SemaphoreType.DMA
    vmem = pl.BlockSpec(memory_space=pltpu.VMEM)
    hbm = pl.BlockSpec(memory_space=pl.ANY)
    sums = pl.pallas_call(
        step_kernel,
        name='gcn_step',
        out_shape=pltpu.VMEM((OUT_ROWS, HID), F32),
        in_specs=[hbm] * 7,
        out_specs=vmem,
        scratch_shapes=[
            pltpu.VMEM((F_IN, BLK), BF16),
            pltpu.VMEM((F_IN, HID), F32),
            pltpu.VMEM((CLS, HID), F32),
            pltpu.VMEM((1, BLK), jnp.int32),
            pltpu.VMEM((1, BLK), jnp.int32),
            pltpu.SMEM((NB, NB), jnp.int32),
            pltpu.SMEM((NB,), jnp.int32),
            pltpu.VMEM((NB, BLK, BLK), BF16),
            pltpu.VMEM((NB, F_PAD, BLK), BF16),
            pltpu.VMEM((NB, CLS_PAD, BLK), BF16),
            pltpu.VMEM((2, HID, BLK), BF16),
            pltpu.VMEM((BLK, HID), F32),
            pltpu.VMEM((HID, BLK), F32),
            pltpu.VMEM((BLK, CLS_PAD), F32),
            pltpu.VMEM((CLS_PAD, BLK), F32),
            pltpu.VMEM((2, BLK, M_TILE), BF16),
            pltpu.VMEM((BLK, HID), BF16),
            pltpu.VMEM((CLS_PAD, BLK), BF16),
            pltpu.VMEM((HID, BLK), BF16),
            pltpu.VMEM((NB, HID, BLK), F32),
            pltpu.VMEM((8, CLS_PAD, BLK), F32),
            pltpu.VMEM((8, HID, BLK), F32),
            pltpu.VMEM((7, CLS_PAD, BLK), F32),
            pltpu.VMEM((7, HID, BLK), F32),
            pltpu.VMEM((F_PAD, HID), BF16),
            pltpu.VMEM((CLS_PAD, HID), BF16),
            pltpu.VMEM((16, BLK), F32),
            pltpu.VMEM((1, 128), F32),
            pltpu.VMEM((CLS_PAD, HID), F32),
            pltpu.VMEM((2, GWO_HALF, HID), F32),
            pltpu.VMEM((GWO_HALF, HID), F32),
            pltpu.VMEM((8, GWO_HALF, HID), F32),
            pltpu.VMEM((2, GWO_HALF, HID), F32),
            pltpu.VMEM((F_PAD, HID), F32),
            pltpu.VMEM((2, GWH_HALF, HID), F32),
            pltpu.VMEM((GWH_HALF, HID), F32),
            pltpu.VMEM((8, GWH_HALF, HID), F32),
            pltpu.VMEM((2, GWH_HALF, HID), F32),
            dma((6,)), dma((NB,)), dma, dma, dma((21,)), dma((11,)), dma((42,)), dma((11,)),
            dma((3,)), dma((9,)), dma((3,)), dma((9,)),
        ],
        compiler_params=pltpu.CompilerParams(collective_id=0, has_side_effects=True, vmem_limit_bytes=64000000),
    )(adj_rows, feat_rows.T, w_hidden, w_output.T, labels[None, :], train_mask[None, :], block_mask)
    gwh, gwot, loss = pl.pallas_call(
        split_kernel,
        name='split_sums',
        out_shape=(jax.ShapeDtypeStruct((F_IN, HID), F32), jax.ShapeDtypeStruct((CLS, HID), F32),
                   jax.ShapeDtypeStruct((1, 1), F32)),
        in_specs=[vmem],
        out_specs=(vmem, vmem, vmem),
    )(pltpu.with_memory_space_constraint(sums, pltpu.VMEM))
    return loss[0, 0], gwh, gwot.T


def solution(mesh):
    row_spec = P(AXIS_NAME, None)
    vec_spec = P(AXIS_NAME)
    return jax.shard_map(device_step, mesh=mesh, in_specs=(row_spec, row_spec, P(), P(), vec_spec, vec_spec, P()), out_specs=(P(), P(), P()), check_vma=False)
```
